32 devices in a mesh: data: 8 (over z, y), pipe: 4 (over x, core).
Axes of the slice: x: 2, y: 2, z: 4, core: 2. Of those that a mesh axis runs over, the one named last changes fastest.
Arguments:
- acts_in: bfloat16 [192, 64, 512], P(('data', 'pipe'))
- cot_out: bfloat16 [192, 64, 512], P(('data', 'pipe'))
- seq_lens: int32 [192], P(('data', 'pipe'))
- w_qkv: bfloat16 [4, 512, 1536], P('pipe')
- w_out: bfloat16 [4, 8, 64, 512], P('pipe')
- w_up: bfloat16 [4, 512, 2048], P('pipe')
- w_down: bfloat16 [4, 2048, 512], P('pipe')
- gain_attn: bfloat16 [4, 512], P('pipe')
- gain_mlp: bfloat16 [4, 512], P('pipe')
Outputs:
- output 1: bfloat16 [192, 64, 512], P(('data', 'pipe'))
- output 2: float32 [4, 512, 1536], P('pipe')
- output 3: float32 [4, 8, 64, 512], P('pipe')
- output 4: float32 [4, 512, 2048], P('pipe')
- output 5: float32 [4, 2048, 512], P('pipe')
- output 6: float32 [4, 512], P('pipe')
- output 7: float32 [4, 512], P('pipe')
All inputs are finite; a program needn't handle non-finite values.
Results may differ from the reference program's by a relative error of at most 0.02.
Values are sent between devices in bfloat16 or wider.
A program may use at most 1 GiB of HBM per device.

```python
import jax
import jax.numpy as jnp
from jax import lax

D = 512
HEADS = 8
HEAD = 64
SEQ = 64
MICRO = 6
LAYERS_STAGE = 1
DATA_DEVS = 8
PIPE_DEVS = 4

NUM_LAYERS = PIPE_DEVS * LAYERS_STAGE
NUM_SEQS = DATA_DEVS * PIPE_DEVS * MICRO
FFN_DIM = 4 * D
MIN_LEN = SEQ // 4
NORM_EPS = 1e-5


def draw_lengths(key):
    key_len, key_perm = jax.random.split(key)
    len_draw = jax.random.randint(key_len, (NUM_SEQS,), MIN_LEN, SEQ + 1)
    rank_perm = jax.random.permutation(key_perm, NUM_SEQS)
    return jnp.where(rank_perm == 0, SEQ, jnp.where(rank_perm == 1, MIN_LEN, len_draw)).astype(jnp.int32)


def setup_inputs(seed: int = 0) -> dict:
    key_list = jax.random.split(jax.random.key(seed), 9)
    depth_scale = (2.0 / NUM_LAYERS) ** 0.5

    def normal_draw(key_idx, shape, scale):
        return (jax.random.normal(key_list[key_idx], shape, jnp.float32) * scale).astype(jnp.bfloat16)

    def gain_draw(key_idx):
        noise = jax.random.uniform(key_list[key_idx], (NUM_LAYERS, D), jnp.float32, -1.0, 1.0)
        return (1.0 + 0.5 * noise).astype(jnp.bfloat16)

    return {
        'acts_in': normal_draw(0, (NUM_SEQS, SEQ, D), 1.0),
        'cot_out': normal_draw(1, (NUM_SEQS, SEQ, D), (NUM_SEQS * SEQ) ** -0.5),
        'seq_lens': draw_lengths(key_list[2]),
        'w_qkv': normal_draw(3, (NUM_LAYERS, D, 3 * D), D ** -0.5),
        'w_out': normal_draw(4, (NUM_LAYERS, HEADS, HEAD, D), D ** -0.5),
        'w_up': normal_draw(5, (NUM_LAYERS, D, FFN_DIM), D ** -0.5),
        'w_down': normal_draw(6, (NUM_LAYERS, FFN_DIM, D), FFN_DIM ** -0.5 * depth_scale),
        'gain_attn': gain_draw(7),
        'gain_mlp': gain_draw(8),
    }


def rms_norm(hidden, gain):
    hid_f32 = hidden.astype(jnp.float32)
    inv_rms = lax.rsqrt(jnp.mean(hid_f32 * hid_f32, axis=-1, keepdims=True) + NORM_EPS)
    return (hid_f32 * inv_rms * gain.astype(jnp.float32)).astype(jnp.bfloat16)


def attend(qkv_all, seq_len):
    heads_all = qkv_all.astype(jnp.float32).reshape(SEQ, 3, HEADS, HEAD)
    scores = jnp.einsum('qhe,khe->hqk', heads_all[:, 0], heads_all[:, 1]) * HEAD ** -0.5
    positions = jnp.arange(SEQ)
    visible = (positions[None, :] <= positions[:, None]) & (positions[None, :] < seq_len)
    scores = jnp.where(visible[None], scores, -1e30)
    attn_probs = jax.nn.softmax(scores, axis=-1).astype(jnp.bfloat16)
    context = jnp.einsum('hqk,khe->qhe', attn_probs.astype(jnp.float32), heads_all[:, 2])
    return context.astype(jnp.bfloat16).reshape(SEQ, D)


def layer_apply(hidden, layer_w, seq_len):
    w_qkv, w_out, w_up, w_down, gain_attn, gain_mlp = layer_w
    qkv_all = jnp.dot(rms_norm(hidden, gain_attn), w_qkv, preferred_element_type=jnp.float32).astype(jnp.bfloat16)
    context = attend(qkv_all, seq_len)
    attn_out = jnp.dot(context, w_out.reshape(D, D), preferred_element_type=jnp.float32)
    mid_hidden = (hidden.astype(jnp.float32) + attn_out).astype(jnp.bfloat16)
    pre_act = jnp.dot(rms_norm(mid_hidden, gain_mlp), w_up, preferred_element_type=jnp.float32)
    gelu_out = jax.nn.gelu(pre_act, approximate=False).astype(jnp.bfloat16)
    mlp_out = jnp.dot(gelu_out, w_down, preferred_element_type=jnp.float32)
    return (mid_hidden.astype(jnp.float32) + mlp_out).astype(jnp.bfloat16)


def forward_seq(weights, seq_in, seq_len):
    def body(hidden, layer_w):
        return layer_apply(hidden, layer_w, seq_len), None

    hidden, _ = lax.scan(jax.checkpoint(body), seq_in, weights)
    valid = jnp.arange(SEQ)[:, None] < seq_len
    return jnp.where(valid, hidden, jnp.zeros_like(hidden))


def reference(acts_in, cot_out, seq_lens, w_qkv, w_out, w_up, w_down, gain_attn, gain_mlp):
    weights = (w_qkv, w_out, w_up, w_down, gain_attn, gain_mlp)

    def seq_step(grad_acc, seq_item):
        seq_in, seq_cot, seq_len = seq_item
        seq_out, pullback = jax.vjp(lambda layer_ws: forward_seq(layer_ws, seq_in, seq_len), weights)
        grad_seq = pullback(seq_cot)[0]
        new_acc = tuple(acc_part + grad_part.astype(jnp.float32) for acc_part, grad_part in zip(grad_acc, grad_seq))
        return new_acc, seq_out

    grad_init = tuple(jnp.zeros(w_part.shape, jnp.float32) for w_part in weights)
    grad_total, acts_out = lax.scan(seq_step, grad_init, (acts_in, cot_out, seq_lens))
    return (acts_out, grad_total[0], grad_total[1], grad_total[2], grad_total[3], grad_total[4], grad_total[5])
```

```python
import functools
import jax
import jax.numpy as jnp
from jax import lax
from jax.experimental import pallas as pl
from jax.experimental.pallas import tpu as pltpu
from jax.sharding import PartitionSpec as P

NORM_EPS = 1e-5
MESH = pl.DeviceIdType.MESH
F32 = jnp.float32
BF16 = jnp.bfloat16
SEQ = 64
HEAD = 64
D = 512
FFN = 2048
PIPE = 4
SEQ_MB = 3
ROWS = SEQ_MB * SEQ
PAIRS = 4
UNIT = SEQ_MB * PAIRS * SEQ


def dot_nn(lhs, rhs):
    return lax.dot_general(lhs, rhs, (((1,), (0,)), ((), ())), preferred_element_type=F32)


def dot_nt(lhs, rhs):
    return lax.dot_general(lhs, rhs, (((1,), (1,)), ((), ())), preferred_element_type=F32)


def dot_tn(lhs, rhs):
    return lax.dot_general(lhs, rhs, (((0,), (0,)), ((), ())), preferred_element_type=F32)


def pass_kernel(n_mb, acts_ref, cot_ref, lens_ref, wqkv_hbm, wout_hbm, wup_hbm, wdown_hbm, ga_ref, gm_ref,
                out_ref, gqkv_ref, gout_ref, gup_ref, gdown_ref, gga_ref, ggm_ref,
                wqkv, wout, wup, wdown, lens_buf, xin, cin, hout, na_s, qkv_s, ctx_s, mid_s, nm_s, gelu_s, gp_s,
                dpre_s, dmid_s, p_s, s_scr, gstage,
                w_sem, in_sem, x_sem, c_sem, len_sem, send_sem, home_sem, g_sem):
    pos = lax.axis_index('pipe')
    mb_home = n_mb // PIPE
    last = PIPE - 1

    w_copies = [pltpu.make_async_copy(src, dst, w_sem.at[idx]) for idx, (src, dst) in enumerate(
        ((wqkv_hbm, wqkv), (wout_hbm, wout), (wup_hbm, wup), (wdown_hbm, wdown)))]
    for w_copy in w_copies:
        w_copy.start()

    barrier = pltpu.get_barrier_semaphore()
    for step in range(1, PIPE):
        pl.semaphore_signal(barrier, inc=1, device_id={'pipe': (pos + step) % PIPE}, device_id_type=MESH)
    pl.semaphore_wait(barrier, PIPE - 1)

    def rows_of(mb):
        return pl.ds(pl.multiple_of(mb * ROWS, 64), ROWS)

    def place(src, dst, send, recv, target):
        @pl.when(target == pos)
        def _():
            pltpu.make_async_copy(src, dst, recv).start()

        @pl.when(target != pos)
        def _():
            pltpu.make_async_remote_copy(src_ref=src, dst_ref=dst, send_sem=send, recv_sem=recv,
                                         device_id={'pipe': target}, device_id_type=MESH).start()

    def place_done(src, send, target):
        @pl.when(target != pos)
        def _():
            pltpu.make_async_copy(src, src, send).wait()

    n_len = lens_ref.shape[0]
    spread = []
    for half in range(mb_home):
        mb = pos * mb_home + half
        own = pl.ds(half * ROWS, ROWS)
        spread.append((acts_ref.at[own], xin.at[rows_of(mb)], in_sem.at[half], x_sem.at[mb], 0))
        spread.append((cot_ref.at[own], cin.at[rows_of(mb)], in_sem.at[mb_home + half], c_sem.at[mb], last))
    for step in range(PIPE):
        spread.append((lens_ref, lens_buf.at[pl.ds(pos * n_len, n_len)], in_sem.at[2 * mb_home + step], len_sem.at[pos],
                       (pos + step) % PIPE))
    for item in spread:
        place(*item)
    for home in range(PIPE):
        slab = lens_buf.at[pl.ds(home * n_len, n_len)]
        pltpu.make_async_copy(slab, slab, len_sem.at[home]).wait()

    lane = lax.broadcasted_iota(jnp.int32, (SEQ, 128), 1)
    row = lax.broadcasted_iota(jnp.int32, (SEQ, 128), 0)
    first = lane < HEAD
    key_pos = jnp.where(first, lane, lane - HEAD)
    lane_row = lax.broadcasted_iota(jnp.int32, (1, 128), 1)
    take_a = jnp.where(lane_row < HEAD, 1.0, 0.0).astype(BF16)
    take_b = jnp.where(lane_row < HEAD, 0.0, 1.0).astype(BF16)

    def blocks(pair_cols):
        return jnp.concatenate([pair_cols * take_a, pair_cols * take_b], axis=0)

    def halves_sum(arr):
        sum_a = jnp.sum(jnp.where(first[None], arr, 0.0), axis=-1, keepdims=True)
        sum_b = jnp.sum(jnp.where(first[None], 0.0, arr), axis=-1, keepdims=True)
        return sum_a, sum_b

    def lens_of(mb, seq):
        return lens_buf[mb * SEQ_MB + seq][0:1, :]

    def valid_mask(lens_row):
        ok = jnp.where(row < lens_row, 1.0, 0.0)
        return jnp.concatenate([ok] * (D // 128), axis=1)

    def inv_rms(val):
        return lax.rsqrt(jnp.mean(val * val, axis=-1, keepdims=True) + NORM_EPS)

    def forward(mb, _):
        rows = rows_of(mb)
        x_view = xin.at[rows]
        pltpu.make_async_copy(x_view, x_view, x_sem.at[mb]).wait()
        gain_a = ga_ref[...]
        hid = xin[rows, :].astype(F32)
        normed = (hid * inv_rms(hid) * gain_a).astype(BF16)
        na_s[rows, :] = normed
        for part in range(3):
            cols = slice(part * D, (part + 1) * D)
            qkv_s[rows, cols] = dot_nn(normed, wqkv[:, cols]).astype(BF16)

        def seq_rows(seq):
            return pl.ds(pl.multiple_of(mb * ROWS + seq * SEQ, 64), SEQ)

        for seq in range(SEQ_MB):
            for pair in range(PAIRS):
                q_cols = qkv_s[seq_rows(seq), pair * 128:(pair + 1) * 128]
                k_cols = qkv_s[seq_rows(seq), D + pair * 128:D + (pair + 1) * 128]
                spot = (seq * PAIRS + pair) * SEQ
                s_scr[spot:spot + SEQ, :] = dot_nt(q_cols, blocks(k_cols))
        for seq in range(SEQ_MB):
            visible = (key_pos <= row) & (key_pos < lens_of(mb, seq))
            spot = seq * PAIRS * SEQ
            scores = s_scr[spot:spot + PAIRS * SEQ, :].reshape(PAIRS, SEQ, 128) * (HEAD ** -0.5)
            scores = jnp.where(visible[None], scores, -1e30)
            max_a = jnp.max(jnp.where(first[None], scores, -3e38), axis=-1, keepdims=True)
            max_b = jnp.max(jnp.where(first[None], -3e38, scores), axis=-1, keepdims=True)
            expd = jnp.exp(scores - jnp.where(first[None], max_a, max_b))
            sum_a, sum_b = halves_sum(expd)
            probs = expd * jnp.where(first[None], 1.0 / sum_a, 1.0 / sum_b)
            p_rows = pl.ds(pl.multiple_of(mb * UNIT + spot, 64), PAIRS * SEQ)
            p_s[p_rows, :] = probs.reshape(PAIRS * SEQ, 128)
        for seq in range(SEQ_MB):
            for pair in range(PAIRS):
                v_cols = qkv_s[seq_rows(seq), 2 * D + pair * 128:2 * D + (pair + 1) * 128]
                p_rows = pl.ds(pl.multiple_of(mb * UNIT + (seq * PAIRS + pair) * SEQ, 64), SEQ)
                ctx_s[seq_rows(seq), pair * 128:(pair + 1) * 128] = dot_nn(
                    p_s[p_rows, :].astype(BF16), blocks(v_cols)).astype(BF16)
        mid = (hid + dot_nn(ctx_s[rows, :], wout[...])).astype(BF16)
        mid_s[rows, :] = mid
        mid_f = mid.astype(F32)
        normed_m = (mid_f * inv_rms(mid_f) * gm_ref[...]).astype(BF16)
        nm_s[rows, :] = normed_m
        for part in range(FFN // D):
            cols = slice(part * D, (part + 1) * D)
            pre = dot_nn(normed_m, wup[:, cols])
            cdf = 0.5 + 0.5 * lax.erf(pre * (0.5 ** 0.5))
            gelu_s[rows, cols] = (pre * cdf).astype(BF16)
            gp_s[rows, cols] = cdf + pre * (jnp.exp(pre * pre * -0.5) * 0.3989422804014327)
        top = mid_f + dot_nn(gelu_s[rows, :], wdown[...])
        for seq in range(SEQ_MB):
            mask = valid_mask(jnp.where(pos == last, lens_of(mb, seq), SEQ))
            piece = top[seq * SEQ:(seq + 1) * SEQ, :].astype(BF16)
            hout[seq_rows(seq), :] = jnp.where(mask > 0.0, piece.astype(F32), 0.0).astype(BF16)

        h_view = hout.at[rows]

        @pl.when(pos < last)
        def _():
            pltpu.make_async_remote_copy(src_ref=h_view, dst_ref=xin.at[rows], send_sem=send_sem.at[mb],
                                         recv_sem=x_sem.at[mb], device_id={'pipe': pos + 1}, device_id_type=MESH).start()

        @pl.when(pos == last)
        def _():
            half = mb % mb_home
            place(h_view, out_ref.at[pl.ds(pl.multiple_of(half * ROWS, 64), ROWS)], send_sem.at[mb], home_sem.at[half],
                  mb // mb_home)

        return 0

    for w_copy in w_copies:
        w_copy.wait()
    lax.fori_loop(0, n_mb, forward, 0)

    def forward_sent(mb, _):
        h_view = hout.at[rows_of(mb)]

        @pl.when(pos < last)
        def _():
            pltpu.make_async_copy(h_view, h_view, send_sem.at[mb]).wait()

        @pl.when(pos == last)
        def _():
            place_done(h_view, send_sem.at[mb], mb // mb_home)

        return 0

    lax.fori_loop(0, n_mb, forward_sent, 0)
    for half in range(mb_home):
        o_view = out_ref.at[pl.ds(half * ROWS, ROWS)]
        pltpu.make_async_copy(o_view, o_view, home_sem.at[half]).wait()

    gga_ref[...] = jnp.zeros_like(gga_ref)
    ggm_ref[...] = jnp.zeros_like(ggm_ref)

    def norm_back(hid, gain, d_normed):
        inv = inv_rms(hid)
        unit = hid * inv
        d_gain = jnp.sum((d_normed * unit).reshape(ROWS // 8, 8, D), axis=0)
        scaled = d_normed * gain
        return inv * (scaled - unit * jnp.mean(unit * scaled, axis=-1, keepdims=True)), d_gain

    def backward(mb, _):
        rows = rows_of(mb)
        c_view = cin.at[rows]
        pltpu.make_async_copy(c_view, c_view, c_sem.at[mb]).wait()

        def seq_rows(seq):
            return pl.ds(pl.multiple_of(mb * ROWS + seq * SEQ, 64), SEQ)

        for seq in range(SEQ_MB):
            mask = valid_mask(lens_of(mb, seq))
            cin[seq_rows(seq), :] = jnp.where(mask > 0.0, cin[seq_rows(seq), :].astype(F32), 0.0).astype(BF16)
        d_top = cin[rows, :]
        for part in range(FFN // D):
            cols = slice(part * D, (part + 1) * D)
            d_gelu = dot_nt(d_top, wdown[cols, :])
            dpre_s[rows, cols] = (d_gelu * gp_s[rows, cols]).astype(BF16)
        d_nm = dot_nt(dpre_s[rows, :], wup[...])
        d_add, d_gain = norm_back(mid_s[rows, :].astype(F32), gm_ref[...], d_nm)
        ggm_ref[...] += d_gain
        d_mid = d_top.astype(F32) + d_add
        d_mid_bf = d_mid.astype(BF16)
        dmid_s[rows, :] = d_mid_bf
        d_ctx = dot_nt(d_mid_bf, wout[...]).astype(BF16)
        for seq in range(SEQ_MB):
            for pair in range(PAIRS):
                v_cols = qkv_s[seq_rows(seq), 2 * D + pair * 128:2 * D + (pair + 1) * 128]
                dc = d_ctx[seq * SEQ:(seq + 1) * SEQ, pair * 128:(pair + 1) * 128]
                spot = (seq * PAIRS + pair) * SEQ
                p_rows = pl.ds(pl.multiple_of(mb * UNIT + spot, 64), SEQ)
                s_scr[spot:spot + SEQ, :] = dot_nt(dc, blocks(v_cols))
                both = dot_tn(p_s[p_rows, :].astype(BF16), dc)
                qkv_s[seq_rows(seq), 2 * D + pair * 128:2 * D + (pair + 1) * 128] = jnp.where(
                    first, both[:SEQ], both[SEQ:]).astype(BF16)
        for seq in range(SEQ_MB):
            spot = seq * PAIRS * SEQ
            p_rows = pl.ds(pl.multiple_of(mb * UNIT + spot, 64), PAIRS * SEQ)
            probs = p_s[p_rows, :].reshape(PAIRS, SEQ, 128)
            d_probs = s_scr[spot:spot + PAIRS * SEQ, :].reshape(PAIRS, SEQ, 128)
            sum_a, sum_b = halves_sum(probs * d_probs)
            d_scores = probs * (d_probs - jnp.where(first[None], sum_a, sum_b)) * (HEAD ** -0.5)
            s_scr[spot:spot + PAIRS * SEQ, :] = d_scores.reshape(PAIRS * SEQ, 128)
        for seq in range(SEQ_MB):
            for pair in range(PAIRS):
                q_at = slice(pair * 128, (pair + 1) * 128)
                k_at = slice(D + pair * 128, D + (pair + 1) * 128)
                q_cols = qkv_s[seq_rows(seq), q_at]
                k_cols = qkv_s[seq_rows(seq), k_at]
                spot = (seq * PAIRS + pair) * SEQ
                d_sc = s_scr[spot:spot + SEQ, :].astype(BF16)
                both = dot_tn(d_sc, q_cols)
                qkv_s[seq_rows(seq), q_at] = dot_nn(d_sc, blocks(k_cols)).astype(BF16)
                qkv_s[seq_rows(seq), k_at] = jnp.where(first, both[:SEQ], both[SEQ:]).astype(BF16)
        d_na = dot_nt(qkv_s[rows, :], wqkv[...])
        d_add, d_gain = norm_back(xin[rows, :].astype(F32), ga_ref[...], d_na)
        gga_ref[...] += d_gain

        @pl.when(pos > 0)
        def _():
            hout[rows, :] = (d_mid + d_add).astype(BF16)
            pltpu.make_async_remote_copy(src_ref=hout.at[rows], dst_ref=cin.at[rows], send_sem=send_sem.at[mb],
                                         recv_sem=c_sem.at[mb], device_id={'pipe': pos - 1}, device_id_type=MESH).start()

        return 0

    lax.fori_loop(0, n_mb, backward, 0)

    def wgrad(lhs, rhs, dst, n_row, n_col):
        total = n_row * n_col

        def put(tile):
            slot = tile % 2
            at_row = pl.multiple_of((tile // n_col) * 256, 256)
            at_col = pl.multiple_of((tile % n_col) * D, D)
            return pltpu.make_async_copy(gstage.at[slot], dst.at[pl.ds(at_row, 256), pl.ds(at_col, D)], g_sem.at[slot])

        def step(tile, _):
            slot = tile % 2

            @pl.when(tile >= 2)
            def _():
                put(tile - 2).wait()

            at_row = pl.multiple_of((tile // n_col) * 256, 256)
            at_col = pl.multiple_of((tile % n_col) * D, D)
            gstage[slot] = dot_tn(lhs[:, pl.ds(at_row, 256)], rhs[:, pl.ds(at_col, D)])
            put(tile).start()
            return 0

        lax.fori_loop(0, total, step, 0)
        for tile in range(total - 2, total):
            put(tile).wait()

    wgrad(gelu_s, cin, gdown_ref, FFN // 256, 1)
    wgrad(nm_s, dpre_s, gup_ref, D // 256, FFN // D)
    wgrad(ctx_s, dmid_s, gout_ref, D // 256, 1)
    wgrad(na_s, qkv_s, gqkv_ref, D // 256, 3)

    def backward_sent(mb, _):
        @pl.when(pos > 0)
        def _():
            h_view = hout.at[rows_of(mb)]
            pltpu.make_async_copy(h_view, h_view, send_sem.at[mb]).wait()

        return 0

    lax.fori_loop(0, n_mb, backward_sent, 0)
    for src, _, send, _, target in spread:
        place_done(src, send, target)


def run_pass(acts, cots, lens_tile, w_qkv, w_out, w_up, w_down, gain_a, gain_m):
    n_tok = acts.shape[0] * PIPE
    n_mb = n_tok // ROWS
    any_spec = pl.BlockSpec(memory_space=pl.ANY)
    vmem_spec = pl.BlockSpec(memory_space=pltpu.VMEM)
    dma = pltpu.SemaphoreType.DMA
    return pl.pallas_call(
        functools.partial(pass_kernel, n_mb),
        out_shape=(
            jax.ShapeDtypeStruct(acts.shape, BF16),
            jax.ShapeDtypeStruct((D, 3 * D), F32),
            jax.ShapeDtypeStruct((D, D), F32),
            jax.ShapeDtypeStruct((D, FFN), F32),
            jax.ShapeDtypeStruct((FFN, D), F32),
            jax.ShapeDtypeStruct((8, D), F32),
            jax.ShapeDtypeStruct((8, D), F32),
        ),
        in_specs=[any_spec] * 7 + [vmem_spec] * 2,
        out_specs=[any_spec] * 5 + [vmem_spec] * 2,
        scratch_shapes=[
            pltpu.VMEM((D, 3 * D), BF16),
            pltpu.VMEM((D, D), BF16),
            pltpu.VMEM((D, FFN), BF16),
            pltpu.VMEM((FFN, D), BF16),
            pltpu.VMEM((n_mb * SEQ_MB, 8, 128), jnp.int32),
            pltpu.VMEM((n_tok, D), BF16),
            pltpu.VMEM((n_tok, D), BF16),
            pltpu.VMEM((n_tok, D), BF16),
            pltpu.VMEM((n_tok, D), BF16),
            pltpu.VMEM((n_tok, 3 * D), BF16),
            pltpu.VMEM((n_tok, D), BF16),
            pltpu.VMEM((n_tok, D), BF16),
            pltpu.VMEM((n_tok, D), BF16),
            pltpu.VMEM((n_tok, FFN), BF16),
            pltpu.VMEM((n_tok, FFN), F32),
            pltpu.VMEM((n_tok, FFN), BF16),
            pltpu.VMEM((n_tok, D), BF16),
            pltpu.VMEM((n_mb * UNIT, 128), F32),
            pltpu.VMEM((UNIT, 128), F32),
            pltpu.VMEM((2, 256, D), F32),
            dma((4,)),
            dma((2 * (n_mb // PIPE) + PIPE,)),
            dma((n_mb,)),
            dma((n_mb,)),
            dma((PIPE,)),
            dma((n_mb,)),
            dma((n_mb // PIPE,)),
            dma((2,)),
        ],
        compiler_params=pltpu.CompilerParams(collective_id=0, has_side_effects=True, vmem_limit_bytes=64 * 1024 * 1024 - 131072),
    )(acts, cots, lens_tile, w_qkv, w_out, w_up, w_down, gain_a, gain_m)


def solution(mesh):
    row_spec = P(('data', 'pipe'))
    stage_spec = P('pipe')

    def device_pass(acts_in, cot_out, seq_lens, w_qkv, w_out, w_up, w_down, gain_attn, gain_mlp):
        lens_tile = jnp.broadcast_to(seq_lens[:, None, None], (seq_lens.shape[0], 8, 128))
        outs = run_pass(acts_in.reshape(-1, D), cot_out.reshape(-1, D), lens_tile, w_qkv.reshape(D, 3 * D),
                        w_out.reshape(D, D), w_up.reshape(D, FFN), w_down.reshape(FFN, D),
                        gain_attn.astype(F32), gain_mlp.astype(F32))
        acts_out, g_qkv, g_out, g_up, g_down, g_ga, g_gm = outs
        grads = (g_qkv.reshape(w_qkv.shape), g_out.reshape(w_out.shape), g_up.reshape(w_up.shape), g_down.reshape(w_down.shape),
                 jnp.sum(g_ga, axis=0, keepdims=True), jnp.sum(g_gm, axis=0, keepdims=True))
        return (acts_out.reshape(acts_in.shape),) + tuple(lax.psum(part, 'data') for part in grads)

    return jax.shard_map(device_pass, mesh=mesh, in_specs=(row_spec, row_spec, row_spec) + (stage_spec,) * 6, out_specs=(row_spec,) + (stage_spec,) * 6, check_vma=False)
```

```python
import functools
import jax
import jax.numpy as jnp
from jax import lax
from jax.experimental import pallas as pl
from jax.experimental.pallas import tpu as pltpu
from jax.sharding import PartitionSpec as P

NORM_EPS = 1e-5
MESH = pl.DeviceIdType.MESH
F32 = jnp.float32
BF16 = jnp.bfloat16
SEQ = 64
HEAD = 64
D = 512
FFN = 2048
PIPE = 4
DATA = 8
LINE = 4
TILE = 128
UNITS_A = 28
UNITS_B = 20
SLOTS = 4
SEQ_MB = 3
ROWS = SEQ_MB * SEQ
PAIRS = 4
UNIT = SEQ_MB * PAIRS * SEQ


def dot_nn(lhs, rhs):
    return lax.dot_general(lhs, rhs, (((1,), (0,)), ((), ())), preferred_element_type=F32)


def dot_nt(lhs, rhs):
    return lax.dot_general(lhs, rhs, (((1,), (1,)), ((), ())), preferred_element_type=F32)


def dot_tn(lhs, rhs):
    return lax.dot_general(lhs, rhs, (((0,), (0,)), ((), ())), preferred_element_type=F32)


def pass_kernel(n_mb, acts_ref, cot_ref, lens_ref, wqkv_hbm, wout_hbm, wup_hbm, wdown_hbm, ga_ref, gm_ref,
                out_ref, gqkv_ref, gout_ref, gup_ref, gdown_ref, gain_ref,
                wqkv, wout, wup, wdown, lens_buf, xin, cin, hout, na_s, qkv_s, ctx_s, mid_s, nm_s, gelu_s, gp_s,
                dpre_s, dmid_s, p_s, s_scr, gain_acc, gain_all, ya_buf, la_buf, ra_buf, yb_buf, lb_buf, rb_buf,
                ya_out, la_out, ra_out, yb_out, lb_out, rb_out,
                w_sem, in_sem, x_sem, c_sem, len_sem, send_sem, home_sem, sum_recv, sum_send, part_send, gain_recv, gain_send, put_sem):
    pos = lax.axis_index('pipe')
    rep = lax.axis_index('data')
    rep_z, rep_y = rep // 2, rep % 2
    n_tok = n_mb * ROWS
    mb_home = n_mb // PIPE
    last = PIPE - 1

    w_copies = [pltpu.make_async_copy(src, dst, w_sem.at[idx]) for idx, (src, dst) in enumerate(
        ((wqkv_hbm, wqkv), (wout_hbm, wout), (wup_hbm, wup), (wdown_hbm, wdown)))]
    for w_copy in w_copies:
        w_copy.start()

    barrier = pltpu.get_barrier_semaphore()
    for step in range(1, PIPE):
        pl.semaphore_signal(barrier, inc=1, device_id={'pipe': (pos + step) % PIPE}, device_id_type=MESH)
    for step in range(1, DATA):
        pl.semaphore_signal(barrier, inc=1, device_id={'data': (rep + step) % DATA}, device_id_type=MESH)
    pl.semaphore_wait(barrier, PIPE - 1 + DATA - 1)

    def rows_of(mb):
        return pl.ds(pl.multiple_of(mb * ROWS, 64), ROWS)

    def part_rows(mb, part):
        return pl.ds(pl.multiple_of(part * n_tok + mb * ROWS, 64), ROWS)

    def place(src, dst, send, recv, target):
        @pl.when(target == pos)
        def _():
            pltpu.make_async_copy(src, dst, recv).start()

        @pl.when(target != pos)
        def _():
            pltpu.make_async_remote_copy(src_ref=src, dst_ref=dst, send_sem=send, recv_sem=recv,
                                         device_id={'pipe': target}, device_id_type=MESH).start()

    def place_done(src, send, target):
        @pl.when(target != pos)
        def _():
            pltpu.make_async_copy(src, src, send).wait()

    n_len = lens_ref.shape[0]
    spread = []
    for half in range(mb_home):
        mb = pos * mb_home + half
        own = pl.ds(half * ROWS, ROWS)
        spread.append((acts_ref.at[own], xin.at[rows_of(mb)], in_sem.at[half], x_sem.at[mb], 0))
        spread.append((cot_ref.at[own], cin.at[rows_of(mb)], in_sem.at[mb_home + half], c_sem.at[mb], last))
    for step in range(PIPE):
        spread.append((lens_ref, lens_buf.at[pl.ds(pos * n_len, n_len)], in_sem.at[2 * mb_home + step], len_sem.at[pos],
                       (pos + step) % PIPE))
    for item in spread:
        place(*item)
    for home in range(PIPE):
        slab = lens_buf.at[pl.ds(home * n_len, n_len)]
        pltpu.make_async_copy(slab, slab, len_sem.at[home]).wait()

    lane = lax.broadcasted_iota(jnp.int32, (SEQ, 128), 1)
    row = lax.broadcasted_iota(jnp.int32, (SEQ, 128), 0)
    first = lane < HEAD
    key_pos = jnp.where(first, lane, lane - HEAD)
    lane_row = lax.broadcasted_iota(jnp.int32, (1, 128), 1)
    take_a = jnp.where(lane_row < HEAD, 1.0, 0.0).astype(BF16)
    take_b = jnp.where(lane_row < HEAD, 0.0, 1.0).astype(BF16)

    def blocks(pair_cols):
        return jnp.concatenate([pair_cols * take_a, pair_cols * take_b], axis=0)

    def halves_sum(arr):
        sum_a = jnp.sum(jnp.where(first[None], arr, 0.0), axis=-1, keepdims=True)
        sum_b = jnp.sum(jnp.where(first[None], 0.0, arr), axis=-1, keepdims=True)
        return sum_a, sum_b

    def lens_of(mb, seq):
        return lens_buf[mb * SEQ_MB + seq][0:1, :]

    def valid_mask(lens_row):
        ok = jnp.where(row < lens_row, 1.0, 0.0)
        return jnp.concatenate([ok] * (D // 128), axis=1)

    def inv_rms(val):
        return lax.rsqrt(jnp.mean(val * val, axis=-1, keepdims=True) + NORM_EPS)

    def forward(mb, _):
        rows = rows_of(mb)
        x_view = xin.at[rows]
        pltpu.make_async_copy(x_view, x_view, x_sem.at[mb]).wait()
        gain_a = ga_ref[...]
        hid = xin[rows, :].astype(F32)
        normed = (hid * inv_rms(hid) * gain_a).astype(BF16)
        na_s[rows, :] = normed
        for part in range(3):
            cols = slice(part * D, (part + 1) * D)
            qkv_s[rows, cols] = dot_nn(normed, wqkv[:, cols]).astype(BF16)

        def seq_rows(seq):
            return pl.ds(pl.multiple_of(mb * ROWS + seq * SEQ, 64), SEQ)

        for seq in range(SEQ_MB):
            for pair in range(PAIRS):
                q_cols = qkv_s[seq_rows(seq), pair * 128:(pair + 1) * 128]
                k_cols = qkv_s[seq_rows(seq), D + pair * 128:D + (pair + 1) * 128]
                spot = (seq * PAIRS + pair) * SEQ
                s_scr[spot:spot + SEQ, :] = dot_nt(q_cols, blocks(k_cols))
        for seq in range(SEQ_MB):
            visible = (key_pos <= row) & (key_pos < lens_of(mb, seq))
            spot = seq * PAIRS * SEQ
            scores = s_scr[spot:spot + PAIRS * SEQ, :].reshape(PAIRS, SEQ, 128) * (HEAD ** -0.5)
            scores = jnp.where(visible[None], scores, -1e30)
            max_a = jnp.max(jnp.where(first[None], scores, -3e38), axis=-1, keepdims=True)
            max_b = jnp.max(jnp.where(first[None], -3e38, scores), axis=-1, keepdims=True)
            expd = jnp.exp(scores - jnp.where(first[None], max_a, max_b))
            sum_a, sum_b = halves_sum(expd)
            probs = expd * jnp.where(first[None], 1.0 / sum_a, 1.0 / sum_b)
            p_rows = pl.ds(pl.multiple_of(mb * UNIT + spot, 64), PAIRS * SEQ)
            p_s[p_rows, :] = probs.reshape(PAIRS * SEQ, 128)
        for seq in range(SEQ_MB):
            for pair in range(PAIRS):
                v_cols = qkv_s[seq_rows(seq), 2 * D + pair * 128:2 * D + (pair + 1) * 128]
                p_rows = pl.ds(pl.multiple_of(mb * UNIT + (seq * PAIRS + pair) * SEQ, 64), SEQ)
                ctx_s[seq_rows(seq), pair * 128:(pair + 1) * 128] = dot_nn(
                    p_s[p_rows, :].astype(BF16), blocks(v_cols)).astype(BF16)
        mid = (hid + dot_nn(ctx_s[rows, :], wout[...])).astype(BF16)
        mid_s[rows, :] = mid
        mid_f = mid.astype(F32)
        normed_m = (mid_f * inv_rms(mid_f) * gm_ref[...]).astype(BF16)
        nm_s[rows, :] = normed_m
        for part in range(FFN // D):
            cols = slice(part * D, (part + 1) * D)
            pre = dot_nn(normed_m, wup[:, cols])
            cdf = 0.5 + 0.5 * lax.erf(pre * (0.5 ** 0.5))
            gelu_s[rows, cols] = (pre * cdf).astype(BF16)
            gp_s[part_rows(mb, part), :] = cdf + pre * (jnp.exp(pre * pre * -0.5) * 0.3989422804014327)
        top = mid_f + dot_nn(gelu_s[rows, :], wdown[...])
        for seq in range(SEQ_MB):
            mask = valid_mask(jnp.where(pos == last, lens_of(mb, seq), SEQ))
            piece = top[seq * SEQ:(seq + 1) * SEQ, :].astype(BF16)
            hout[seq_rows(seq), :] = jnp.where(mask > 0.0, piece.astype(F32), 0.0).astype(BF16)

        h_view = hout.at[rows]

        @pl.when(pos < last)
        def _():
            pltpu.make_async_remote_copy(src_ref=h_view, dst_ref=xin.at[rows], send_sem=send_sem.at[mb],
                                         recv_sem=x_sem.at[mb], device_id={'pipe': pos + 1}, device_id_type=MESH).start()

        @pl.when(pos == last)
        def _():
            half = mb % mb_home
            place(h_view, out_ref.at[pl.ds(pl.multiple_of(half * ROWS, 64), ROWS)], send_sem.at[mb], home_sem.at[half],
                  mb // mb_home)

        return 0

    for w_copy in w_copies:
        w_copy.wait()
    lax.fori_loop(0, n_mb, forward, 0)

    def forward_sent(mb, _):
        h_view = hout.at[rows_of(mb)]

        @pl.when(pos < last)
        def _():
            pltpu.make_async_copy(h_view, h_view, send_sem.at[mb]).wait()

        @pl.when(pos == last)
        def _():
            place_done(h_view, send_sem.at[mb], mb // mb_home)

        return 0

    lax.fori_loop(0, n_mb, forward_sent, 0)
    for half in range(mb_home):
        o_view = out_ref.at[pl.ds(half * ROWS, ROWS)]
        pltpu.make_async_copy(o_view, o_view, home_sem.at[half]).wait()

    gain_acc[...] = jnp.zeros_like(gain_acc)

    def norm_back(hid, gain, d_normed):
        inv = inv_rms(hid)
        unit = hid * inv
        d_gain = jnp.sum((d_normed * unit).reshape(ROWS // 8, 8, D), axis=0)
        scaled = d_normed * gain
        return inv * (scaled - unit * jnp.mean(unit * scaled, axis=-1, keepdims=True)), d_gain

    def backward(mb, _):
        rows = rows_of(mb)
        c_view = cin.at[rows]
        pltpu.make_async_copy(c_view, c_view, c_sem.at[mb]).wait()

        def seq_rows(seq):
            return pl.ds(pl.multiple_of(mb * ROWS + seq * SEQ, 64), SEQ)

        for seq in range(SEQ_MB):
            mask = valid_mask(lens_of(mb, seq))
            cin[seq_rows(seq), :] = jnp.where(mask > 0.0, cin[seq_rows(seq), :].astype(F32), 0.0).astype(BF16)
        d_top = cin[rows, :]
        for part in range(FFN // D):
            cols = slice(part * D, (part + 1) * D)
            d_gelu = dot_nt(d_top, wdown[cols, :])
            dpre_s[rows, cols] = (d_gelu * gp_s[part_rows(mb, part), :]).astype(BF16)
        d_nm = dot_nt(dpre_s[rows, :], wup[...])
        d_add, d_gain = norm_back(mid_s[rows, :].astype(F32), gm_ref[...], d_nm)
        gain_acc[1] += d_gain
        d_mid = d_top.astype(F32) + d_add
        d_mid_bf = d_mid.astype(BF16)
        dmid_s[rows, :] = d_mid_bf
        d_ctx = dot_nt(d_mid_bf, wout[...]).astype(BF16)
        for seq in range(SEQ_MB):
            for pair in range(PAIRS):
                v_cols = qkv_s[seq_rows(seq), 2 * D + pair * 128:2 * D + (pair + 1) * 128]
                dc = d_ctx[seq * SEQ:(seq + 1) * SEQ, pair * 128:(pair + 1) * 128]
                spot = (seq * PAIRS + pair) * SEQ
                p_rows = pl.ds(pl.multiple_of(mb * UNIT + spot, 64), SEQ)
                s_scr[spot:spot + SEQ, :] = dot_nt(dc, blocks(v_cols))
                both = dot_tn(p_s[p_rows, :].astype(BF16), dc)
                qkv_s[seq_rows(seq), 2 * D + pair * 128:2 * D + (pair + 1) * 128] = jnp.where(
                    first, both[:SEQ], both[SEQ:]).astype(BF16)
        for seq in range(SEQ_MB):
            spot = seq * PAIRS * SEQ
            p_rows = pl.ds(pl.multiple_of(mb * UNIT + spot, 64), PAIRS * SEQ)
            probs = p_s[p_rows, :].reshape(PAIRS, SEQ, 128)
            d_probs = s_scr[spot:spot + PAIRS * SEQ, :].reshape(PAIRS, SEQ, 128)
            sum_a, sum_b = halves_sum(probs * d_probs)
            d_scores = probs * (d_probs - jnp.where(first[None], sum_a, sum_b)) * (HEAD ** -0.5)
            s_scr[spot:spot + PAIRS * SEQ, :] = d_scores.reshape(PAIRS * SEQ, 128)
        for seq in range(SEQ_MB):
            for pair in range(PAIRS):
                q_at = slice(pair * 128, (pair + 1) * 128)
                k_at = slice(D + pair * 128, D + (pair + 1) * 128)
                q_cols = qkv_s[seq_rows(seq), q_at]
                k_cols = qkv_s[seq_rows(seq), k_at]
                spot = (seq * PAIRS + pair) * SEQ
                d_sc = s_scr[spot:spot + SEQ, :].astype(BF16)
                both = dot_tn(d_sc, q_cols)
                qkv_s[seq_rows(seq), q_at] = dot_nn(d_sc, blocks(k_cols)).astype(BF16)
                qkv_s[seq_rows(seq), k_at] = jnp.where(first, both[:SEQ], both[SEQ:]).astype(BF16)
        d_na = dot_nt(qkv_s[rows, :], wqkv[...])
        d_add, d_gain = norm_back(xin[rows, :].astype(F32), ga_ref[...], d_na)
        gain_acc[0] += d_gain

        @pl.when(pos > 0)
        def _():
            hout[rows, :] = (d_mid + d_add).astype(BF16)
            pltpu.make_async_remote_copy(src_ref=hout.at[rows], dst_ref=cin.at[rows], send_sem=send_sem.at[mb],
                                         recv_sem=c_sem.at[mb], device_id={'pipe': pos - 1}, device_id_type=MESH).start()

        return 0

    lax.fori_loop(0, n_mb, backward, 0)

    gain_all[rep] = jnp.concatenate([jnp.sum(gain_acc[0], axis=0, keepdims=True), jnp.sum(gain_acc[1], axis=0, keepdims=True),
                                     jnp.zeros((6, D), F32)], axis=0)
    for step in range(1, DATA):
        pltpu.make_async_remote_copy(src_ref=gain_all.at[rep], dst_ref=gain_all.at[rep], send_sem=gain_send,
                                     recv_sem=gain_recv.at[rep], device_id={'data': (rep + step) % DATA},
                                     device_id_type=MESH).start()

    n_down, n_up, n_qkv = FFN // TILE, (D // TILE) * (FFN // D), (D // TILE) * 3

    def tile_kinds(tile):
        up, qkv, out = tile - n_down, tile - n_down - n_up, tile - n_down - n_up - n_qkv
        return (
            (tile < n_down, gelu_s, cin, gdown_ref, tile, 0),
            ((up >= 0) & (qkv < 0), nm_s, dpre_s, gup_ref, up // (FFN // D), up % (FFN // D)),
            ((qkv >= 0) & (out < 0), na_s, qkv_s, gqkv_ref, qkv // 3, qkv % 3),
            (out >= 0, ctx_s, dmid_s, gout_ref, out, 0),
        )

    def tile_at(tile):
        return pl.ds(pl.multiple_of(tile * TILE, TILE), TILE)

    def compute_tile(tile):
        for cond, lhs, rhs, _, at_row, at_col in tile_kinds(tile):
            @pl.when(cond)
            def _(lhs=lhs, rhs=rhs, at_row=at_row, at_col=at_col):
                cols = pl.ds(0, D) if rhs.shape[1] == D else pl.ds(pl.multiple_of(at_col * D, D), D)
                gp_s[tile_at(tile), :] = dot_tn(lhs[:, pl.ds(pl.multiple_of(at_row * TILE, TILE), TILE)], rhs[:, cols])

    def put_tile(tile):
        for cond, _, rhs, dst, at_row, at_col in tile_kinds(tile):
            @pl.when(cond)
            def _(rhs=rhs, dst=dst, at_row=at_row, at_col=at_col):
                cols = pl.ds(0, D) if rhs.shape[1] == D else pl.ds(pl.multiple_of(at_col * D, D), D)
                dst_view = dst.at[pl.ds(pl.multiple_of(at_row * TILE, TILE), TILE), cols]
                pltpu.make_async_copy(gp_s.at[tile_at(tile)], dst_view, put_sem).start()

    to_y, to_right, to_left = rep + 1 - 2 * rep_y, rep + 2, rep - 2

    def part_done(src, colour, link, slot):
        pltpu.make_async_copy(src, src, part_send.at[colour, link, slot]).wait()

    def ship_part(unit, slot, src, dst, colour, link, target, value):
        @pl.when(unit >= SLOTS)
        def _():
            part_done(src, colour, link, slot)

        src[...] = value
        pltpu.make_async_remote_copy(src_ref=src, dst_ref=dst, send_sem=part_send.at[colour, link, slot],
                                     recv_sem=sum_recv.at[colour, link, slot], device_id={'data': target},
                                     device_id_type=MESH).start()

    def ship(src, dst, link, recv, target):
        pltpu.make_async_remote_copy(src_ref=src, dst_ref=dst, send_sem=sum_send.at[link], recv_sem=recv,
                                     device_id={'data': target}, device_id_type=MESH).start()

    def arrived(view, recv):
        pltpu.make_async_copy(view, view, recv).wait()

    def gp_rows(start, size):
        return pl.ds(pl.multiple_of(start, 8), size)

    def line_actions(zz, colour, block, size, buf_l, buf_r, out_l, out_r, hop_rs, hop_ag):
        chunk = size // LINE
        own, above = zz * chunk, (zz + 1) * chunk

        def rs_right(unit, slot):
            at = block(unit)
            if zz > 0:
                arrived(buf_l.at[slot, own:size], sum_recv.at[colour, 1, slot])
                gp_s[gp_rows(at + own, chunk), :] += buf_l[slot, own:above, :]
            if zz < LINE - 1:
                value = gp_s[gp_rows(at + above, size - above), :]
                if zz > 0:
                    value = value + buf_l[slot, above:size, :]
                ship_part(unit, slot, out_r.at[slot, above:size], buf_l.at[slot, above:size], colour, 1, to_right, value)

        def rs_left(unit, slot):
            at = block(unit)
            if zz < LINE - 1:
                arrived(buf_r.at[slot, 0:above], sum_recv.at[colour, 2, slot])
                gp_s[gp_rows(at + own, chunk), :] += buf_r[slot, own:above, :]
            if zz > 0:
                value = gp_s[gp_rows(at, own), :]
                if zz < LINE - 1:
                    value = value + buf_r[slot, 0:own, :]
                ship_part(unit, slot, out_l.at[slot, 0:own], buf_r.at[slot, 0:own], colour, 2, to_left, value)

        def ag_right(unit, slot):
            at = block(unit)
            if zz > 0:
                arrived(gp_s.at[gp_rows(at, own)], sum_recv.at[colour, 3, slot])
            if zz < LINE - 1:
                view = gp_s.at[gp_rows(at, above)]
                ship(view, view, 1, sum_recv.at[colour, 3, slot], to_right)

        def ag_left(unit, slot):
            at = block(unit)
            if zz < LINE - 1:
                arrived(gp_s.at[gp_rows(at + above, size - above)], sum_recv.at[colour, 4, slot])
            if zz > 0:
                view = gp_s.at[gp_rows(at + own, size - own)]
                ship(view, view, 2, sum_recv.at[colour, 4, slot], to_left)

        return ([(hop_rs + zz, rs_right), (hop_rs + LINE - 1 - zz, rs_left)],
                [(hop_ag + zz, ag_right), (hop_ag + LINE - 1 - zz, ag_left)])

    half_a, part_b = TILE // 2, TILE // LINE
    half_b = part_b // 2

    def actions_a(zz):
        def mine(unit):
            return unit * TILE + rep_y * half_a

        def theirs(unit):
            return unit * TILE + (1 - rep_y) * half_a

        def y_send(unit, slot):
            ship_part(unit, slot, ya_out.at[slot], ya_buf.at[slot], 0, 0, to_y, gp_s[gp_rows(theirs(unit), half_a), :])

        def y_add(unit, slot):
            arrived(ya_buf.at[slot], sum_recv.at[0, 0, slot])
            gp_s[gp_rows(mine(unit), half_a), :] += ya_buf[slot]

        def y_give(unit, slot):
            view = gp_s.at[gp_rows(mine(unit), half_a)]
            ship(view, view, 0, sum_recv.at[0, 5, slot], to_y)

        def finish(unit, slot):
            arrived(gp_s.at[gp_rows(theirs(unit), half_a)], sum_recv.at[0, 5, slot])
            put_tile(unit)

        scatter, gather = line_actions(zz, 0, mine, half_a, la_buf, ra_buf, la_out, ra_out, 1, 4)
        return [(0, y_send), (1, y_add)] + scatter + gather + [(7, y_give), (8, finish)]

    def actions_b(zz):
        def block(unit):
            return (UNITS_A + unit) * TILE

        def mine(unit):
            return block(unit) + zz * part_b + rep_y * half_b

        def theirs(unit):
            return block(unit) + zz * part_b + (1 - rep_y) * half_b

        def y_send(unit, slot):
            ship_part(unit, slot, yb_out.at[slot], yb_buf.at[slot], 1, 0, to_y, gp_s[gp_rows(theirs(unit), half_b), :])

        def y_add(unit, slot):
            arrived(yb_buf.at[slot], sum_recv.at[1, 0, slot])
            gp_s[gp_rows(mine(unit), half_b), :] += yb_buf[slot]
            view = gp_s.at[gp_rows(mine(unit), half_b)]
            ship(view, view, 0, sum_recv.at[1, 5, slot], to_y)

        def y_done(unit, slot):
            arrived(gp_s.at[gp_rows(theirs(unit), half_b)], sum_recv.at[1, 5, slot])

        def finish(unit, slot):
            put_tile(UNITS_A + unit)

        scatter, gather = line_actions(zz, 1, block, TILE, lb_buf, rb_buf, lb_out, rb_out, 0, 5)
        return scatter + [(3, y_send), (4, y_add), (5, y_done)] + gather + [(8, finish)]

    def b_unit(tick):
        unit = tick * UNITS_B // UNITS_A
        fresh = (tick >= 0) & (tick < UNITS_A) & ((tick + 1) * UNITS_B // UNITS_A > unit)
        return fresh, unit

    def run_actions(tick, hops):
        for zz in range(LINE):
            @pl.when(rep_z == zz)
            def _(zz=zz):
                todo = [(hop, 0, fn) for hop, fn in actions_a(zz)] + [(hop, 1, fn) for hop, fn in actions_b(zz)]
                for want in hops:
                    for colour in range(2):
                        fns = [fn for hop, col, fn in todo if hop == want and col == colour]
                        if not fns:
                            continue
                        start = tick - want
                        if colour == 0:
                            fresh, unit = (start >= 0) & (start < UNITS_A), start
                        else:
                            fresh, unit = b_unit(start)

                        @pl.when(fresh)
                        def _(fns=fns, unit=unit):
                            for fn in fns:
                                fn(unit, unit % SLOTS)

    def compute_for(tick):
        @pl.when(tick < UNITS_A)
        def _():
            compute_tile(tick)

        fresh, unit = b_unit(tick)

        @pl.when(fresh)
        def _():
            compute_tile(UNITS_A + unit)

    compute_for(0)

    def tick_step(tick, _):
        run_actions(tick, [0])
        compute_for(tick + 1)
        run_actions(tick, range(1, 9))
        return 0

    lax.fori_loop(0, UNITS_A + 8, tick_step, 0)

    def sent_all(link, size):
        view = gp_s.at[pl.ds(0, size)]
        pltpu.make_async_copy(view, view, sum_send.at[link]).wait()

    for zz in range(LINE):
        @pl.when(rep_z == zz)
        def _(zz=zz):
            line_rows = UNITS_A * (half_a // LINE) + UNITS_B * part_b
            sent_all(0, UNITS_A * half_a + UNITS_B * half_b)
            if zz < LINE - 1:
                sent_all(1, line_rows * (zz + 1))
            if zz > 0:
                sent_all(2, line_rows * (LINE - zz))
            for slot in range(SLOTS):
                for colour, (out_y, out_l, out_r) in enumerate(((ya_out, la_out, ra_out), (yb_out, lb_out, rb_out))):
                    size = out_l.shape[1]
                    part_done(out_y.at[slot], colour, 0, slot)
                    if zz < LINE - 1:
                        part_done(out_r.at[slot, (zz + 1) * size // LINE:size], colour, 1, slot)
                    if zz > 0:
                        part_done(out_l.at[slot, 0:zz * size // LINE], colour, 2, slot)

    pltpu.make_async_copy(gp_s, gp_s, put_sem).wait()

    for step in range(1, DATA):
        peer = (rep + step) % DATA
        pltpu.make_async_copy(gain_all.at[peer], gain_all.at[peer], gain_recv.at[peer]).wait()
    total = gain_all[0]
    for peer in range(1, DATA):
        total = total + gain_all[peer]
    gain_ref[...] = total
    pltpu.make_async_copy(gain_all.at[pl.ds(0, DATA - 1)], gain_all.at[pl.ds(0, DATA - 1)], gain_send).wait()

    def backward_sent(mb, _):
        @pl.when(pos > 0)
        def _():
            h_view = hout.at[rows_of(mb)]
            pltpu.make_async_copy(h_view, h_view, send_sem.at[mb]).wait()

        return 0

    lax.fori_loop(0, n_mb, backward_sent, 0)
    for src, _, send, _, target in spread:
        place_done(src, send, target)


def run_pass(acts, cots, lens_tile, w_qkv, w_out, w_up, w_down, gain_a, gain_m):
    n_tok = acts.shape[0] * PIPE
    n_mb = n_tok // ROWS
    any_spec = pl.BlockSpec(memory_space=pl.ANY)
    vmem_spec = pl.BlockSpec(memory_space=pltpu.VMEM)
    dma = pltpu.SemaphoreType.DMA
    return pl.pallas_call(
        functools.partial(pass_kernel, n_mb),
        out_shape=(
            jax.ShapeDtypeStruct(acts.shape, BF16),
            jax.ShapeDtypeStruct((D, 3 * D), F32),
            jax.ShapeDtypeStruct((D, D), F32),
            jax.ShapeDtypeStruct((D, FFN), F32),
            jax.ShapeDtypeStruct((FFN, D), F32),
            jax.ShapeDtypeStruct((8, D), F32),
        ),
        in_specs=[any_spec] * 7 + [vmem_spec] * 2,
        out_specs=[any_spec] * 5 + [vmem_spec],
        scratch_shapes=[
            pltpu.VMEM((D, 3 * D), BF16),
            pltpu.VMEM((D, D), BF16),
            pltpu.VMEM((D, FFN), BF16),
            pltpu.VMEM((FFN, D), BF16),
            pltpu.VMEM((n_mb * SEQ_MB, 8, 128), jnp.int32),
            pltpu.VMEM((n_tok, D), BF16),
            pltpu.VMEM((n_tok, D), BF16),
            pltpu.VMEM((n_tok, D), BF16),
            pltpu.VMEM((n_tok, D), BF16),
            pltpu.VMEM((n_tok, 3 * D), BF16),
            pltpu.VMEM((n_tok, D), BF16),
            pltpu.VMEM((n_tok, D), BF16),
            pltpu.VMEM((n_tok, D), BF16),
            pltpu.VMEM((n_tok, FFN), BF16),
            pltpu.VMEM((n_tok * FFN // D, D), F32),
            pltpu.VMEM((n_tok, FFN), BF16),
            pltpu.VMEM((n_tok, D), BF16),
            pltpu.VMEM((n_mb * UNIT, 128), F32),
            pltpu.VMEM((UNIT, 128), F32),
            pltpu.VMEM((2, 8, D), F32),
            pltpu.VMEM((DATA, 8, D), F32),
        ] + [
            pltpu.VMEM((SLOTS, size, D), F32)
            for size in (TILE // 2, TILE // 2, TILE // 2, TILE // LINE // 2, TILE, TILE) * 2
        ] + [
            dma((4,)),
            dma((2 * (n_mb // PIPE) + PIPE,)),
            dma((n_mb,)),
            dma((n_mb,)),
            dma((PIPE,)),
            dma((n_mb,)),
            dma((n_mb // PIPE,)),
            dma((2, 6, SLOTS)),
            dma((3,)),
            dma((2, 3, SLOTS)),
            dma((DATA,)),
            dma,
            dma,
        ],
        compiler_params=pltpu.CompilerParams(collective_id=0, has_side_effects=True, vmem_limit_bytes=64 * 1024 * 1024 - 131072),
    )(acts, cots, lens_tile, w_qkv, w_out, w_up, w_down, gain_a, gain_m)


def solution(mesh):
    row_spec = P(('data', 'pipe'))
    stage_spec = P('pipe')

    def device_pass(acts_in, cot_out, seq_lens, w_qkv, w_out, w_up, w_down, gain_attn, gain_mlp):
        lens_tile = jnp.broadcast_to(seq_lens[:, None, None], (seq_lens.shape[0], 8, 128))
        outs = run_pass(acts_in.reshape(-1, D), cot_out.reshape(-1, D), lens_tile, w_qkv.reshape(D, 3 * D),
                        w_out.reshape(D, D), w_up.reshape(D, FFN), w_down.reshape(FFN, D),
                        gain_attn.astype(F32), gain_mlp.astype(F32))
        acts_out, g_qkv, g_out, g_up, g_down, g_gain = outs
        grads = (g_qkv.reshape(w_qkv.shape), g_out.reshape(w_out.shape), g_up.reshape(w_up.shape), g_down.reshape(w_down.shape),
                 g_gain[0:1], g_gain[1:2])
        return (acts_out.reshape(acts_in.shape),) + grads

    return jax.shard_map(device_pass, mesh=mesh, in_specs=(row_spec, row_spec, row_spec) + (stage_spec,) * 6, out_specs=(row_spec,) + (stage_spec,) * 6, check_vma=False)
```

```python
import functools
import jax
import jax.numpy as jnp
from jax import lax
from jax.experimental import pallas as pl
from jax.experimental.pallas import tpu as pltpu
from jax.sharding import PartitionSpec as P

NORM_EPS = 1e-5
MESH = pl.DeviceIdType.MESH
F32 = jnp.float32
BF16 = jnp.bfloat16
SEQ = 64
HEAD = 64
D = 512
FFN = 2048
PIPE = 4
DATA = 8
LINE = 4
TILE = 128
PART = 64
UNITS_A = 56
UNITS_B = 40
SLOTS = 4
SEQ_MB = 3
PAIRS = 4


def dot_nn(lhs, rhs):
    return lax.dot_general(lhs, rhs, (((1,), (0,)), ((), ())), preferred_element_type=F32)


def dot_nt(lhs, rhs):
    return lax.dot_general(lhs, rhs, (((1,), (1,)), ((), ())), preferred_element_type=F32)


def dot_tn(lhs, rhs):
    return lax.dot_general(lhs, rhs, (((0,), (0,)), ((), ())), preferred_element_type=F32)


def pass_kernel(n_seq, acts_ref, cot_ref, lens_ref, wqkv_hbm, wout_hbm, wup_hbm, wdown_hbm, ga_ref, gm_ref,
                out_ref, gqkv_ref, gout_ref, gup_ref, gdown_ref, gain_ref,
                wqkv, wout, wup, wdown, lens_buf, xin, cin, hout, na_s, qkv_s, ctx_s, mid_s, nm_s, gelu_s, gp_s,
                dpre_s, dmid_s, p_s, s_scr, gain_acc, gain_all, ya_buf, la_buf, ra_buf, yb_buf, lb_buf, rb_buf,
                ya_out, la_out, ra_out, yb_out, lb_out, rb_out,
                w_sem, in_sem, x_sem, c_sem, len_sem, send_sem, home_sem, sum_recv, sum_send, part_send, gain_recv, gain_send, put_sem):
    pos = lax.axis_index('pipe')
    rep = lax.axis_index('data')
    rep_z, rep_y = rep // 2, rep % 2
    n_tok = n_seq * SEQ
    n_mb = n_seq // SEQ_MB + SEQ_MB - 1
    n_own = n_seq // PIPE
    own_slab = pl.ds(pos * n_own, n_own)
    for seq in range(n_own):
        lens_buf[pos * n_own + seq] = jnp.full((8, 128), lens_ref[seq], jnp.int32)
    last = PIPE - 1

    w_copies = [pltpu.make_async_copy(src, dst, w_sem.at[idx]) for idx, (src, dst) in enumerate(
        ((wqkv_hbm, wqkv), (wout_hbm, wout), (wup_hbm, wup), (wdown_hbm, wdown)))]
    for w_copy in w_copies:
        w_copy.start()

    barrier = pltpu.get_barrier_semaphore()
    for step in range(1, PIPE):
        pl.semaphore_signal(barrier, inc=1, device_id={'pipe': (pos + step) % PIPE}, device_id_type=MESH)
    for step in range(1, DATA):
        pl.semaphore_signal(barrier, inc=1, device_id={'data': (rep + step) % DATA}, device_id_type=MESH)
    pl.semaphore_wait(barrier, PIPE - 1 + DATA - 1)

    def first_seq(mb, size):
        return mb if size == 1 else (mb - SEQ_MB + 1) * SEQ_MB

    def rows_of(mb, size):
        return pl.ds(pl.multiple_of(first_seq(mb, size) * SEQ, SEQ), size * SEQ)

    def seq_rows(mb, size, seq):
        return pl.ds(pl.multiple_of((first_seq(mb, size) + seq) * SEQ, SEQ), SEQ)

    def part_rows(mb, size, part):
        return pl.ds(pl.multiple_of(part * n_tok + first_seq(mb, size) * SEQ, SEQ), size * SEQ)

    def send_to(src, dst, send, recv, target):
        pltpu.make_async_remote_copy(src_ref=src, dst_ref=dst, send_sem=send, recv_sem=recv,
                                     device_id={'pipe': target}, device_id_type=MESH).start()

    def place(src, dst, send, recv, target):
        @pl.when(target == pos)
        def _():
            pltpu.make_async_copy(src, dst, recv).start()

        @pl.when(target != pos)
        def _():
            send_to(src, dst, send, recv, target)

    for step in range(1, PIPE):
        send_to(lens_buf.at[own_slab], lens_buf.at[own_slab], in_sem.at[step - 1], len_sem.at[pos], (pos + step) % PIPE)
    spread = []
    for src, dst, sem, target in ((acts_ref, xin, x_sem, 0), (cot_ref, cin, c_sem, last)):
        for seq in range(n_own):
            at = pos * n_own + seq
            mb = jnp.where(at < SEQ_MB, at, at // SEQ_MB + SEQ_MB - 1)
            spread.append((src.at[pl.ds(seq * SEQ, SEQ)], dst.at[pl.ds(pl.multiple_of(at * SEQ, SEQ), SEQ)],
                           in_sem.at[PIPE - 1 + len(spread)], sem.at[mb], target))
    for item in spread:
        place(*item)

    lane = lax.broadcasted_iota(jnp.int32, (SEQ, 128), 1)
    row = lax.broadcasted_iota(jnp.int32, (SEQ, 128), 0)
    first = lane < HEAD
    key_pos = jnp.where(first, lane, lane - HEAD)
    lane_row = lax.broadcasted_iota(jnp.int32, (1, 128), 1)
    take_a = jnp.where(lane_row < HEAD, 1.0, 0.0).astype(BF16)
    take_b = jnp.where(lane_row < HEAD, 0.0, 1.0).astype(BF16)

    def blocks(pair_cols):
        return jnp.concatenate([pair_cols * take_a, pair_cols * take_b], axis=0)

    def halves_sum(arr):
        sum_a = jnp.sum(jnp.where(first[None], arr, 0.0), axis=-1, keepdims=True)
        sum_b = jnp.sum(jnp.where(first[None], 0.0, arr), axis=-1, keepdims=True)
        return sum_a, sum_b

    def lens_of(mb, size, seq):
        return lens_buf[first_seq(mb, size) + seq][0:1, :]

    def valid_mask(lens_row):
        ok = jnp.where(row < lens_row, 1.0, 0.0)
        return jnp.concatenate([ok] * (D // 128), axis=1)

    def inv_rms(val):
        return lax.rsqrt(jnp.mean(val * val, axis=-1, keepdims=True) + NORM_EPS)

    def forward(size, mb, _):
        rows = rows_of(mb, size)
        start = first_seq(mb, size)

        @pl.when((start % n_own == 0) & (start // n_own != pos))
        def _():
            slab = lens_buf.at[pl.ds(start, n_own)]
            pltpu.make_async_copy(slab, slab, len_sem.at[start // n_own]).wait()

        x_view = xin.at[rows]
        pltpu.make_async_copy(x_view, x_view, x_sem.at[mb]).wait()
        gain_a = ga_ref[...].astype(F32)
        hid = xin[rows, :].astype(F32)
        normed = (hid * inv_rms(hid) * gain_a).astype(BF16)
        na_s[rows, :] = normed
        for part in range(3):
            cols = slice(part * D, (part + 1) * D)
            qkv_s[rows, cols] = dot_nn(normed, wqkv[:, cols]).astype(BF16)

        for seq in range(size):
            for pair in range(PAIRS):
                q_cols = qkv_s[seq_rows(mb, size, seq), pair * 128:(pair + 1) * 128]
                k_cols = qkv_s[seq_rows(mb, size, seq), D + pair * 128:D + (pair + 1) * 128]
                spot = (seq * PAIRS + pair) * SEQ
                s_scr[spot:spot + SEQ, :] = dot_nt(q_cols, blocks(k_cols))
        for seq in range(size):
            visible = (key_pos <= row) & (key_pos < lens_of(mb, size, seq))
            spot = seq * PAIRS * SEQ
            scores = s_scr[spot:spot + PAIRS * SEQ, :].reshape(PAIRS, SEQ, 128) * (HEAD ** -0.5)
            scores = jnp.where(visible[None], scores, -1e30)
            max_a = jnp.max(jnp.where(first[None], scores, -3e38), axis=-1, keepdims=True)
            max_b = jnp.max(jnp.where(first[None], -3e38, scores), axis=-1, keepdims=True)
            expd = jnp.exp(scores - jnp.where(first[None], max_a, max_b))
            sum_a, sum_b = halves_sum(expd)
            probs = expd * jnp.where(first[None], 1.0 / sum_a, 1.0 / sum_b)
            p_rows = pl.ds(pl.multiple_of(start * PAIRS * SEQ + spot, SEQ), PAIRS * SEQ)
            p_s[p_rows, :] = probs.reshape(PAIRS * SEQ, 128)
        for seq in range(size):
            for pair in range(PAIRS):
                v_cols = qkv_s[seq_rows(mb, size, seq), 2 * D + pair * 128:2 * D + (pair + 1) * 128]
                p_rows = pl.ds(pl.multiple_of((start * PAIRS + seq * PAIRS + pair) * SEQ, SEQ), SEQ)
                ctx_s[seq_rows(mb, size, seq), pair * 128:(pair + 1) * 128] = dot_nn(
                    p_s[p_rows, :].astype(BF16), blocks(v_cols)).astype(BF16)
        mid = (hid + dot_nn(ctx_s[rows, :], wout[...])).astype(BF16)
        mid_s[rows, :] = mid
        mid_f = mid.astype(F32)
        normed_m = (mid_f * inv_rms(mid_f) * gm_ref[...].astype(F32)).astype(BF16)
        nm_s[rows, :] = normed_m
        for part in range(FFN // D):
            cols = slice(part * D, (part + 1) * D)
            pre = dot_nn(normed_m, wup[:, cols])
            cdf = 0.5 + 0.5 * lax.erf(pre * (0.5 ** 0.5))
            gelu_s[rows, cols] = (pre * cdf).astype(BF16)
            gp_s[part_rows(mb, size, part), :] = cdf + pre * (jnp.exp(pre * pre * -0.5) * 0.3989422804014327)
        top = mid_f + dot_nn(gelu_s[rows, :], wdown[...])
        for seq in range(size):
            mask = valid_mask(jnp.where(pos == last, lens_of(mb, size, seq), SEQ))
            piece = top[seq * SEQ:(seq + 1) * SEQ, :].astype(BF16)
            hout[seq_rows(mb, size, seq), :] = jnp.where(mask > 0.0, piece.astype(F32), 0.0).astype(BF16)

        h_view = hout.at[rows]

        @pl.when(pos < last)
        def _():
            send_to(h_view, xin.at[rows], send_sem.at[mb], x_sem.at[mb], pos + 1)

        @pl.when(pos == last)
        def _():
            home = start // n_own
            o_view = out_ref.at[pl.ds(pl.multiple_of((start % n_own) * SEQ, SEQ), size * SEQ)]

            @pl.when(home == pos)
            def _():
                pltpu.make_async_copy(h_view, o_view, send_sem.at[mb]).start()

            @pl.when(home != pos)
            def _():
                send_to(h_view, o_view, send_sem.at[mb], home_sem, home)

        return 0

    for w_copy in w_copies:
        w_copy.wait()
    lax.fori_loop(0, SEQ_MB, functools.partial(forward, 1), 0)
    lax.fori_loop(SEQ_MB, n_mb, functools.partial(forward, SEQ_MB), 0)

    def sent(size, mb, _):
        h_view = hout.at[rows_of(mb, size)]
        pltpu.make_async_copy(h_view, h_view, send_sem.at[mb]).wait()
        return 0

    gain_acc[...] = jnp.zeros_like(gain_acc)

    def norm_back(hid, gain, d_normed):
        inv = inv_rms(hid)
        unit = hid * inv
        d_gain = jnp.sum((d_normed * unit).reshape(hid.shape[0] // 8, 8, D), axis=0)
        scaled = d_normed * gain
        return inv * (scaled - unit * jnp.mean(unit * scaled, axis=-1, keepdims=True)), d_gain

    def backward(size, mb, _):
        rows = rows_of(mb, size)
        start = first_seq(mb, size)
        c_view = cin.at[rows]
        pltpu.make_async_copy(c_view, c_view, c_sem.at[mb]).wait()

        for seq in range(size):
            mask = valid_mask(lens_of(mb, size, seq))
            cin[seq_rows(mb, size, seq), :] = jnp.where(mask > 0.0, cin[seq_rows(mb, size, seq), :].astype(F32), 0.0).astype(BF16)
        d_top = cin[rows, :]
        for part in range(FFN // D):
            cols = slice(part * D, (part + 1) * D)
            d_gelu = dot_nt(d_top, wdown[cols, :])
            dpre_s[rows, cols] = (d_gelu * gp_s[part_rows(mb, size, part), :]).astype(BF16)
        d_nm = dot_nt(dpre_s[rows, :], wup[...])
        d_add, d_gain = norm_back(mid_s[rows, :].astype(F32), gm_ref[...].astype(F32), d_nm)
        gain_acc[1] += d_gain
        d_mid = d_top.astype(F32) + d_add
        d_mid_bf = d_mid.astype(BF16)
        dmid_s[rows, :] = d_mid_bf
        d_ctx = dot_nt(d_mid_bf, wout[...]).astype(BF16)
        for seq in range(size):
            for pair in range(PAIRS):
                v_cols = qkv_s[seq_rows(mb, size, seq), 2 * D + pair * 128:2 * D + (pair + 1) * 128]
                dc = d_ctx[seq * SEQ:(seq + 1) * SEQ, pair * 128:(pair + 1) * 128]
                spot = (seq * PAIRS + pair) * SEQ
                p_rows = pl.ds(pl.multiple_of(start * PAIRS * SEQ + spot, SEQ), SEQ)
                s_scr[spot:spot + SEQ, :] = dot_nt(dc, blocks(v_cols))
                both = dot_tn(p_s[p_rows, :].astype(BF16), dc)
                qkv_s[seq_rows(mb, size, seq), 2 * D + pair * 128:2 * D + (pair + 1) * 128] = jnp.where(
                    first, both[:SEQ], both[SEQ:]).astype(BF16)
        for seq in range(size):
            spot = seq * PAIRS * SEQ
            p_rows = pl.ds(pl.multiple_of(start * PAIRS * SEQ + spot, SEQ), PAIRS * SEQ)
            probs = p_s[p_rows, :].reshape(PAIRS, SEQ, 128)
            d_probs = s_scr[spot:spot + PAIRS * SEQ, :].reshape(PAIRS, SEQ, 128)
            sum_a, sum_b = halves_sum(probs * d_probs)
            d_scores = probs * (d_probs - jnp.where(first[None], sum_a, sum_b)) * (HEAD ** -0.5)
            s_scr[spot:spot + PAIRS * SEQ, :] = d_scores.reshape(PAIRS * SEQ, 128)
        for seq in range(size):
            for pair in range(PAIRS):
                q_at = slice(pair * 128, (pair + 1) * 128)
                k_at = slice(D + pair * 128, D + (pair + 1) * 128)
                q_cols = qkv_s[seq_rows(mb, size, seq), q_at]
                k_cols = qkv_s[seq_rows(mb, size, seq), k_at]
                spot = (seq * PAIRS + pair) * SEQ
                d_sc = s_scr[spot:spot + SEQ, :].astype(BF16)
                both = dot_tn(d_sc, q_cols)
                qkv_s[seq_rows(mb, size, seq), q_at] = dot_nn(d_sc, blocks(k_cols)).astype(BF16)
                qkv_s[seq_rows(mb, size, seq), k_at] = jnp.where(first, both[:SEQ], both[SEQ:]).astype(BF16)
        d_na = dot_nt(qkv_s[rows, :], wqkv[...])
        d_add, d_gain = norm_back(xin[rows, :].astype(F32), ga_ref[...].astype(F32), d_na)
        gain_acc[0] += d_gain

        @pl.when(pos > 0)
        def _():
            sent(size, mb, 0)
            hout[rows, :] = (d_mid + d_add).astype(BF16)
            send_to(hout.at[rows], cin.at[rows], send_sem.at[mb], c_sem.at[mb], pos - 1)

        return 0

    lax.fori_loop(SEQ_MB, n_mb, functools.partial(backward, SEQ_MB), 0)
    lax.fori_loop(0, SEQ_MB, functools.partial(backward, 1), 0)

    gain_all[rep] = jnp.concatenate([jnp.sum(gain_acc[0], axis=0, keepdims=True), jnp.sum(gain_acc[1], axis=0, keepdims=True),
                                     jnp.zeros((6, D), F32)], axis=0)
    for step in range(1, DATA):
        pltpu.make_async_remote_copy(src_ref=gain_all.at[rep], dst_ref=gain_all.at[rep], send_sem=gain_send,
                                     recv_sem=gain_recv.at[rep], device_id={'data': (rep + step) % DATA},
                                     device_id_type=MESH).start()

    per_tile = TILE // PART
    n_down, n_up, n_qkv = FFN // TILE, (D // TILE) * (FFN // D), (D // TILE) * 3

    def tile_kinds(tile):
        up, qkv, out = tile - n_down, tile - n_down - n_up, tile - n_down - n_up - n_qkv
        return (
            (tile < n_down, gelu_s, cin, gdown_ref, tile, 0),
            ((up >= 0) & (qkv < 0), nm_s, dpre_s, gup_ref, up // (FFN // D), up % (FFN // D)),
            ((qkv >= 0) & (out < 0), na_s, qkv_s, gqkv_ref, qkv // 3, qkv % 3),
            (out >= 0, ctx_s, dmid_s, gout_ref, out, 0),
        )

    def tile_at(tile):
        return pl.ds(pl.multiple_of(tile * TILE, TILE), TILE)

    def compute_tile(tile):
        for cond, lhs, rhs, _, at_row, at_col in tile_kinds(tile):
            @pl.when(cond)
            def _(lhs=lhs, rhs=rhs, at_row=at_row, at_col=at_col):
                cols = pl.ds(0, D) if rhs.shape[1] == D else pl.ds(pl.multiple_of(at_col * D, D), D)
                gp_s[tile_at(tile), :] = dot_tn(lhs[:, pl.ds(pl.multiple_of(at_row * TILE, TILE), TILE)], rhs[:, cols])

    def put_unit(unit):
        for cond, _, rhs, dst, at_row, at_col in tile_kinds(unit // per_tile):
            @pl.when(cond)
            def _(rhs=rhs, dst=dst, at_row=at_row, at_col=at_col):
                cols = pl.ds(0, D) if rhs.shape[1] == D else pl.ds(pl.multiple_of(at_col * D, D), D)
                dst_view = dst.at[pl.ds(pl.multiple_of(at_row * TILE + (unit % per_tile) * PART, PART), PART), cols]
                pltpu.make_async_copy(gp_s.at[gp_rows(unit * PART, PART)], dst_view, put_sem).start()

    to_y, to_right, to_left = rep + 1 - 2 * rep_y, rep + 2, rep - 2

    def part_done(src, colour, link, slot):
        pltpu.make_async_copy(src, src, part_send.at[colour, link, slot]).wait()

    def ship_part(unit, slot, src, dst, colour, link, target, value):
        @pl.when(unit >= SLOTS)
        def _():
            part_done(src, colour, link, slot)

        src[...] = value
        pltpu.make_async_remote_copy(src_ref=src, dst_ref=dst, send_sem=part_send.at[colour, link, slot],
                                     recv_sem=sum_recv.at[colour, link, slot], device_id={'data': target},
                                     device_id_type=MESH).start()

    def ship(src, dst, link, recv, target):
        pltpu.make_async_remote_copy(src_ref=src, dst_ref=dst, send_sem=sum_send.at[link], recv_sem=recv,
                                     device_id={'data': target}, device_id_type=MESH).start()

    def arrived(view, recv):
        pltpu.make_async_copy(view, view, recv).wait()

    def gp_rows(start, size):
        return pl.ds(pl.multiple_of(start, 8), size)

    def line_actions(zz, colour, block, size, buf_l, buf_r, out_l, out_r, hop_rs, hop_ag):
        chunk = size // LINE
        own, above = zz * chunk, (zz + 1) * chunk

        def rs_right(unit, slot):
            at = block(unit)
            if zz > 0:
                arrived(buf_l.at[slot, own:size], sum_recv.at[colour, 1, slot])
                gp_s[gp_rows(at + own, chunk), :] += buf_l[slot, own:above, :]
            if zz < LINE - 1:
                value = gp_s[gp_rows(at + above, size - above), :]
                if zz > 0:
                    value = value + buf_l[slot, above:size, :]
                ship_part(unit, slot, out_r.at[slot, above:size], buf_l.at[slot, above:size], colour, 1, to_right, value)

        def rs_left(unit, slot):
            at = block(unit)
            if zz < LINE - 1:
                arrived(buf_r.at[slot, 0:above], sum_recv.at[colour, 2, slot])
                gp_s[gp_rows(at + own, chunk), :] += buf_r[slot, own:above, :]
            if zz > 0:
                value = gp_s[gp_rows(at, own), :]
                if zz < LINE - 1:
                    value = value + buf_r[slot, 0:own, :]
                ship_part(unit, slot, out_l.at[slot, 0:own], buf_r.at[slot, 0:own], colour, 2, to_left, value)

        def ag_right(unit, slot):
            at = block(unit)
            if zz > 0:
                arrived(gp_s.at[gp_rows(at, own)], sum_recv.at[colour, 3, slot])
            if zz < LINE - 1:
                view = gp_s.at[gp_rows(at, above)]
                ship(view, view, 1, sum_recv.at[colour, 3, slot], to_right)

        def ag_left(unit, slot):
            at = block(unit)
            if zz < LINE - 1:
                arrived(gp_s.at[gp_rows(at + above, size - above)], sum_recv.at[colour, 4, slot])
            if zz > 0:
                view = gp_s.at[gp_rows(at + own, size - own)]
                ship(view, view, 2, sum_recv.at[colour, 4, slot], to_left)

        return ([(hop_rs + zz, rs_right), (hop_rs + LINE - 1 - zz, rs_left)],
                [(hop_ag + zz, ag_right), (hop_ag + LINE - 1 - zz, ag_left)])

    half_a, part_b = PART // 2, PART // LINE
    half_b = part_b // 2

    def actions_a(zz):
        def mine(unit):
            return unit * PART + rep_y * half_a

        def theirs(unit):
            return unit * PART + (1 - rep_y) * half_a

        def y_send(unit, slot):
            ship_part(unit, slot, ya_out.at[slot], ya_buf.at[slot], 0, 0, to_y, gp_s[gp_rows(theirs(unit), half_a), :])

        def y_add(unit, slot):
            arrived(ya_buf.at[slot], sum_recv.at[0, 0, slot])
            gp_s[gp_rows(mine(unit), half_a), :] += ya_buf[slot]

        def y_give(unit, slot):
            view = gp_s.at[gp_rows(mine(unit), half_a)]
            ship(view, view, 0, sum_recv.at[0, 5, slot], to_y)

        def finish(unit, slot):
            arrived(gp_s.at[gp_rows(theirs(unit), half_a)], sum_recv.at[0, 5, slot])
            put_unit(unit)

        scatter, gather = line_actions(zz, 0, mine, half_a, la_buf, ra_buf, la_out, ra_out, 1, 4)
        return [(0, y_send), (1, y_add)] + scatter + gather + [(7, y_give), (8, finish)]

    def actions_b(zz):
        def block(unit):
            return (UNITS_A + unit) * PART

        def mine(unit):
            return block(unit) + zz * part_b + rep_y * half_b

        def theirs(unit):
            return block(unit) + zz * part_b + (1 - rep_y) * half_b

        def y_send(unit, slot):
            ship_part(unit, slot, yb_out.at[slot], yb_buf.at[slot], 1, 0, to_y, gp_s[gp_rows(theirs(unit), half_b), :])

        def y_add(unit, slot):
            arrived(yb_buf.at[slot], sum_recv.at[1, 0, slot])
            gp_s[gp_rows(mine(unit), half_b), :] += yb_buf[slot]
            view = gp_s.at[gp_rows(mine(unit), half_b)]
            ship(view, view, 0, sum_recv.at[1, 5, slot], to_y)

        def y_done(unit, slot):
            arrived(gp_s.at[gp_rows(theirs(unit), half_b)], sum_recv.at[1, 5, slot])

        def finish(unit, slot):
            put_unit(UNITS_A + unit)

        scatter, gather = line_actions(zz, 1, block, PART, lb_buf, rb_buf, lb_out, rb_out, 0, 5)
        return scatter + [(3, y_send), (4, y_add), (5, y_done)] + gather + [(8, finish)]

    def b_unit(tick):
        unit = tick * UNITS_B // UNITS_A
        fresh = (tick >= 0) & (tick < UNITS_A) & ((tick + 1) * UNITS_B // UNITS_A > unit)
        return fresh, unit

    def run_actions(tick, hops):
        for zz in range(LINE):
            @pl.when(rep_z == zz)
            def _(zz=zz):
                todo = [(hop, 0, fn) for hop, fn in actions_a(zz)] + [(hop, 1, fn) for hop, fn in actions_b(zz)]
                for want in hops:
                    for colour in range(2):
                        fns = [fn for hop, col, fn in todo if hop == want and col == colour]
                        if not fns:
                            continue
                        start = tick - want
                        if colour == 0:
                            fresh, unit = (start >= 0) & (start < UNITS_A), start
                        else:
                            fresh, unit = b_unit(start)

                        @pl.when(fresh)
                        def _(fns=fns, unit=unit):
                            for fn in fns:
                                fn(unit, unit % SLOTS)

    def compute_for(tick):
        @pl.when((tick < UNITS_A) & (tick % per_tile == 0))
        def _():
            compute_tile(tick // per_tile)

        fresh, unit = b_unit(tick)

        @pl.when(fresh & (unit % per_tile == 0))
        def _():
            compute_tile((UNITS_A + unit) // per_tile)

    compute_for(0)

    def tick_step(tick, _):
        run_actions(tick, [0])
        compute_for(tick + 1)
        run_actions(tick, range(1, 9))
        return 0

    lax.fori_loop(0, UNITS_A + 8, tick_step, 0)

    def sent_all(link, size):
        view = gp_s.at[pl.ds(0, size)]
        pltpu.make_async_copy(view, view, sum_send.at[link]).wait()

    for zz in range(LINE):
        @pl.when(rep_z == zz)
        def _(zz=zz):
            line_rows = UNITS_A * (half_a // LINE) + UNITS_B * part_b
            sent_all(0, UNITS_A * half_a + UNITS_B * half_b)
            if zz < LINE - 1:
                sent_all(1, line_rows * (zz + 1))
            if zz > 0:
                sent_all(2, line_rows * (LINE - zz))
            for slot in range(SLOTS):
                for colour, (out_y, out_l, out_r) in enumerate(((ya_out, la_out, ra_out), (yb_out, lb_out, rb_out))):
                    size = out_l.shape[1]
                    part_done(out_y.at[slot], colour, 0, slot)
                    if zz < LINE - 1:
                        part_done(out_r.at[slot, (zz + 1) * size // LINE:size], colour, 1, slot)
                    if zz > 0:
                        part_done(out_l.at[slot, 0:zz * size // LINE], colour, 2, slot)

    pltpu.make_async_copy(gp_s, gp_s, put_sem).wait()

    for step in range(1, DATA):
        peer = (rep + step) % DATA
        pltpu.make_async_copy(gain_all.at[peer], gain_all.at[peer], gain_recv.at[peer]).wait()
    total = gain_all[0]
    for peer in range(1, DATA):
        total = total + gain_all[peer]
    gain_ref[...] = total
    pltpu.make_async_copy(gain_all.at[pl.ds(0, DATA - 1)], gain_all.at[pl.ds(0, DATA - 1)], gain_send).wait()

    lax.fori_loop(0, SEQ_MB, functools.partial(sent, 1), 0)
    lax.fori_loop(SEQ_MB, n_mb, functools.partial(sent, SEQ_MB), 0)

    @pl.when(pos < last)
    def _():
        pltpu.make_async_copy(out_ref, out_ref, home_sem).wait()

    for step in range(1, PIPE):
        pltpu.make_async_copy(lens_buf.at[own_slab], lens_buf.at[own_slab], in_sem.at[step - 1]).wait()
    for src, _, send, _, target in spread:
        @pl.when(target != pos)
        def _(src=src, send=send):
            pltpu.make_async_copy(src, src, send).wait()


def run_pass(acts, cots, lens, w_qkv, w_out, w_up, w_down, gain_a, gain_m):
    n_tok = acts.shape[0] * PIPE
    n_seq = n_tok // SEQ
    n_mb = n_seq // SEQ_MB + SEQ_MB - 1
    any_spec = pl.BlockSpec(memory_space=pl.ANY)
    vmem_spec = pl.BlockSpec(memory_space=pltpu.VMEM)
    dma = pltpu.SemaphoreType.DMA
    return pl.pallas_call(
        functools.partial(pass_kernel, n_seq),
        out_shape=(
            jax.ShapeDtypeStruct(acts.shape, BF16),
            jax.ShapeDtypeStruct((D, 3 * D), F32),
            jax.ShapeDtypeStruct((D, D), F32),
            jax.ShapeDtypeStruct((D, FFN), F32),
            jax.ShapeDtypeStruct((FFN, D), F32),
            jax.ShapeDtypeStruct((8, D), F32),
        ),
        in_specs=[any_spec] * 2 + [pl.BlockSpec(memory_space=pltpu.SMEM)] + [any_spec] * 4 + [vmem_spec] * 2,
        out_specs=[any_spec] * 5 + [vmem_spec],
        scratch_shapes=[
            pltpu.VMEM((D, 3 * D), BF16),
            pltpu.VMEM((D, D), BF16),
            pltpu.VMEM((D, FFN), BF16),
            pltpu.VMEM((FFN, D), BF16),
            pltpu.VMEM((n_seq, 8, 128), jnp.int32),
            pltpu.VMEM((n_tok, D), BF16),
            pltpu.VMEM((n_tok, D), BF16),
            pltpu.VMEM((n_tok, D), BF16),
            pltpu.VMEM((n_tok, D), BF16),
            pltpu.VMEM((n_tok, 3 * D), BF16),
            pltpu.VMEM((n_tok, D), BF16),
            pltpu.VMEM((n_tok, D), BF16),
            pltpu.VMEM((n_tok, D), BF16),
            pltpu.VMEM((n_tok, FFN), BF16),
            pltpu.VMEM((n_tok * FFN // D, D), F32),
            pltpu.VMEM((n_tok, FFN), BF16),
            pltpu.VMEM((n_tok, D), BF16),
            pltpu.VMEM((n_tok * PAIRS, 128), F32),
            pltpu.VMEM((SEQ_MB * PAIRS * SEQ, 128), F32),
            pltpu.VMEM((2, 8, D), F32),
            pltpu.VMEM((DATA, 8, D), F32),
        ] + [
            pltpu.VMEM((SLOTS, size, D), F32)
            for size in (PART // 2, PART // 2, PART // 2, PART // LINE // 2, PART, PART) * 2
        ] + [
            dma((4,)),
            dma((2 * (n_seq // PIPE) + PIPE - 1,)),
            dma((n_mb,)),
            dma((n_mb,)),
            dma((PIPE,)),
            dma((n_mb,)),
            dma,
            dma((2, 6, SLOTS)),
            dma((3,)),
            dma((2, 3, SLOTS)),
            dma((DATA,)),
            dma,
            dma,
        ],
        compiler_params=pltpu.CompilerParams(collective_id=0, has_side_effects=True, vmem_limit_bytes=64 * 1024 * 1024 - 131072),
    )(acts, cots, lens, w_qkv, w_out, w_up, w_down, gain_a, gain_m)


def solution(mesh):
    row_spec = P(('data', 'pipe'))
    stage_spec = P('pipe')

    def device_pass(acts_in, cot_out, seq_lens, w_qkv, w_out, w_up, w_down, gain_attn, gain_mlp):
        outs = run_pass(acts_in.reshape(-1, D), cot_out.reshape(-1, D), seq_lens, w_qkv.reshape(D, 3 * D),
                        w_out.reshape(D, D), w_up.reshape(D, FFN), w_down.reshape(FFN, D),
                        gain_attn, gain_mlp)
        acts_out, g_qkv, g_out, g_up, g_down, g_gain = outs
        grads = (g_qkv.reshape(w_qkv.shape), g_out.reshape(w_out.shape), g_up.reshape(w_up.shape), g_down.reshape(w_down.shape),
                 g_gain[0:1], g_gain[1:2])
        return (acts_out.reshape(acts_in.shape),) + grads

    return jax.shard_map(device_pass, mesh=mesh, in_specs=(row_spec, row_spec, row_spec) + (stage_spec,) * 6, out_specs=(row_spec,) + (stage_spec,) * 6, check_vma=False)
```

```python
import functools
import jax
import jax.numpy as jnp
from jax import lax
from jax.experimental import pallas as pl
from jax.experimental.pallas import tpu as pltpu
from jax.sharding import PartitionSpec as P

NORM_EPS = 1e-5
MESH = pl.DeviceIdType.MESH
F32 = jnp.float32
BF16 = jnp.bfloat16
SEQ = 64
HEAD = 64
D = 512
FFN = 2048
PIPE = 4
DATA = 8
LINE = 4
TILE = 128
PART = 128
UNITS_A = 28
UNITS_B = 20
SLOTS = 4
SEQ_MB = 3
PAIRS = 4


def dot_nn(lhs, rhs):
    return lax.dot_general(lhs, rhs, (((1,), (0,)), ((), ())), preferred_element_type=F32)


def dot_nt(lhs, rhs):
    return lax.dot_general(lhs, rhs, (((1,), (1,)), ((), ())), preferred_element_type=F32)


def dot_tn(lhs, rhs):
    return lax.dot_general(lhs, rhs, (((0,), (0,)), ((), ())), preferred_element_type=F32)


def pass_kernel(n_seq, acts_ref, cot_ref, lens_ref, wqkv_hbm, wout_hbm, wup_hbm, wdown_hbm, ga_ref, gm_ref,
                out_ref, gp_s, gain_ref,
                wqkv, wout, wup, wdown, lens_buf, xin, cin, hout, na_s, qkv_s, ctx_s, mid_s, nm_s, gelu_s,
                dpre_s, dmid_s, p_s, s_scr, gain_acc, gain_all, ya_buf, la_buf, ra_buf, yb_buf, lb_buf, rb_buf,
                ya_out, la_out, ra_out, yb_out, lb_out, rb_out,
                w_sem, in_sem, x_sem, c_sem, len_sem, send_sem, home_sem, sum_recv, sum_send, part_send, gain_recv, gain_send):
    pos = lax.axis_index('pipe')
    rep = lax.axis_index('data')
    rep_z, rep_y = rep // 2, rep % 2
    n_tok = n_seq * SEQ
    n_mb = n_seq // SEQ_MB + SEQ_MB - 1
    n_own = n_seq // PIPE
    own_slab = pl.ds(pos * n_own, n_own)
    for seq in range(n_own):
        lens_buf[pos * n_own + seq] = jnp.full((8, 128), lens_ref[seq], jnp.int32)
    last = PIPE - 1

    w_copies = [pltpu.make_async_copy(src, dst, w_sem.at[idx]) for idx, (src, dst) in enumerate(
        ((wqkv_hbm, wqkv), (wout_hbm, wout), (wup_hbm, wup), (wdown_hbm, wdown)))]
    for w_copy in w_copies:
        w_copy.start()

    barrier = pltpu.get_barrier_semaphore()
    for step in range(1, PIPE):
        pl.semaphore_signal(barrier, inc=1, device_id={'pipe': (pos + step) % PIPE}, device_id_type=MESH)
    for step in range(1, DATA):
        pl.semaphore_signal(barrier, inc=1, device_id={'data': (rep + step) % DATA}, device_id_type=MESH)
    with jax.named_scope('barrier'):
        pl.semaphore_wait(barrier, PIPE - 1 + DATA - 1)

    def first_seq(mb, size):
        return mb if size == 1 else (mb - SEQ_MB + 1) * SEQ_MB

    def rows_of(mb, size):
        return pl.ds(pl.multiple_of(first_seq(mb, size) * SEQ, SEQ), size * SEQ)

    def seq_rows(mb, size, seq):
        return pl.ds(pl.multiple_of((first_seq(mb, size) + seq) * SEQ, SEQ), SEQ)

    def part_rows(mb, size, part):
        return pl.ds(pl.multiple_of(part * n_tok + first_seq(mb, size) * SEQ, SEQ), size * SEQ)

    def send_to(src, dst, send, recv, target):
        pltpu.make_async_remote_copy(src_ref=src, dst_ref=dst, send_sem=send, recv_sem=recv,
                                     device_id={'pipe': target}, device_id_type=MESH).start()

    def place(src, dst, send, recv, target):
        @pl.when(target == pos)
        def _():
            pltpu.make_async_copy(src, dst, recv).start()

        @pl.when(target != pos)
        def _():
            send_to(src, dst, send, recv, target)

    for step in range(1, PIPE):
        send_to(lens_buf.at[own_slab], lens_buf.at[own_slab], in_sem.at[step - 1], len_sem.at[pos], (pos + step) % PIPE)
    spread = []
    for src, dst, sem, target in ((acts_ref, xin, x_sem, 0), (cot_ref, cin, c_sem, last)):
        for seq in range(n_own):
            at = pos * n_own + seq
            mb = jnp.where(at < SEQ_MB, at, at // SEQ_MB + SEQ_MB - 1)
            spread.append((src.at[pl.ds(seq * SEQ, SEQ)], dst.at[pl.ds(pl.multiple_of(at * SEQ, SEQ), SEQ)],
                           in_sem.at[PIPE - 1 + len(spread)], sem.at[mb], target))
    for item in spread:
        place(*item)

    lane = lax.broadcasted_iota(jnp.int32, (SEQ, 128), 1)
    row = lax.broadcasted_iota(jnp.int32, (SEQ, 128), 0)
    first = lane < HEAD
    key_pos = jnp.where(first, lane, lane - HEAD)
    lane_row = lax.broadcasted_iota(jnp.int32, (1, 128), 1)
    take_a = jnp.where(lane_row < HEAD, 1.0, 0.0).astype(BF16)
    take_b = jnp.where(lane_row < HEAD, 0.0, 1.0).astype(BF16)

    def blocks(pair_cols):
        return jnp.concatenate([pair_cols * take_a, pair_cols * take_b], axis=0)

    def halves_sum(arr):
        sum_a = jnp.sum(jnp.where(first[None], arr, 0.0), axis=-1, keepdims=True)
        sum_b = jnp.sum(jnp.where(first[None], 0.0, arr), axis=-1, keepdims=True)
        return sum_a, sum_b

    def lens_of(mb, size, seq):
        return lens_buf[first_seq(mb, size) + seq][0:1, :]

    def valid_mask(lens_row):
        ok = jnp.where(row < lens_row, 1.0, 0.0)
        return jnp.concatenate([ok] * (D // 128), axis=1)

    def inv_rms(val):
        return lax.rsqrt(jnp.mean(val * val, axis=-1, keepdims=True) + NORM_EPS)

    def forward(size, mb, _):
        rows = rows_of(mb, size)
        start = first_seq(mb, size)

        @pl.when((start % n_own == 0) & (start // n_own != pos))
        def _():
            slab = lens_buf.at[pl.ds(start, n_own)]
            pltpu.make_async_copy(slab, slab, len_sem.at[start // n_own]).wait()

        x_view = xin.at[rows]
        with jax.named_scope('fwait'):
            pltpu.make_async_copy(x_view, x_view, x_sem.at[mb]).wait()
        gain_a = ga_ref[...].astype(F32)
        hid = xin[rows, :].astype(F32)
        normed = (hid * inv_rms(hid) * gain_a).astype(BF16)
        na_s[rows, :] = normed
        for part in range(3):
            cols = slice(part * D, (part + 1) * D)
            qkv_s[rows, cols] = dot_nn(normed, wqkv[:, cols]).astype(BF16)

        for seq in range(size):
            for pair in range(PAIRS):
                q_cols = qkv_s[seq_rows(mb, size, seq), pair * 128:(pair + 1) * 128]
                k_cols = qkv_s[seq_rows(mb, size, seq), D + pair * 128:D + (pair + 1) * 128]
                spot = (seq * PAIRS + pair) * SEQ
                s_scr[spot:spot + SEQ, :] = dot_nt(q_cols, blocks(k_cols))
        for seq in range(size):
            visible = (key_pos <= row) & (key_pos < lens_of(mb, size, seq))
            spot = seq * PAIRS * SEQ
            scores = s_scr[spot:spot + PAIRS * SEQ, :].reshape(PAIRS, SEQ, 128) * (HEAD ** -0.5)
            scores = jnp.where(visible[None], scores, -1e30)
            max_a = jnp.max(jnp.where(first[None], scores, -3e38), axis=-1, keepdims=True)
            max_b = jnp.max(jnp.where(first[None], -3e38, scores), axis=-1, keepdims=True)
            expd = jnp.exp(scores - jnp.where(first[None], max_a, max_b))
            sum_a, sum_b = halves_sum(expd)
            probs = expd * jnp.where(first[None], 1.0 / sum_a, 1.0 / sum_b)
            p_rows = pl.ds(pl.multiple_of(start * PAIRS * SEQ + spot, SEQ), PAIRS * SEQ)
            p_s[p_rows, :] = probs.reshape(PAIRS * SEQ, 128)
        for seq in range(size):
            for pair in range(PAIRS):
                v_cols = qkv_s[seq_rows(mb, size, seq), 2 * D + pair * 128:2 * D + (pair + 1) * 128]
                p_rows = pl.ds(pl.multiple_of((start * PAIRS + seq * PAIRS + pair) * SEQ, SEQ), SEQ)
                ctx_s[seq_rows(mb, size, seq), pair * 128:(pair + 1) * 128] = dot_nn(
                    p_s[p_rows, :].astype(BF16), blocks(v_cols)).astype(BF16)
        mid = (hid + dot_nn(ctx_s[rows, :], wout[...])).astype(BF16)
        mid_s[rows, :] = mid
        mid_f = mid.astype(F32)
        normed_m = (mid_f * inv_rms(mid_f) * gm_ref[...].astype(F32)).astype(BF16)
        nm_s[rows, :] = normed_m
        for part in range(FFN // D):
            cols = slice(part * D, (part + 1) * D)
            pre = dot_nn(normed_m, wup[:, cols])
            cdf = 0.5 + 0.5 * lax.erf(pre * (0.5 ** 0.5))
            gelu_s[rows, cols] = (pre * cdf).astype(BF16)
            gp_s[part_rows(mb, size, part), :] = cdf + pre * (jnp.exp(pre * pre * -0.5) * 0.3989422804014327)
        top = mid_f + dot_nn(gelu_s[rows, :], wdown[...])
        for seq in range(size):
            mask = valid_mask(jnp.where(pos == last, lens_of(mb, size, seq), SEQ))
            piece = top[seq * SEQ:(seq + 1) * SEQ, :].astype(BF16)
            hout[seq_rows(mb, size, seq), :] = jnp.where(mask > 0.0, piece.astype(F32), 0.0).astype(BF16)

        h_view = hout.at[rows]

        @pl.when(pos < last)
        def _():
            send_to(h_view, xin.at[rows], send_sem.at[mb], x_sem.at[mb], pos + 1)

        @pl.when(pos == last)
        def _():
            home = start // n_own
            o_view = out_ref.at[pl.ds(pl.multiple_of((start % n_own) * SEQ, SEQ), size * SEQ)]

            @pl.when(home == pos)
            def _():
                pltpu.make_async_copy(h_view, o_view, send_sem.at[mb]).start()

            @pl.when(home != pos)
            def _():
                send_to(h_view, o_view, send_sem.at[mb], home_sem, home)

        return 0

    with jax.named_scope('wwait'):
        for w_copy in w_copies:
            w_copy.wait()
    lax.fori_loop(0, SEQ_MB, functools.partial(forward, 1), 0)
    lax.fori_loop(SEQ_MB, n_mb, functools.partial(forward, SEQ_MB), 0)

    def sent(size, mb, _):
        h_view = hout.at[rows_of(mb, size)]
        pltpu.make_async_copy(h_view, h_view, send_sem.at[mb]).wait()
        return 0

    gain_acc[...] = jnp.zeros_like(gain_acc)

    def norm_back(hid, gain, d_normed):
        inv = inv_rms(hid)
        unit = hid * inv
        d_gain = jnp.sum((d_normed * unit).reshape(hid.shape[0] // 8, 8, D), axis=0)
        scaled = d_normed * gain
        return inv * (scaled - unit * jnp.mean(unit * scaled, axis=-1, keepdims=True)), d_gain

    def backward(size, mb, _):
        rows = rows_of(mb, size)
        start = first_seq(mb, size)
        c_view = cin.at[rows]
        with jax.named_scope('bwait'):
            pltpu.make_async_copy(c_view, c_view, c_sem.at[mb]).wait()

        for seq in range(size):
            mask = valid_mask(lens_of(mb, size, seq))
            cin[seq_rows(mb, size, seq), :] = jnp.where(mask > 0.0, cin[seq_rows(mb, size, seq), :].astype(F32), 0.0).astype(BF16)
        d_top = cin[rows, :]
        for part in range(FFN // D):
            cols = slice(part * D, (part + 1) * D)
            d_gelu = dot_nt(d_top, wdown[cols, :])
            dpre_s[rows, cols] = (d_gelu * gp_s[part_rows(mb, size, part), :]).astype(BF16)
        d_nm = dot_nt(dpre_s[rows, :], wup[...])
        d_add, d_gain = norm_back(mid_s[rows, :].astype(F32), gm_ref[...].astype(F32), d_nm)
        gain_acc[1] += d_gain
        d_mid = d_top.astype(F32) + d_add
        d_mid_bf = d_mid.astype(BF16)
        dmid_s[rows, :] = d_mid_bf
        d_ctx = dot_nt(d_mid_bf, wout[...]).astype(BF16)
        for seq in range(size):
            for pair in range(PAIRS):
                v_cols = qkv_s[seq_rows(mb, size, seq), 2 * D + pair * 128:2 * D + (pair + 1) * 128]
                dc = d_ctx[seq * SEQ:(seq + 1) * SEQ, pair * 128:(pair + 1) * 128]
                spot = (seq * PAIRS + pair) * SEQ
                p_rows = pl.ds(pl.multiple_of(start * PAIRS * SEQ + spot, SEQ), SEQ)
                s_scr[spot:spot + SEQ, :] = dot_nt(dc, blocks(v_cols))
                both = dot_tn(p_s[p_rows, :].astype(BF16), dc)
                qkv_s[seq_rows(mb, size, seq), 2 * D + pair * 128:2 * D + (pair + 1) * 128] = jnp.where(
                    first, both[:SEQ], both[SEQ:]).astype(BF16)
        for seq in range(size):
            spot = seq * PAIRS * SEQ
            p_rows = pl.ds(pl.multiple_of(start * PAIRS * SEQ + spot, SEQ), PAIRS * SEQ)
            probs = p_s[p_rows, :].reshape(PAIRS, SEQ, 128)
            d_probs = s_scr[spot:spot + PAIRS * SEQ, :].reshape(PAIRS, SEQ, 128)
            sum_a, sum_b = halves_sum(probs * d_probs)
            d_scores = probs * (d_probs - jnp.where(first[None], sum_a, sum_b)) * (HEAD ** -0.5)
            s_scr[spot:spot + PAIRS * SEQ, :] = d_scores.reshape(PAIRS * SEQ, 128)
        for seq in range(size):
            for pair in range(PAIRS):
                q_at = slice(pair * 128, (pair + 1) * 128)
                k_at = slice(D + pair * 128, D + (pair + 1) * 128)
                q_cols = qkv_s[seq_rows(mb, size, seq), q_at]
                k_cols = qkv_s[seq_rows(mb, size, seq), k_at]
                spot = (seq * PAIRS + pair) * SEQ
                d_sc = s_scr[spot:spot + SEQ, :].astype(BF16)
                both = dot_tn(d_sc, q_cols)
                qkv_s[seq_rows(mb, size, seq), q_at] = dot_nn(d_sc, blocks(k_cols)).astype(BF16)
                qkv_s[seq_rows(mb, size, seq), k_at] = jnp.where(first, both[:SEQ], both[SEQ:]).astype(BF16)
        d_na = dot_nt(qkv_s[rows, :], wqkv[...])
        d_add, d_gain = norm_back(xin[rows, :].astype(F32), ga_ref[...].astype(F32), d_na)
        gain_acc[0] += d_gain

        @pl.when(pos > 0)
        def _():
            sent(size, mb, 0)
            hout[rows, :] = (d_mid + d_add).astype(BF16)
            send_to(hout.at[rows], cin.at[rows], send_sem.at[mb], c_sem.at[mb], pos - 1)

        return 0

    lax.fori_loop(SEQ_MB, n_mb, functools.partial(backward, SEQ_MB), 0)
    lax.fori_loop(0, SEQ_MB, functools.partial(backward, 1), 0)

    gain_all[rep] = jnp.concatenate([jnp.sum(gain_acc[0], axis=0, keepdims=True), jnp.sum(gain_acc[1], axis=0, keepdims=True),
                                     jnp.zeros((6, D), F32)], axis=0)
    for step in range(1, DATA):
        pltpu.make_async_remote_copy(src_ref=gain_all.at[rep], dst_ref=gain_all.at[rep], send_sem=gain_send,
                                     recv_sem=gain_recv.at[rep], device_id={'data': (rep + step) % DATA},
                                     device_id_type=MESH).start()

    per_tile = TILE // PART
    n_down, n_up, n_qkv = FFN // TILE, (D // TILE) * (FFN // D), (D // TILE) * 3

    def tile_kinds(tile):
        up, qkv, out = tile - n_down, tile - n_down - n_up, tile - n_down - n_up - n_qkv
        return (
            (tile < n_down, gelu_s, cin, tile, 0),
            ((up >= 0) & (qkv < 0), nm_s, dpre_s, up // (FFN // D), up % (FFN // D)),
            ((qkv >= 0) & (out < 0), na_s, qkv_s, qkv // 3, qkv % 3),
            (out >= 0, ctx_s, dmid_s, out, 0),
        )

    def tile_at(tile):
        return pl.ds(pl.multiple_of(tile * TILE, TILE), TILE)

    def compute_tile(tile):
        for cond, lhs, rhs, at_row, at_col in tile_kinds(tile):
            @pl.when(cond)
            def _(lhs=lhs, rhs=rhs, at_row=at_row, at_col=at_col):
                cols = pl.ds(0, D) if rhs.shape[1] == D else pl.ds(pl.multiple_of(at_col * D, D), D)
                gp_s[tile_at(tile), :] = dot_tn(lhs[:, pl.ds(pl.multiple_of(at_row * TILE, TILE), TILE)], rhs[:, cols])

    to_y, to_right, to_left = rep + 1 - 2 * rep_y, rep + 2, rep - 2

    def part_done(src, colour, link, slot):
        pltpu.make_async_copy(src, src, part_send.at[colour, link, slot]).wait()

    def ship_part(unit, slot, src, dst, colour, link, target, value):
        @pl.when(unit >= SLOTS)
        def _():
            part_done(src, colour, link, slot)

        src[...] = value
        pltpu.make_async_remote_copy(src_ref=src, dst_ref=dst, send_sem=part_send.at[colour, link, slot],
                                     recv_sem=sum_recv.at[colour, link, slot], device_id={'data': target},
                                     device_id_type=MESH).start()

    def ship(src, dst, link, recv, target):
        pltpu.make_async_remote_copy(src_ref=src, dst_ref=dst, send_sem=sum_send.at[link], recv_sem=recv,
                                     device_id={'data': target}, device_id_type=MESH).start()

    def arrived(view, recv):
        pltpu.make_async_copy(view, view, recv).wait()

    def gp_rows(start, size):
        return pl.ds(pl.multiple_of(start, 8), size)

    def line_actions(zz, colour, block, size, buf_l, buf_r, out_l, out_r, hop_rs, hop_ag):
        chunk = size // LINE
        own, above = zz * chunk, (zz + 1) * chunk

        def rs_right(unit, slot):
            at = block(unit)
            if zz > 0:
                arrived(buf_l.at[slot, own:size], sum_recv.at[colour, 1, slot])
                gp_s[gp_rows(at + own, chunk), :] += buf_l[slot, own:above, :]
            if zz < LINE - 1:
                value = gp_s[gp_rows(at + above, size - above), :]
                if zz > 0:
                    value = value + buf_l[slot, above:size, :]
                ship_part(unit, slot, out_r.at[slot, above:size], buf_l.at[slot, above:size], colour, 1, to_right, value)

        def rs_left(unit, slot):
            at = block(unit)
            if zz < LINE - 1:
                arrived(buf_r.at[slot, 0:above], sum_recv.at[colour, 2, slot])
                gp_s[gp_rows(at + own, chunk), :] += buf_r[slot, own:above, :]
            if zz > 0:
                value = gp_s[gp_rows(at, own), :]
                if zz < LINE - 1:
                    value = value + buf_r[slot, 0:own, :]
                ship_part(unit, slot, out_l.at[slot, 0:own], buf_r.at[slot, 0:own], colour, 2, to_left, value)

        def ag_right(unit, slot):
            at = block(unit)
            if zz > 0:
                arrived(gp_s.at[gp_rows(at, own)], sum_recv.at[colour, 3, slot])
            if zz < LINE - 1:
                view = gp_s.at[gp_rows(at, above)]
                ship(view, view, 1, sum_recv.at[colour, 3, slot], to_right)

        def ag_left(unit, slot):
            at = block(unit)
            if zz < LINE - 1:
                arrived(gp_s.at[gp_rows(at + above, size - above)], sum_recv.at[colour, 4, slot])
            if zz > 0:
                view = gp_s.at[gp_rows(at + own, size - own)]
                ship(view, view, 2, sum_recv.at[colour, 4, slot], to_left)

        return ([(hop_rs + zz, rs_right), (hop_rs + LINE - 1 - zz, rs_left)],
                [(hop_ag + zz, ag_right), (hop_ag + LINE - 1 - zz, ag_left)])

    half_a, part_b = PART // 2, PART // LINE
    half_b = part_b // 2

    def actions_a(zz):
        def mine(unit):
            return unit * PART + rep_y * half_a

        def theirs(unit):
            return unit * PART + (1 - rep_y) * half_a

        def y_send(unit, slot):
            ship_part(unit, slot, ya_out.at[slot], ya_buf.at[slot], 0, 0, to_y, gp_s[gp_rows(theirs(unit), half_a), :])

        def y_add(unit, slot):
            arrived(ya_buf.at[slot], sum_recv.at[0, 0, slot])
            gp_s[gp_rows(mine(unit), half_a), :] += ya_buf[slot]

        def y_give(unit, slot):
            view = gp_s.at[gp_rows(mine(unit), half_a)]
            ship(view, view, 0, sum_recv.at[0, 5, slot], to_y)

        def finish(unit, slot):
            arrived(gp_s.at[gp_rows(theirs(unit), half_a)], sum_recv.at[0, 5, slot])

        scatter, gather = line_actions(zz, 0, mine, half_a, la_buf, ra_buf, la_out, ra_out, 1, 4)
        return [(0, y_send), (1, y_add)] + scatter + gather + [(7, y_give), (8, finish)]

    def actions_b(zz):
        def block(unit):
            return (UNITS_A + unit) * PART

        def mine(unit):
            return block(unit) + zz * part_b + rep_y * half_b

        def theirs(unit):
            return block(unit) + zz * part_b + (1 - rep_y) * half_b

        def y_send(unit, slot):
            ship_part(unit, slot, yb_out.at[slot], yb_buf.at[slot], 1, 0, to_y, gp_s[gp_rows(theirs(unit), half_b), :])

        def y_add(unit, slot):
            arrived(yb_buf.at[slot], sum_recv.at[1, 0, slot])
            gp_s[gp_rows(mine(unit), half_b), :] += yb_buf[slot]
            view = gp_s.at[gp_rows(mine(unit), half_b)]
            ship(view, view, 0, sum_recv.at[1, 5, slot], to_y)

        def y_done(unit, slot):
            arrived(gp_s.at[gp_rows(theirs(unit), half_b)], sum_recv.at[1, 5, slot])

        scatter, gather = line_actions(zz, 1, block, PART, lb_buf, rb_buf, lb_out, rb_out, 0, 5)
        return scatter + [(3, y_send), (4, y_add), (5, y_done)] + gather

    def b_unit(tick):
        unit = tick * UNITS_B // UNITS_A
        fresh = (tick >= 0) & (tick < UNITS_A) & ((tick + 1) * UNITS_B // UNITS_A > unit)
        return fresh, unit

    def run_actions(tick, hops):
        for zz in range(LINE):
            @pl.when(rep_z == zz)
            def _(zz=zz):
                todo = [(hop, 0, fn) for hop, fn in actions_a(zz)] + [(hop, 1, fn) for hop, fn in actions_b(zz)]
                for want in hops:
                    for colour in range(2):
                        fns = [fn for hop, col, fn in todo if hop == want and col == colour]
                        if not fns:
                            continue
                        start = tick - want
                        if colour == 0:
                            fresh, unit = (start >= 0) & (start < UNITS_A), start
                        else:
                            fresh, unit = b_unit(start)

                        @pl.when(fresh)
                        def _(fns=fns, unit=unit):
                            for fn in fns:
                                fn(unit, unit % SLOTS)

    def compute_for(tick):
        @pl.when((tick < UNITS_A) & (tick % per_tile == 0))
        def _():
            compute_tile(tick // per_tile)

        fresh, unit = b_unit(tick)

        @pl.when(fresh & (unit % per_tile == 0))
        def _():
            compute_tile((UNITS_A + unit) // per_tile)

    compute_for(0)

    def tick_step(tick, _):
        with jax.named_scope('tsend'):
            run_actions(tick, [0])
        with jax.named_scope('tcomp'):
            compute_for(tick + 1)
        with jax.named_scope('trest'):
            run_actions(tick, range(1, 9))
        return 0

    lax.fori_loop(0, UNITS_A + 8, tick_step, 0)

    def sent_all(link, size):
        view = gp_s.at[pl.ds(0, size)]
        pltpu.make_async_copy(view, view, sum_send.at[link]).wait()

    for zz in range(LINE):
        @pl.when(rep_z == zz)
        def _(zz=zz):
            line_rows = UNITS_A * (half_a // LINE) + UNITS_B * part_b
            sent_all(0, UNITS_A * half_a + UNITS_B * half_b)
            if zz < LINE - 1:
                sent_all(1, line_rows * (zz + 1))
            if zz > 0:
                sent_all(2, line_rows * (LINE - zz))
            for slot in range(SLOTS):
                for colour, (out_y, out_l, out_r) in enumerate(((ya_out, la_out, ra_out), (yb_out, lb_out, rb_out))):
                    size = out_l.shape[1]
                    part_done(out_y.at[slot], colour, 0, slot)
                    if zz < LINE - 1:
                        part_done(out_r.at[slot, (zz + 1) * size // LINE:size], colour, 1, slot)
                    if zz > 0:
                        part_done(out_l.at[slot, 0:zz * size // LINE], colour, 2, slot)

    for step in range(1, DATA):
        peer = (rep + step) % DATA
        pltpu.make_async_copy(gain_all.at[peer], gain_all.at[peer], gain_recv.at[peer]).wait()
    total = gain_all[0]
    for peer in range(1, DATA):
        total = total + gain_all[peer]
    gain_ref[...] = total
    pltpu.make_async_copy(gain_all.at[pl.ds(0, DATA - 1)], gain_all.at[pl.ds(0, DATA - 1)], gain_send).wait()

    lax.fori_loop(0, SEQ_MB, functools.partial(sent, 1), 0)
    lax.fori_loop(SEQ_MB, n_mb, functools.partial(sent, SEQ_MB), 0)

    @pl.when(pos < last)
    def _():
        pltpu.make_async_copy(out_ref, out_ref, home_sem).wait()

    for step in range(1, PIPE):
        pltpu.make_async_copy(lens_buf.at[own_slab], lens_buf.at[own_slab], in_sem.at[step - 1]).wait()
    for src, _, send, _, target in spread:
        @pl.when(target != pos)
        def _(src=src, send=send):
            pltpu.make_async_copy(src, src, send).wait()


def run_pass(acts, cots, lens, w_qkv, w_out, w_up, w_down, gain_a, gain_m):
    n_tok = acts.shape[0] * PIPE
    n_seq = n_tok // SEQ
    n_mb = n_seq // SEQ_MB + SEQ_MB - 1
    any_spec = pl.BlockSpec(memory_space=pl.ANY)
    vmem_spec = pl.BlockSpec(memory_space=pltpu.VMEM)
    dma = pltpu.SemaphoreType.DMA
    return pl.pallas_call(
        functools.partial(pass_kernel, n_seq),
        out_shape=(
            pltpu.VMEM(acts.shape, BF16),
            pltpu.VMEM((n_tok * FFN // D, D), F32),
            pltpu.VMEM((8, D), F32),
        ),
        in_specs=[any_spec] * 2 + [pl.BlockSpec(memory_space=pltpu.SMEM)] + [any_spec] * 4 + [vmem_spec] * 2,
        out_specs=[vmem_spec] * 3,
        scratch_shapes=[
            pltpu.VMEM((D, 3 * D), BF16),
            pltpu.VMEM((D, D), BF16),
            pltpu.VMEM((D, FFN), BF16),
            pltpu.VMEM((FFN, D), BF16),
            pltpu.VMEM((n_seq, 8, 128), jnp.int32),
            pltpu.VMEM((n_tok, D), BF16),
            pltpu.VMEM((n_tok, D), BF16),
            pltpu.VMEM((n_tok, D), BF16),
            pltpu.VMEM((n_tok, D), BF16),
            pltpu.VMEM((n_tok, 3 * D), BF16),
            pltpu.VMEM((n_tok, D), BF16),
            pltpu.VMEM((n_tok, D), BF16),
            pltpu.VMEM((n_tok, D), BF16),
            pltpu.VMEM((n_tok, FFN), BF16),
            pltpu.VMEM((n_tok, FFN), BF16),
            pltpu.VMEM((n_tok, D), BF16),
            pltpu.VMEM((n_tok * PAIRS, 128), F32),
            pltpu.VMEM((SEQ_MB * PAIRS * SEQ, 128), F32),
            pltpu.VMEM((2, 8, D), F32),
            pltpu.VMEM((DATA, 8, D), F32),
        ] + [
            pltpu.VMEM((SLOTS, size, D), F32)
            for size in (PART // 2, PART // 2, PART // 2, PART // LINE // 2, PART, PART) * 2
        ] + [
            dma((4,)),
            dma((2 * (n_seq // PIPE) + PIPE - 1,)),
            dma((n_mb,)),
            dma((n_mb,)),
            dma((PIPE,)),
            dma((n_mb,)),
            dma,
            dma((2, 6, SLOTS)),
            dma((3,)),
            dma((2, 3, SLOTS)),
            dma((DATA,)),
            dma,
        ],
        compiler_params=pltpu.CompilerParams(collective_id=0, has_side_effects=True, vmem_limit_bytes=50 * 1024 * 1024),
    )(acts, cots, lens, w_qkv, w_out, w_up, w_down, gain_a, gain_m)


def write_kernel(acts_ref, tiles_ref, gain_ref, out_ref, gqkv_ref, gout_ref, gup_ref, gdown_ref, gga_ref, ggm_ref,
                 out_sem, put_sem):
    give = pltpu.make_async_copy(acts_ref, out_ref, out_sem)
    give.start()
    row = 0
    dsts = (gdown_ref, gup_ref, gqkv_ref, gout_ref)
    for dst in dsts:
        for at_row in range(0, dst.shape[0], TILE):
            for at_col in range(0, dst.shape[1], D):
                pltpu.make_async_copy(tiles_ref.at[row:row + TILE], dst.at[at_row:at_row + TILE, at_col:at_col + D],
                                      put_sem).start()
                row += TILE
    gga_ref[...] = gain_ref[0:1, :]
    ggm_ref[...] = gain_ref[1:2, :]
    give.wait()
    pltpu.make_async_copy(tiles_ref, tiles_ref, put_sem).wait()


def write_out(acts, tiles, gains):
    any_spec = pl.BlockSpec(memory_space=pl.ANY)
    vmem_spec = pl.BlockSpec(memory_space=pltpu.VMEM)
    dma = pltpu.SemaphoreType.DMA
    return pl.pallas_call(
        write_kernel,
        out_shape=(
            jax.ShapeDtypeStruct(acts.shape, BF16),
            jax.ShapeDtypeStruct((D, 3 * D), F32),
            jax.ShapeDtypeStruct((D, D), F32),
            jax.ShapeDtypeStruct((D, FFN), F32),
            jax.ShapeDtypeStruct((FFN, D), F32),
            jax.ShapeDtypeStruct((1, D), F32),
            jax.ShapeDtypeStruct((1, D), F32),
        ),
        in_specs=[any_spec, any_spec, vmem_spec],
        out_specs=[any_spec] * 5 + [vmem_spec] * 2,
        scratch_shapes=[dma, dma],
        compiler_params=pltpu.CompilerParams(vmem_limit_bytes=4 * 1024 * 1024),
    )(acts, tiles, gains)


def solution(mesh):
    row_spec = P(('data', 'pipe'))
    stage_spec = P('pipe')

    def device_pass(acts_in, cot_out, seq_lens, w_qkv, w_out, w_up, w_down, gain_attn, gain_mlp):
        outs = run_pass(acts_in.reshape(-1, D), cot_out.reshape(-1, D), seq_lens, w_qkv.reshape(D, 3 * D),
                        w_out.reshape(D, D), w_up.reshape(D, FFN), w_down.reshape(FFN, D),
                        gain_attn, gain_mlp)
        acts_out, g_qkv, g_out, g_up, g_down, g_ga, g_gm = write_out(*outs)
        grads = (g_qkv.reshape(w_qkv.shape), g_out.reshape(w_out.shape), g_up.reshape(w_up.shape), g_down.reshape(w_down.shape),
                 g_ga, g_gm)
        return (acts_out.reshape(acts_in.shape),) + grads

    return jax.shard_map(device_pass, mesh=mesh, in_specs=(row_spec, row_spec, row_spec) + (stage_spec,) * 6, out_specs=(row_spec,) + (stage_spec,) * 6, check_vma=False)
```

```python
import functools
import jax
import jax.numpy as jnp
from jax import lax
from jax.experimental import pallas as pl
from jax.experimental.pallas import tpu as pltpu
from jax.sharding import PartitionSpec as P

NORM_EPS = 1e-5
MESH = pl.DeviceIdType.MESH
F32 = jnp.float32
BF16 = jnp.bfloat16
SEQ = 64
HEAD = 64
D = 512
FFN = 2048
PIPE = 4
DATA = 8
LINE = 4
TILE = 128
PART = 128
UNITS_A = 28
UNITS_B = 20
SLOTS = 4
SEQ_MB = 3
PAIRS = 4


def dot_nn(lhs, rhs):
    return lax.dot_general(lhs, rhs, (((1,), (0,)), ((), ())), preferred_element_type=F32)


def dot_nt(lhs, rhs):
    return lax.dot_general(lhs, rhs, (((1,), (1,)), ((), ())), preferred_element_type=F32)


def dot_tn(lhs, rhs):
    return lax.dot_general(lhs, rhs, (((0,), (0,)), ((), ())), preferred_element_type=F32)


def pass_kernel(n_seq, acts_ref, cot_ref, lens_ref, wqkv_hbm, wout_hbm, wup_hbm, wdown_hbm, ga_ref, gm_ref,
                out_ref, gp_s, gain_ref,
                wqkv, wout, wup, wdown, lens_buf, xin, cin, hout, na_s, qkv_s, ctx_s, mid_s, nm_s, gelu_s,
                dpre_s, dmid_s, p_s, s_scr, gain_acc, gain_all, ya_buf, la_buf, ra_buf, yb_buf, lb_buf, rb_buf,
                ya_out, la_out, ra_out, yb_out, lb_out, rb_out,
                w_sem, in_sem, x_sem, c_sem, len_sem, send_sem, home_sem, sum_recv, sum_send, part_send, gain_recv, gain_send):
    pos = lax.axis_index('pipe')
    rep = lax.axis_index('data')
    rep_z, rep_y = rep // 2, rep % 2
    n_tok = n_seq * SEQ
    n_mb = n_seq // SEQ_MB
    n_own = n_seq // PIPE
    own_slab = pl.ds(pos * n_own, n_own)
    for seq in range(n_own):
        lens_buf[pos * n_own + seq] = jnp.full((8, 128), lens_ref[seq], jnp.int32)
    last = PIPE - 1

    w_copies = [pltpu.make_async_copy(src, dst, w_sem.at[idx]) for idx, (src, dst) in enumerate(
        ((wqkv_hbm, wqkv), (wout_hbm, wout), (wup_hbm, wup), (wdown_hbm, wdown)))]
    for w_copy in w_copies:
        w_copy.start()

    barrier = pltpu.get_barrier_semaphore()
    for step in range(1, PIPE):
        pl.semaphore_signal(barrier, inc=1, device_id={'pipe': (pos + step) % PIPE}, device_id_type=MESH)
    for step in range(1, DATA):
        pl.semaphore_signal(barrier, inc=1, device_id={'data': (rep + step) % DATA}, device_id_type=MESH)
    with jax.named_scope('barrier'):
        pl.semaphore_wait(barrier, PIPE - 1 + DATA - 1)

    def first_seq(mb, size):
        return mb * size

    def rows_of(mb, size):
        return pl.ds(pl.multiple_of(first_seq(mb, size) * SEQ, SEQ), size * SEQ)

    def seq_rows(mb, size, seq):
        return pl.ds(pl.multiple_of((first_seq(mb, size) + seq) * SEQ, SEQ), SEQ)

    def part_rows(mb, size, part):
        return pl.ds(pl.multiple_of(part * n_tok + first_seq(mb, size) * SEQ, SEQ), size * SEQ)

    def send_to(src, dst, send, recv, target):
        pltpu.make_async_remote_copy(src_ref=src, dst_ref=dst, send_sem=send, recv_sem=recv,
                                     device_id={'pipe': target}, device_id_type=MESH).start()

    def place(src, dst, send, recv, target):
        @pl.when(target == pos)
        def _():
            pltpu.make_async_copy(src, dst, recv).start()

        @pl.when(target != pos)
        def _():
            send_to(src, dst, send, recv, target)

    for step in range(1, PIPE):
        send_to(lens_buf.at[own_slab], lens_buf.at[own_slab], in_sem.at[step - 1], len_sem.at[pos], (pos + step) % PIPE)
    spread = []
    for src, dst, sem, target in ((acts_ref, xin, x_sem, 0), (cot_ref, cin, c_sem, last)):
        for seq in range(n_own):
            at = pos * n_own + seq
            mb = at // SEQ_MB
            spread.append((src.at[pl.ds(seq * SEQ, SEQ)], dst.at[pl.ds(pl.multiple_of(at * SEQ, SEQ), SEQ)],
                           in_sem.at[PIPE - 1 + len(spread)], sem.at[mb], target))
    for item in spread:
        place(*item)

    lane = lax.broadcasted_iota(jnp.int32, (SEQ, 128), 1)
    row = lax.broadcasted_iota(jnp.int32, (SEQ, 128), 0)
    first = lane < HEAD
    key_pos = jnp.where(first, lane, lane - HEAD)
    lane_row = lax.broadcasted_iota(jnp.int32, (1, 128), 1)
    take_a = jnp.where(lane_row < HEAD, 1.0, 0.0).astype(BF16)
    take_b = jnp.where(lane_row < HEAD, 0.0, 1.0).astype(BF16)

    def blocks(pair_cols):
        return jnp.concatenate([pair_cols * take_a, pair_cols * take_b], axis=0)

    def halves_sum(arr):
        sum_a = jnp.sum(jnp.where(first[None], arr, 0.0), axis=-1, keepdims=True)
        sum_b = jnp.sum(jnp.where(first[None], 0.0, arr), axis=-1, keepdims=True)
        return sum_a, sum_b

    def lens_of(mb, size, seq):
        return lens_buf[first_seq(mb, size) + seq][0:1, :]

    def valid_mask(lens_row):
        ok = jnp.where(row < lens_row, 1.0, 0.0)
        return jnp.concatenate([ok] * (D // 128), axis=1)

    def inv_rms(val):
        return lax.rsqrt(jnp.mean(val * val, axis=-1, keepdims=True) + NORM_EPS)

    def forward(size, mb, _):
        rows = rows_of(mb, size)
        start = first_seq(mb, size)

        @pl.when((start % n_own == 0) & (start // n_own != pos))
        def _():
            slab = lens_buf.at[pl.ds(start, n_own)]
            pltpu.make_async_copy(slab, slab, len_sem.at[start // n_own]).wait()

        x_view = xin.at[rows]
        with jax.named_scope('fwait'):
            pltpu.make_async_copy(x_view, x_view, x_sem.at[mb]).wait()
        gain_a = ga_ref[...].astype(F32)
        hid = xin[rows, :].astype(F32)
        normed = (hid * inv_rms(hid) * gain_a).astype(BF16)
        na_s[rows, :] = normed
        for part in range(3):
            cols = slice(part * D, (part + 1) * D)
            qkv_s[rows, cols] = dot_nn(normed, wqkv[:, cols]).astype(BF16)

        for seq in range(size):
            for pair in range(PAIRS):
                q_cols = qkv_s[seq_rows(mb, size, seq), pair * 128:(pair + 1) * 128]
                k_cols = qkv_s[seq_rows(mb, size, seq), D + pair * 128:D + (pair + 1) * 128]
                spot = (seq * PAIRS + pair) * SEQ
                s_scr[spot:spot + SEQ, :] = dot_nt(q_cols, blocks(k_cols))
        for seq in range(size):
            visible = (key_pos <= row) & (key_pos < lens_of(mb, size, seq))
            spot = seq * PAIRS * SEQ
            scores = s_scr[spot:spot + PAIRS * SEQ, :].reshape(PAIRS, SEQ, 128) * (HEAD ** -0.5)
            scores = jnp.where(visible[None], scores, -1e30)
            max_a = jnp.max(jnp.where(first[None], scores, -3e38), axis=-1, keepdims=True)
            max_b = jnp.max(jnp.where(first[None], -3e38, scores), axis=-1, keepdims=True)
            expd = jnp.exp(scores - jnp.where(first[None], max_a, max_b))
            sum_a, sum_b = halves_sum(expd)
            probs = expd * jnp.where(first[None], 1.0 / sum_a, 1.0 / sum_b)
            p_rows = pl.ds(pl.multiple_of(start * PAIRS * SEQ + spot, SEQ), PAIRS * SEQ)
            p_s[p_rows, :] = probs.reshape(PAIRS * SEQ, 128)
        for seq in range(size):
            for pair in range(PAIRS):
                v_cols = qkv_s[seq_rows(mb, size, seq), 2 * D + pair * 128:2 * D + (pair + 1) * 128]
                p_rows = pl.ds(pl.multiple_of((start * PAIRS + seq * PAIRS + pair) * SEQ, SEQ), SEQ)
                ctx_s[seq_rows(mb, size, seq), pair * 128:(pair + 1) * 128] = dot_nn(
                    p_s[p_rows, :].astype(BF16), blocks(v_cols)).astype(BF16)
        mid = (hid + dot_nn(ctx_s[rows, :], wout[...])).astype(BF16)
        mid_s[rows, :] = mid
        mid_f = mid.astype(F32)
        normed_m = (mid_f * inv_rms(mid_f) * gm_ref[...].astype(F32)).astype(BF16)
        nm_s[rows, :] = normed_m
        for part in range(FFN // D):
            cols = slice(part * D, (part + 1) * D)
            pre = dot_nn(normed_m, wup[:, cols])
            cdf = 0.5 + 0.5 * lax.erf(pre * (0.5 ** 0.5))
            gelu_s[rows, cols] = (pre * cdf).astype(BF16)
            gp_s[part_rows(mb, size, part), :] = cdf + pre * (jnp.exp(pre * pre * -0.5) * 0.3989422804014327)
        top = mid_f + dot_nn(gelu_s[rows, :], wdown[...])
        for seq in range(size):
            mask = valid_mask(jnp.where(pos == last, lens_of(mb, size, seq), SEQ))
            piece = top[seq * SEQ:(seq + 1) * SEQ, :].astype(BF16)
            hout[seq_rows(mb, size, seq), :] = jnp.where(mask > 0.0, piece.astype(F32), 0.0).astype(BF16)

        h_view = hout.at[rows]

        @pl.when(pos < last)
        def _():
            send_to(h_view, xin.at[rows], send_sem.at[mb], x_sem.at[mb], pos + 1)

        @pl.when(pos == last)
        def _():
            home = start // n_own
            o_view = out_ref.at[pl.ds(pl.multiple_of((start % n_own) * SEQ, SEQ), size * SEQ)]

            @pl.when(home == pos)
            def _():
                pltpu.make_async_copy(h_view, o_view, send_sem.at[mb]).start()

            @pl.when(home != pos)
            def _():
                send_to(h_view, o_view, send_sem.at[mb], home_sem, home)

        return 0

    with jax.named_scope('wwait'):
        for w_copy in w_copies:
            w_copy.wait()
    lax.fori_loop(0, n_mb, functools.partial(forward, SEQ_MB), 0)

    def sent(size, mb, _):
        h_view = hout.at[rows_of(mb, size)]
        pltpu.make_async_copy(h_view, h_view, send_sem.at[mb]).wait()
        return 0

    gain_acc[...] = jnp.zeros_like(gain_acc)

    def norm_back(hid, gain, d_normed):
        inv = inv_rms(hid)
        unit = hid * inv
        d_gain = jnp.sum((d_normed * unit).reshape(hid.shape[0] // 8, 8, D), axis=0)
        scaled = d_normed * gain
        return inv * (scaled - unit * jnp.mean(unit * scaled, axis=-1, keepdims=True)), d_gain

    def backward(size, mb, _):
        rows = rows_of(mb, size)
        start = first_seq(mb, size)
        c_view = cin.at[rows]
        with jax.named_scope('bwait'):
            pltpu.make_async_copy(c_view, c_view, c_sem.at[mb]).wait()

        for seq in range(size):
            mask = valid_mask(lens_of(mb, size, seq))
            cin[seq_rows(mb, size, seq), :] = jnp.where(mask > 0.0, cin[seq_rows(mb, size, seq), :].astype(F32), 0.0).astype(BF16)
        d_top = cin[rows, :]
        for part in range(FFN // D):
            cols = slice(part * D, (part + 1) * D)
            d_gelu = dot_nt(d_top, wdown[cols, :])
            dpre_s[rows, cols] = (d_gelu * gp_s[part_rows(mb, size, part), :]).astype(BF16)
        d_nm = dot_nt(dpre_s[rows, :], wup[...])
        d_add, d_gain = norm_back(mid_s[rows, :].astype(F32), gm_ref[...].astype(F32), d_nm)
        gain_acc[1] += d_gain
        d_mid = d_top.astype(F32) + d_add
        d_mid_bf = d_mid.astype(BF16)
        dmid_s[rows, :] = d_mid_bf
        d_ctx = dot_nt(d_mid_bf, wout[...]).astype(BF16)
        for seq in range(size):
            for pair in range(PAIRS):
                v_cols = qkv_s[seq_rows(mb, size, seq), 2 * D + pair * 128:2 * D + (pair + 1) * 128]
                dc = d_ctx[seq * SEQ:(seq + 1) * SEQ, pair * 128:(pair + 1) * 128]
                spot = (seq * PAIRS + pair) * SEQ
                p_rows = pl.ds(pl.multiple_of(start * PAIRS * SEQ + spot, SEQ), SEQ)
                s_scr[spot:spot + SEQ, :] = dot_nt(dc, blocks(v_cols))
                both = dot_tn(p_s[p_rows, :].astype(BF16), dc)
                qkv_s[seq_rows(mb, size, seq), 2 * D + pair * 128:2 * D + (pair + 1) * 128] = jnp.where(
                    first, both[:SEQ], both[SEQ:]).astype(BF16)
        for seq in range(size):
            spot = seq * PAIRS * SEQ
            p_rows = pl.ds(pl.multiple_of(start * PAIRS * SEQ + spot, SEQ), PAIRS * SEQ)
            probs = p_s[p_rows, :].reshape(PAIRS, SEQ, 128)
            d_probs = s_scr[spot:spot + PAIRS * SEQ, :].reshape(PAIRS, SEQ, 128)
            sum_a, sum_b = halves_sum(probs * d_probs)
            d_scores = probs * (d_probs - jnp.where(first[None], sum_a, sum_b)) * (HEAD ** -0.5)
            s_scr[spot:spot + PAIRS * SEQ, :] = d_scores.reshape(PAIRS * SEQ, 128)
        for seq in range(size):
            for pair in range(PAIRS):
                q_at = slice(pair * 128, (pair + 1) * 128)
                k_at = slice(D + pair * 128, D + (pair + 1) * 128)
                q_cols = qkv_s[seq_rows(mb, size, seq), q_at]
                k_cols = qkv_s[seq_rows(mb, size, seq), k_at]
                spot = (seq * PAIRS + pair) * SEQ
                d_sc = s_scr[spot:spot + SEQ, :].astype(BF16)
                both = dot_tn(d_sc, q_cols)
                qkv_s[seq_rows(mb, size, seq), q_at] = dot_nn(d_sc, blocks(k_cols)).astype(BF16)
                qkv_s[seq_rows(mb, size, seq), k_at] = jnp.where(first, both[:SEQ], both[SEQ:]).astype(BF16)
        d_na = dot_nt(qkv_s[rows, :], wqkv[...])
        d_add, d_gain = norm_back(xin[rows, :].astype(F32), ga_ref[...].astype(F32), d_na)
        gain_acc[0] += d_gain

        @pl.when(pos > 0)
        def _():
            sent(size, mb, 0)
            hout[rows, :] = (d_mid + d_add).astype(BF16)
            send_to(hout.at[rows], cin.at[rows], send_sem.at[mb], c_sem.at[mb], pos - 1)

        return 0

    lax.fori_loop(0, n_mb, functools.partial(backward, SEQ_MB), 0)

    gain_all[rep] = jnp.concatenate([jnp.sum(gain_acc[0], axis=0, keepdims=True), jnp.sum(gain_acc[1], axis=0, keepdims=True),
                                     jnp.zeros((6, D), F32)], axis=0)
    for step in range(1, DATA):
        pltpu.make_async_remote_copy(src_ref=gain_all.at[rep], dst_ref=gain_all.at[rep], send_sem=gain_send,
                                     recv_sem=gain_recv.at[rep], device_id={'data': (rep + step) % DATA},
                                     device_id_type=MESH).start()

    per_tile = TILE // PART
    n_down, n_up, n_qkv = FFN // TILE, (D // TILE) * (FFN // D), (D // TILE) * 3

    def tile_kinds(tile):
        up, qkv, out = tile - n_down, tile - n_down - n_up, tile - n_down - n_up - n_qkv
        return (
            (tile < n_down, gelu_s, cin, tile, 0),
            ((up >= 0) & (qkv < 0), nm_s, dpre_s, up // (FFN // D), up % (FFN // D)),
            ((qkv >= 0) & (out < 0), na_s, qkv_s, qkv // 3, qkv % 3),
            (out >= 0, ctx_s, dmid_s, out, 0),
        )

    def tile_at(tile):
        return pl.ds(pl.multiple_of(tile * TILE, TILE), TILE)

    def compute_tile(tile):
        for cond, lhs, rhs, at_row, at_col in tile_kinds(tile):
            @pl.when(cond)
            def _(lhs=lhs, rhs=rhs, at_row=at_row, at_col=at_col):
                cols = pl.ds(0, D) if rhs.shape[1] == D else pl.ds(pl.multiple_of(at_col * D, D), D)
                gp_s[tile_at(tile), :] = dot_tn(lhs[:, pl.ds(pl.multiple_of(at_row * TILE, TILE), TILE)], rhs[:, cols])

    to_y, to_right, to_left = rep + 1 - 2 * rep_y, rep + 2, rep - 2

    def part_done(src, colour, link, slot):
        pltpu.make_async_copy(src, src, part_send.at[colour, link, slot]).wait()

    def ship_part(unit, slot, src, dst, colour, link, target, value):
        @pl.when(unit >= SLOTS)
        def _():
            part_done(src, colour, link, slot)

        src[...] = value
        pltpu.make_async_remote_copy(src_ref=src, dst_ref=dst, send_sem=part_send.at[colour, link, slot],
                                     recv_sem=sum_recv.at[colour, link, slot], device_id={'data': target},
                                     device_id_type=MESH).start()

    def ship(src, dst, link, recv, target):
        pltpu.make_async_remote_copy(src_ref=src, dst_ref=dst, send_sem=sum_send.at[link], recv_sem=recv,
                                     device_id={'data': target}, device_id_type=MESH).start()

    def arrived(view, recv):
        pltpu.make_async_copy(view, view, recv).wait()

    def gp_rows(start, size):
        return pl.ds(pl.multiple_of(start, 8), size)

    def line_actions(zz, colour, block, size, buf_l, buf_r, out_l, out_r, hop_rs, hop_ag):
        chunk = size // LINE
        own, above = zz * chunk, (zz + 1) * chunk

        def rs_right(unit, slot):
            at = block(unit)
            if zz > 0:
                arrived(buf_l.at[slot, own:size], sum_recv.at[colour, 1, slot])
                gp_s[gp_rows(at + own, chunk), :] += buf_l[slot, own:above, :]
            if zz < LINE - 1:
                value = gp_s[gp_rows(at + above, size - above), :]
                if zz > 0:
                    value = value + buf_l[slot, above:size, :]
                ship_part(unit, slot, out_r.at[slot, above:size], buf_l.at[slot, above:size], colour, 1, to_right, value)

        def rs_left(unit, slot):
            at = block(unit)
            if zz < LINE - 1:
                arrived(buf_r.at[slot, 0:above], sum_recv.at[colour, 2, slot])
                gp_s[gp_rows(at + own, chunk), :] += buf_r[slot, own:above, :]
            if zz > 0:
                value = gp_s[gp_rows(at, own), :]
                if zz < LINE - 1:
                    value = value + buf_r[slot, 0:own, :]
                ship_part(unit, slot, out_l.at[slot, 0:own], buf_r.at[slot, 0:own], colour, 2, to_left, value)

        def ag_right(unit, slot):
            at = block(unit)
            if zz > 0:
                arrived(gp_s.at[gp_rows(at, own)], sum_recv.at[colour, 3, slot])
            if zz < LINE - 1:
                view = gp_s.at[gp_rows(at, above)]
                ship(view, view, 1, sum_recv.at[colour, 3, slot], to_right)

        def ag_left(unit, slot):
            at = block(unit)
            if zz < LINE - 1:
                arrived(gp_s.at[gp_rows(at + above, size - above)], sum_recv.at[colour, 4, slot])
            if zz > 0:
                view = gp_s.at[gp_rows(at + own, size - own)]
                ship(view, view, 2, sum_recv.at[colour, 4, slot], to_left)

        return ([(hop_rs + zz, rs_right), (hop_rs + LINE - 1 - zz, rs_left)],
                [(hop_ag + zz, ag_right), (hop_ag + LINE - 1 - zz, ag_left)])

    half_a, part_b = PART // 2, PART // LINE
    half_b = part_b // 2

    def actions_a(zz):
        def mine(unit):
            return unit * PART + rep_y * half_a

        def theirs(unit):
            return unit * PART + (1 - rep_y) * half_a

        def y_send(unit, slot):
            ship_part(unit, slot, ya_out.at[slot], ya_buf.at[slot], 0, 0, to_y, gp_s[gp_rows(theirs(unit), half_a), :])

        def y_add(unit, slot):
            arrived(ya_buf.at[slot], sum_recv.at[0, 0, slot])
            gp_s[gp_rows(mine(unit), half_a), :] += ya_buf[slot]

        def y_give(unit, slot):
            view = gp_s.at[gp_rows(mine(unit), half_a)]
            ship(view, view, 0, sum_recv.at[0, 5, slot], to_y)

        def finish(unit, slot):
            arrived(gp_s.at[gp_rows(theirs(unit), half_a)], sum_recv.at[0, 5, slot])

        scatter, gather = line_actions(zz, 0, mine, half_a, la_buf, ra_buf, la_out, ra_out, 1, 4)
        return [(0, y_send), (1, y_add)] + scatter + gather + [(7, y_give), (8, finish)]

    def actions_b(zz):
        def block(unit):
            return (UNITS_A + unit) * PART

        def mine(unit):
            return block(unit) + zz * part_b + rep_y * half_b

        def theirs(unit):
            return block(unit) + zz * part_b + (1 - rep_y) * half_b

        def y_send(unit, slot):
            ship_part(unit, slot, yb_out.at[slot], yb_buf.at[slot], 1, 0, to_y, gp_s[gp_rows(theirs(unit), half_b), :])

        def y_add(unit, slot):
            arrived(yb_buf.at[slot], sum_recv.at[1, 0, slot])
            gp_s[gp_rows(mine(unit), half_b), :] += yb_buf[slot]
            view = gp_s.at[gp_rows(mine(unit), half_b)]
            ship(view, view, 0, sum_recv.at[1, 5, slot], to_y)

        def y_done(unit, slot):
            arrived(gp_s.at[gp_rows(theirs(unit), half_b)], sum_recv.at[1, 5, slot])

        scatter, gather = line_actions(zz, 1, block, PART, lb_buf, rb_buf, lb_out, rb_out, 0, 5)
        return scatter + [(3, y_send), (4, y_add), (5, y_done)] + gather

    def b_unit(tick):
        return (tick >= 0) & (tick < UNITS_B), tick

    def run_actions(tick, hops):
        for zz in range(LINE):
            @pl.when(rep_z == zz)
            def _(zz=zz):
                todo = [(hop, 0, fn) for hop, fn in actions_a(zz)] + [(hop, 1, fn) for hop, fn in actions_b(zz)]
                for want in hops:
                    for colour in range(2):
                        fns = [fn for hop, col, fn in todo if hop == want and col == colour]
                        if not fns:
                            continue
                        start = tick - want
                        if colour == 0:
                            fresh, unit = (start >= 0) & (start < UNITS_A), start
                        else:
                            fresh, unit = b_unit(start)

                        @pl.when(fresh)
                        def _(fns=fns, unit=unit):
                            for fn in fns:
                                fn(unit, unit % SLOTS)

    def compute_for(tick):
        @pl.when((tick < UNITS_A) & (tick % per_tile == 0))
        def _():
            compute_tile(tick // per_tile)

        fresh, unit = b_unit(tick)

        @pl.when(fresh & (unit % per_tile == 0))
        def _():
            compute_tile((UNITS_A + unit) // per_tile)

    compute_for(0)

    def tick_step(tick, _):
        with jax.named_scope('tsend'):
            run_actions(tick, [0])
        with jax.named_scope('tcomp'):
            compute_for(tick + 1)
        with jax.named_scope('trest'):
            run_actions(tick, range(1, 9))
        return 0

    lax.fori_loop(0, UNITS_A + 8, tick_step, 0)

    def sent_all(link, size):
        view = gp_s.at[pl.ds(0, size)]
        pltpu.make_async_copy(view, view, sum_send.at[link]).wait()

    for zz in range(LINE):
        @pl.when(rep_z == zz)
        def _(zz=zz):
            line_rows = UNITS_A * (half_a // LINE) + UNITS_B * part_b
            sent_all(0, UNITS_A * half_a + UNITS_B * half_b)
            if zz < LINE - 1:
                sent_all(1, line_rows * (zz + 1))
            if zz > 0:
                sent_all(2, line_rows * (LINE - zz))
            for slot in range(SLOTS):
                for colour, (out_y, out_l, out_r) in enumerate(((ya_out, la_out, ra_out), (yb_out, lb_out, rb_out))):
                    size = out_l.shape[1]
                    part_done(out_y.at[slot], colour, 0, slot)
                    if zz < LINE - 1:
                        part_done(out_r.at[slot, (zz + 1) * size // LINE:size], colour, 1, slot)
                    if zz > 0:
                        part_done(out_l.at[slot, 0:zz * size // LINE], colour, 2, slot)

    for step in range(1, DATA):
        peer = (rep + step) % DATA
        pltpu.make_async_copy(gain_all.at[peer], gain_all.at[peer], gain_recv.at[peer]).wait()
    total = gain_all[0]
    for peer in range(1, DATA):
        total = total + gain_all[peer]
    gain_ref[...] = total
    pltpu.make_async_copy(gain_all.at[pl.ds(0, DATA - 1)], gain_all.at[pl.ds(0, DATA - 1)], gain_send).wait()

    lax.fori_loop(0, n_mb, functools.partial(sent, SEQ_MB), 0)

    @pl.when(pos < last)
    def _():
        pltpu.make_async_copy(out_ref, out_ref, home_sem).wait()

    for step in range(1, PIPE):
        pltpu.make_async_copy(lens_buf.at[own_slab], lens_buf.at[own_slab], in_sem.at[step - 1]).wait()
    for src, _, send, _, target in spread:
        @pl.when(target != pos)
        def _(src=src, send=send):
            pltpu.make_async_copy(src, src, send).wait()


def run_pass(acts, cots, lens, w_qkv, w_out, w_up, w_down, gain_a, gain_m):
    n_tok = acts.shape[0] * PIPE
    n_seq = n_tok // SEQ
    n_mb = n_seq // SEQ_MB
    any_spec = pl.BlockSpec(memory_space=pl.ANY)
    vmem_spec = pl.BlockSpec(memory_space=pltpu.VMEM)
    dma = pltpu.SemaphoreType.DMA
    return pl.pallas_call(
        functools.partial(pass_kernel, n_seq),
        out_shape=(
            pltpu.VMEM(acts.shape, BF16),
            pltpu.VMEM((n_tok * FFN // D, D), F32),
            pltpu.VMEM((8, D), F32),
        ),
        in_specs=[any_spec] * 2 + [pl.BlockSpec(memory_space=pltpu.SMEM)] + [any_spec] * 4 + [vmem_spec] * 2,
        out_specs=[vmem_spec] * 3,
        scratch_shapes=[
            pltpu.VMEM((D, 3 * D), BF16),
            pltpu.VMEM((D, D), BF16),
            pltpu.VMEM((D, FFN), BF16),
            pltpu.VMEM((FFN, D), BF16),
            pltpu.VMEM((n_seq, 8, 128), jnp.int32),
            pltpu.VMEM((n_tok, D), BF16),
            pltpu.VMEM((n_tok, D), BF16),
            pltpu.VMEM((n_tok, D), BF16),
            pltpu.VMEM((n_tok, D), BF16),
            pltpu.VMEM((n_tok, 3 * D), BF16),
            pltpu.VMEM((n_tok, D), BF16),
            pltpu.VMEM((n_tok, D), BF16),
            pltpu.VMEM((n_tok, D), BF16),
            pltpu.VMEM((n_tok, FFN), BF16),
            pltpu.VMEM((n_tok, FFN), BF16),
            pltpu.VMEM((n_tok, D), BF16),
            pltpu.VMEM((n_tok * PAIRS, 128), F32),
            pltpu.VMEM((SEQ_MB * PAIRS * SEQ, 128), F32),
            pltpu.VMEM((2, 8, D), F32),
            pltpu.VMEM((DATA, 8, D), F32),
        ] + [
            pltpu.VMEM((SLOTS, size, D), F32)
            for size in (PART // 2, PART // 2, PART // 2, PART // LINE // 2, PART, PART) * 2
        ] + [
            dma((4,)),
            dma((2 * (n_seq // PIPE) + PIPE - 1,)),
            dma((n_mb,)),
            dma((n_mb,)),
            dma((PIPE,)),
            dma((n_mb,)),
            dma,
            dma((2, 6, SLOTS)),
            dma((3,)),
            dma((2, 3, SLOTS)),
            dma((DATA,)),
            dma,
        ],
        compiler_params=pltpu.CompilerParams(collective_id=0, has_side_effects=True, vmem_limit_bytes=50 * 1024 * 1024),
    )(acts, cots, lens, w_qkv, w_out, w_up, w_down, gain_a, gain_m)


def write_kernel(acts_ref, tiles_ref, gain_ref, out_ref, gqkv_ref, gout_ref, gup_ref, gdown_ref, gga_ref, ggm_ref,
                 out_sem, put_sem):
    give = pltpu.make_async_copy(acts_ref, out_ref, out_sem)
    give.start()
    row = 0
    dsts = (gdown_ref, gup_ref, gqkv_ref, gout_ref)
    for dst in dsts:
        for at_row in range(0, dst.shape[0], TILE):
            for at_col in range(0, dst.shape[1], D):
                pltpu.make_async_copy(tiles_ref.at[row:row + TILE], dst.at[at_row:at_row + TILE, at_col:at_col + D],
                                      put_sem).start()
                row += TILE
    gga_ref[...] = gain_ref[0:1, :]
    ggm_ref[...] = gain_ref[1:2, :]
    give.wait()
    pltpu.make_async_copy(tiles_ref, tiles_ref, put_sem).wait()


def write_out(acts, tiles, gains):
    any_spec = pl.BlockSpec(memory_space=pl.ANY)
    vmem_spec = pl.BlockSpec(memory_space=pltpu.VMEM)
    dma = pltpu.SemaphoreType.DMA
    return pl.pallas_call(
        write_kernel,
        out_shape=(
            jax.ShapeDtypeStruct(acts.shape, BF16),
            jax.ShapeDtypeStruct((D, 3 * D), F32),
            jax.ShapeDtypeStruct((D, D), F32),
            jax.ShapeDtypeStruct((D, FFN), F32),
            jax.ShapeDtypeStruct((FFN, D), F32),
            jax.ShapeDtypeStruct((1, D), F32),
            jax.ShapeDtypeStruct((1, D), F32),
        ),
        in_specs=[any_spec, any_spec, vmem_spec],
        out_specs=[any_spec] * 5 + [vmem_spec] * 2,
        scratch_shapes=[dma, dma],
        compiler_params=pltpu.CompilerParams(vmem_limit_bytes=4 * 1024 * 1024),
    )(acts, tiles, gains)


def solution(mesh):
    row_spec = P(('data', 'pipe'))
    stage_spec = P('pipe')

    def device_pass(acts_in, cot_out, seq_lens, w_qkv, w_out, w_up, w_down, gain_attn, gain_mlp):
        outs = run_pass(acts_in.reshape(-1, D), cot_out.reshape(-1, D), seq_lens, w_qkv.reshape(D, 3 * D),
                        w_out.reshape(D, D), w_up.reshape(D, FFN), w_down.reshape(FFN, D),
                        gain_attn, gain_mlp)
        acts_out, g_qkv, g_out, g_up, g_down, g_ga, g_gm = write_out(*outs)
        grads = (g_qkv.reshape(w_qkv.shape), g_out.reshape(w_out.shape), g_up.reshape(w_up.shape), g_down.reshape(w_down.shape),
                 g_ga, g_gm)
        return (acts_out.reshape(acts_in.shape),) + grads

    return jax.shard_map(device_pass, mesh=mesh, in_specs=(row_spec, row_spec, row_spec) + (stage_spec,) * 6, out_specs=(row_spec,) + (stage_spec,) * 6, check_vma=False)
```

```python
import functools
import jax
import jax.numpy as jnp
from jax import lax
from jax.experimental import pallas as pl
from jax.experimental.pallas import tpu as pltpu
from jax.sharding import PartitionSpec as P

NORM_EPS = 1e-5
MESH = pl.DeviceIdType.MESH
F32 = jnp.float32
BF16 = jnp.bfloat16
SEQ = 64
HEAD = 64
D = 512
FFN = 2048
PIPE = 4
DATA = 8
LINE = 4
TILE = 128
PART_B = 64
UNITS_A = 30
EXTRA = 5
UNITS_X = UNITS_A // EXTRA
SLOTS = 4
SEQ_MB = 3
PAIRS = 4


def dot_nn(lhs, rhs):
    return lax.dot_general(lhs, rhs, (((1,), (0,)), ((), ())), preferred_element_type=F32)


def dot_nt(lhs, rhs):
    return lax.dot_general(lhs, rhs, (((1,), (1,)), ((), ())), preferred_element_type=F32)


def dot_tn(lhs, rhs):
    return lax.dot_general(lhs, rhs, (((0,), (0,)), ((), ())), preferred_element_type=F32)


def pass_kernel(n_seq, acts_ref, cot_ref, lens_ref, wqkv_hbm, wout_hbm, wup_hbm, wdown_hbm, ga_ref, gm_ref,
                out_ref, gp_s, gain_ref,
                wqkv, wout, wup, wdown, lens_buf, xin, cin, hout, na_s, qkv_s, ctx_s, mid_s, nm_s, gelu_s,
                dpre_s, dmid_s, p_s, s_scr, gain_acc, gain_all, ya_buf, la_buf, ra_buf, yb_buf, lb_buf, rb_buf, yx_buf, lx_buf, rx_buf,
                ya_out, la_out, ra_out, yb_out, lb_out, rb_out, yx_out, lx_out, rx_out,
                w_sem, in_sem, x_sem, c_sem, len_sem, send_sem, home_sem, sum_recv, sum_send, part_send, gain_recv, gain_send):
    pos = lax.axis_index('pipe')
    rep = lax.axis_index('data')
    rep_z, rep_y = rep // 2, rep % 2
    n_tok = n_seq * SEQ
    n_mb = n_seq // SEQ_MB
    n_own = n_seq // PIPE
    own_slab = pl.ds(pos * n_own, n_own)
    for seq in range(n_own):
        lens_buf[pos * n_own + seq] = jnp.full((8, 128), lens_ref[seq], jnp.int32)
    last = PIPE - 1

    w_copies = [pltpu.make_async_copy(src, dst, w_sem.at[idx]) for idx, (src, dst) in enumerate(
        ((wqkv_hbm, wqkv), (wout_hbm, wout), (wup_hbm, wup), (wdown_hbm, wdown)))]
    for w_copy in w_copies:
        w_copy.start()

    barrier = pltpu.get_barrier_semaphore()
    for step in range(1, PIPE):
        pl.semaphore_signal(barrier, inc=1, device_id={'pipe': (pos + step) % PIPE}, device_id_type=MESH)
    for step in range(1, DATA):
        pl.semaphore_signal(barrier, inc=1, device_id={'data': (rep + step) % DATA}, device_id_type=MESH)
    with jax.named_scope('barrier'):
        pl.semaphore_wait(barrier, PIPE - 1 + DATA - 1)

    def first_seq(mb, size):
        return mb * size

    def rows_of(mb, size):
        return pl.ds(pl.multiple_of(first_seq(mb, size) * SEQ, SEQ), size * SEQ)

    def seq_rows(mb, size, seq):
        return pl.ds(pl.multiple_of((first_seq(mb, size) + seq) * SEQ, SEQ), SEQ)

    def part_rows(mb, size, part):
        return pl.ds(pl.multiple_of(part * n_tok + first_seq(mb, size) * SEQ, SEQ), size * SEQ)

    def send_to(src, dst, send, recv, target):
        pltpu.make_async_remote_copy(src_ref=src, dst_ref=dst, send_sem=send, recv_sem=recv,
                                     device_id={'pipe': target}, device_id_type=MESH).start()

    def place(src, dst, send, recv, target):
        @pl.when(target == pos)
        def _():
            pltpu.make_async_copy(src, dst, recv).start()

        @pl.when(target != pos)
        def _():
            send_to(src, dst, send, recv, target)

    for step in range(1, PIPE):
        send_to(lens_buf.at[own_slab], lens_buf.at[own_slab], in_sem.at[step - 1], len_sem.at[pos], (pos + step) % PIPE)
    spread = []
    for src, dst, sem, target in ((acts_ref, xin, x_sem, 0), (cot_ref, cin, c_sem, last)):
        for seq in range(n_own):
            at = pos * n_own + seq
            mb = at // SEQ_MB
            spread.append((src.at[pl.ds(seq * SEQ, SEQ)], dst.at[pl.ds(pl.multiple_of(at * SEQ, SEQ), SEQ)],
                           in_sem.at[PIPE - 1 + len(spread)], sem.at[mb], target))
    for item in spread:
        place(*item)

    lane = lax.broadcasted_iota(jnp.int32, (SEQ, 128), 1)
    row = lax.broadcasted_iota(jnp.int32, (SEQ, 128), 0)
    first = lane < HEAD
    key_pos = jnp.where(first, lane, lane - HEAD)
    lane_row = lax.broadcasted_iota(jnp.int32, (1, 128), 1)
    take_a = jnp.where(lane_row < HEAD, 1.0, 0.0).astype(BF16)
    take_b = jnp.where(lane_row < HEAD, 0.0, 1.0).astype(BF16)

    def blocks(pair_cols):
        return jnp.concatenate([pair_cols * take_a, pair_cols * take_b], axis=0)

    def halves_sum(arr):
        sum_a = jnp.sum(jnp.where(first[None], arr, 0.0), axis=-1, keepdims=True)
        sum_b = jnp.sum(jnp.where(first[None], 0.0, arr), axis=-1, keepdims=True)
        return sum_a, sum_b

    def lens_of(mb, size, seq):
        return lens_buf[first_seq(mb, size) + seq][0:1, :]

    def valid_mask(lens_row):
        ok = jnp.where(row < lens_row, 1.0, 0.0)
        return jnp.concatenate([ok] * (D // 128), axis=1)

    def inv_rms(val):
        return lax.rsqrt(jnp.mean(val * val, axis=-1, keepdims=True) + NORM_EPS)

    def forward(size, mb, _):
        rows = rows_of(mb, size)
        start = first_seq(mb, size)

        @pl.when((start % n_own == 0) & (start // n_own != pos))
        def _():
            slab = lens_buf.at[pl.ds(start, n_own)]
            pltpu.make_async_copy(slab, slab, len_sem.at[start // n_own]).wait()

        x_view = xin.at[rows]
        with jax.named_scope('fwait'):
            pltpu.make_async_copy(x_view, x_view, x_sem.at[mb]).wait()
        gain_a = ga_ref[...].astype(F32)
        hid = xin[rows, :].astype(F32)
        normed = (hid * inv_rms(hid) * gain_a).astype(BF16)
        na_s[rows, :] = normed
        for part in range(3):
            cols = slice(part * D, (part + 1) * D)
            qkv_s[rows, cols] = dot_nn(normed, wqkv[:, cols]).astype(BF16)

        for seq in range(size):
            for pair in range(PAIRS):
                q_cols = qkv_s[seq_rows(mb, size, seq), pair * 128:(pair + 1) * 128]
                k_cols = qkv_s[seq_rows(mb, size, seq), D + pair * 128:D + (pair + 1) * 128]
                spot = (seq * PAIRS + pair) * SEQ
                s_scr[spot:spot + SEQ, :] = dot_nt(q_cols, blocks(k_cols))
        for seq in range(size):
            visible = (key_pos <= row) & (key_pos < lens_of(mb, size, seq))
            spot = seq * PAIRS * SEQ
            scores = s_scr[spot:spot + PAIRS * SEQ, :].reshape(PAIRS, SEQ, 128) * (HEAD ** -0.5)
            scores = jnp.where(visible[None], scores, -1e30)
            max_a = jnp.max(jnp.where(first[None], scores, -3e38), axis=-1, keepdims=True)
            max_b = jnp.max(jnp.where(first[None], -3e38, scores), axis=-1, keepdims=True)
            expd = jnp.exp(scores - jnp.where(first[None], max_a, max_b))
            sum_a, sum_b = halves_sum(expd)
            probs = expd * jnp.where(first[None], 1.0 / sum_a, 1.0 / sum_b)
            p_rows = pl.ds(pl.multiple_of(start * PAIRS * SEQ + spot, SEQ), PAIRS * SEQ)
            p_s[p_rows, :] = probs.reshape(PAIRS * SEQ, 128)
        for seq in range(size):
            for pair in range(PAIRS):
                v_cols = qkv_s[seq_rows(mb, size, seq), 2 * D + pair * 128:2 * D + (pair + 1) * 128]
                p_rows = pl.ds(pl.multiple_of((start * PAIRS + seq * PAIRS + pair) * SEQ, SEQ), SEQ)
                ctx_s[seq_rows(mb, size, seq), pair * 128:(pair + 1) * 128] = dot_nn(
                    p_s[p_rows, :].astype(BF16), blocks(v_cols)).astype(BF16)
        mid = (hid + dot_nn(ctx_s[rows, :], wout[...])).astype(BF16)
        mid_s[rows, :] = mid
        mid_f = mid.astype(F32)
        normed_m = (mid_f * inv_rms(mid_f) * gm_ref[...].astype(F32)).astype(BF16)
        nm_s[rows, :] = normed_m
        for part in range(FFN // D):
            cols = slice(part * D, (part + 1) * D)
            pre = dot_nn(normed_m, wup[:, cols])
            cdf = 0.5 + 0.5 * lax.erf(pre * (0.5 ** 0.5))
            gelu_s[rows, cols] = (pre * cdf).astype(BF16)
            gp_s[part_rows(mb, size, part), :] = cdf + pre * (jnp.exp(pre * pre * -0.5) * 0.3989422804014327)
        top = mid_f + dot_nn(gelu_s[rows, :], wdown[...])
        for seq in range(size):
            mask = valid_mask(jnp.where(pos == last, lens_of(mb, size, seq), SEQ))
            piece = top[seq * SEQ:(seq + 1) * SEQ, :].astype(BF16)
            hout[seq_rows(mb, size, seq), :] = jnp.where(mask > 0.0, piece.astype(F32), 0.0).astype(BF16)

        h_view = hout.at[rows]

        @pl.when(pos < last)
        def _():
            send_to(h_view, xin.at[rows], send_sem.at[mb], x_sem.at[mb], pos + 1)

        @pl.when(pos == last)
        def _():
            home = start // n_own
            o_view = out_ref.at[pl.ds(pl.multiple_of((start % n_own) * SEQ, SEQ), size * SEQ)]

            @pl.when(home == pos)
            def _():
                pltpu.make_async_copy(h_view, o_view, send_sem.at[mb]).start()

            @pl.when(home != pos)
            def _():
                send_to(h_view, o_view, send_sem.at[mb], home_sem, home)

        return 0

    with jax.named_scope('wwait'):
        for w_copy in w_copies:
            w_copy.wait()
    lax.fori_loop(0, n_mb, functools.partial(forward, SEQ_MB), 0)

    def sent(size, mb, _):
        h_view = hout.at[rows_of(mb, size)]
        pltpu.make_async_copy(h_view, h_view, send_sem.at[mb]).wait()
        return 0

    gain_acc[...] = jnp.zeros_like(gain_acc)

    def norm_back(hid, gain, d_normed):
        inv = inv_rms(hid)
        unit = hid * inv
        d_gain = jnp.sum((d_normed * unit).reshape(hid.shape[0] // 8, 8, D), axis=0)
        scaled = d_normed * gain
        return inv * (scaled - unit * jnp.mean(unit * scaled, axis=-1, keepdims=True)), d_gain

    def backward(size, mb, _):
        rows = rows_of(mb, size)
        start = first_seq(mb, size)
        c_view = cin.at[rows]
        with jax.named_scope('bwait'):
            pltpu.make_async_copy(c_view, c_view, c_sem.at[mb]).wait()

        for seq in range(size):
            mask = valid_mask(lens_of(mb, size, seq))
            cin[seq_rows(mb, size, seq), :] = jnp.where(mask > 0.0, cin[seq_rows(mb, size, seq), :].astype(F32), 0.0).astype(BF16)
        d_top = cin[rows, :]
        for part in range(FFN // D):
            cols = slice(part * D, (part + 1) * D)
            d_gelu = dot_nt(d_top, wdown[cols, :])
            dpre_s[rows, cols] = (d_gelu * gp_s[part_rows(mb, size, part), :]).astype(BF16)
        d_nm = dot_nt(dpre_s[rows, :], wup[...])
        d_add, d_gain = norm_back(mid_s[rows, :].astype(F32), gm_ref[...].astype(F32), d_nm)
        gain_acc[1] += d_gain
        d_mid = d_top.astype(F32) + d_add
        d_mid_bf = d_mid.astype(BF16)
        dmid_s[rows, :] = d_mid_bf
        d_ctx = dot_nt(d_mid_bf, wout[...]).astype(BF16)
        for seq in range(size):
            for pair in range(PAIRS):
                v_cols = qkv_s[seq_rows(mb, size, seq), 2 * D + pair * 128:2 * D + (pair + 1) * 128]
                dc = d_ctx[seq * SEQ:(seq + 1) * SEQ, pair * 128:(pair + 1) * 128]
                spot = (seq * PAIRS + pair) * SEQ
                p_rows = pl.ds(pl.multiple_of(start * PAIRS * SEQ + spot, SEQ), SEQ)
                s_scr[spot:spot + SEQ, :] = dot_nt(dc, blocks(v_cols))
                both = dot_tn(p_s[p_rows, :].astype(BF16), dc)
                qkv_s[seq_rows(mb, size, seq), 2 * D + pair * 128:2 * D + (pair + 1) * 128] = jnp.where(
                    first, both[:SEQ], both[SEQ:]).astype(BF16)
        for seq in range(size):
            spot = seq * PAIRS * SEQ
            p_rows = pl.ds(pl.multiple_of(start * PAIRS * SEQ + spot, SEQ), PAIRS * SEQ)
            probs = p_s[p_rows, :].reshape(PAIRS, SEQ, 128)
            d_probs = s_scr[spot:spot + PAIRS * SEQ, :].reshape(PAIRS, SEQ, 128)
            sum_a, sum_b = halves_sum(probs * d_probs)
            d_scores = probs * (d_probs - jnp.where(first[None], sum_a, sum_b)) * (HEAD ** -0.5)
            s_scr[spot:spot + PAIRS * SEQ, :] = d_scores.reshape(PAIRS * SEQ, 128)
        for seq in range(size):
            for pair in range(PAIRS):
                q_at = slice(pair * 128, (pair + 1) * 128)
                k_at = slice(D + pair * 128, D + (pair + 1) * 128)
                q_cols = qkv_s[seq_rows(mb, size, seq), q_at]
                k_cols = qkv_s[seq_rows(mb, size, seq), k_at]
                spot = (seq * PAIRS + pair) * SEQ
                d_sc = s_scr[spot:spot + SEQ, :].astype(BF16)
                both = dot_tn(d_sc, q_cols)
                qkv_s[seq_rows(mb, size, seq), q_at] = dot_nn(d_sc, blocks(k_cols)).astype(BF16)
                qkv_s[seq_rows(mb, size, seq), k_at] = jnp.where(first, both[:SEQ], both[SEQ:]).astype(BF16)
        d_na = dot_nt(qkv_s[rows, :], wqkv[...])
        d_add, d_gain = norm_back(xin[rows, :].astype(F32), ga_ref[...].astype(F32), d_na)
        gain_acc[0] += d_gain

        @pl.when(pos > 0)
        def _():
            sent(size, mb, 0)
            hout[rows, :] = (d_mid + d_add).astype(BF16)
            send_to(hout.at[rows], cin.at[rows], send_sem.at[mb], c_sem.at[mb], pos - 1)

        return 0

    lax.fori_loop(0, n_mb, functools.partial(backward, SEQ_MB), 0)

    gain_all[rep] = jnp.concatenate([jnp.sum(gain_acc[0], axis=0, keepdims=True), jnp.sum(gain_acc[1], axis=0, keepdims=True),
                                     jnp.zeros((6, D), F32)], axis=0)
    for step in range(1, DATA):
        pltpu.make_async_remote_copy(src_ref=gain_all.at[rep], dst_ref=gain_all.at[rep], send_sem=gain_send,
                                     recv_sem=gain_recv.at[rep], device_id={'data': (rep + step) % DATA},
                                     device_id_type=MESH).start()

    per_tile = TILE // PART_B
    n_down, n_up, n_qkv = FFN // TILE, (D // TILE) * (FFN // D), (D // TILE) * 3

    def tile_kinds(tile):
        up, qkv, out = tile - n_down, tile - n_down - n_up, tile - n_down - n_up - n_qkv
        return (
            (tile < n_down, gelu_s, cin, tile, 0),
            ((up >= 0) & (qkv < 0), nm_s, dpre_s, up // (FFN // D), up % (FFN // D)),
            ((qkv >= 0) & (out < 0), na_s, qkv_s, qkv // 3, qkv % 3),
            (out >= 0, ctx_s, dmid_s, out, 0),
        )

    def tile_at(tile):
        return pl.ds(pl.multiple_of(tile * TILE, TILE), TILE)

    def compute_tile(tile):
        for cond, lhs, rhs, at_row, at_col in tile_kinds(tile):
            @pl.when(cond)
            def _(lhs=lhs, rhs=rhs, at_row=at_row, at_col=at_col):
                cols = pl.ds(0, D) if rhs.shape[1] == D else pl.ds(pl.multiple_of(at_col * D, D), D)
                gp_s[tile_at(tile), :] = dot_tn(lhs[:, pl.ds(pl.multiple_of(at_row * TILE, TILE), TILE)], rhs[:, cols])

    to_y, to_right, to_left = rep + 1 - 2 * rep_y, rep + 2, rep - 2

    def part_done(src, colour, link, slot):
        pltpu.make_async_copy(src, src, part_send.at[colour, link, slot]).wait()

    def ship_part(unit, slot, src, dst, colour, link, target, value):
        @pl.when(unit >= SLOTS)
        def _():
            part_done(src, colour, link, slot)

        src[...] = value
        pltpu.make_async_remote_copy(src_ref=src, dst_ref=dst, send_sem=part_send.at[colour, link, slot],
                                     recv_sem=sum_recv.at[colour, link, slot], device_id={'data': target},
                                     device_id_type=MESH).start()

    def ship(src, dst, link, recv, target):
        pltpu.make_async_remote_copy(src_ref=src, dst_ref=dst, send_sem=sum_send.at[link], recv_sem=recv,
                                     device_id={'data': target}, device_id_type=MESH).start()

    def arrived(view, recv):
        pltpu.make_async_copy(view, view, recv).wait()

    def gp_rows(start, size):
        return pl.ds(pl.multiple_of(start, 8), size)

    def line_actions(zz, colour, block, size, buf_l, buf_r, out_l, out_r, hop_rs, hop_ag):
        chunk = size // LINE
        own, above = zz * chunk, (zz + 1) * chunk

        def rs_right(unit, slot):
            at = block(unit)
            if zz > 0:
                arrived(buf_l.at[slot, own:size], sum_recv.at[colour, 1, slot])
                gp_s[gp_rows(at + own, chunk), :] += buf_l[slot, own:above, :]
            if zz < LINE - 1:
                value = gp_s[gp_rows(at + above, size - above), :]
                if zz > 0:
                    value = value + buf_l[slot, above:size, :]
                ship_part(unit, slot, out_r.at[slot, above:size], buf_l.at[slot, above:size], colour, 1, to_right, value)

        def rs_left(unit, slot):
            at = block(unit)
            if zz < LINE - 1:
                arrived(buf_r.at[slot, 0:above], sum_recv.at[colour, 2, slot])
                gp_s[gp_rows(at + own, chunk), :] += buf_r[slot, own:above, :]
            if zz > 0:
                value = gp_s[gp_rows(at, own), :]
                if zz < LINE - 1:
                    value = value + buf_r[slot, 0:own, :]
                ship_part(unit, slot, out_l.at[slot, 0:own], buf_r.at[slot, 0:own], colour, 2, to_left, value)

        def ag_right(unit, slot):
            at = block(unit)
            if zz > 0:
                arrived(gp_s.at[gp_rows(at, own)], sum_recv.at[colour, 3, slot])
            if zz < LINE - 1:
                view = gp_s.at[gp_rows(at, above)]
                ship(view, view, 1, sum_recv.at[colour, 3, slot], to_right)

        def ag_left(unit, slot):
            at = block(unit)
            if zz < LINE - 1:
                arrived(gp_s.at[gp_rows(at + above, size - above)], sum_recv.at[colour, 4, slot])
            if zz > 0:
                view = gp_s.at[gp_rows(at + own, size - own)]
                ship(view, view, 2, sum_recv.at[colour, 4, slot], to_left)

        return ([(hop_rs + zz, rs_right), (hop_rs + LINE - 1 - zz, rs_left)],
                [(hop_ag + zz, ag_right), (hop_ag + LINE - 1 - zz, ag_left)])

    half_a, part_b = TILE // 2, PART_B // LINE
    half_b = part_b // 2

    def actions_a(zz):
        def mine(unit):
            return unit * TILE + rep_y * half_a

        def theirs(unit):
            return unit * TILE + (1 - rep_y) * half_a

        def y_send(unit, slot):
            ship_part(unit, slot, ya_out.at[slot], ya_buf.at[slot], 0, 0, to_y, gp_s[gp_rows(theirs(unit), half_a), :])

        def y_add(unit, slot):
            arrived(ya_buf.at[slot], sum_recv.at[0, 0, slot])
            gp_s[gp_rows(mine(unit), half_a), :] += ya_buf[slot]

        def y_give(unit, slot):
            view = gp_s.at[gp_rows(mine(unit), half_a)]
            ship(view, view, 0, sum_recv.at[0, 5, slot], to_y)

        def finish(unit, slot):
            arrived(gp_s.at[gp_rows(theirs(unit), half_a)], sum_recv.at[0, 5, slot])

        scatter, gather = line_actions(zz, 0, mine, half_a, la_buf, ra_buf, la_out, ra_out, 1, 4)
        return [(0, y_send), (1, y_add)] + scatter + gather + [(7, y_give), (8, finish)]

    def actions_b(zz, colour, base, bufs, outs):
        y_buf, l_buf, r_buf = bufs
        y_out, l_out, r_out = outs

        def block(unit):
            return UNITS_A * TILE + (base + unit) * PART_B

        def mine(unit):
            return block(unit) + zz * part_b + rep_y * half_b

        def theirs(unit):
            return block(unit) + zz * part_b + (1 - rep_y) * half_b

        def y_send(unit, slot):
            ship_part(unit, slot, y_out.at[slot], y_buf.at[slot], colour, 0, to_y, gp_s[gp_rows(theirs(unit), half_b), :])

        def y_add(unit, slot):
            arrived(y_buf.at[slot], sum_recv.at[colour, 0, slot])
            gp_s[gp_rows(mine(unit), half_b), :] += y_buf[slot]
            view = gp_s.at[gp_rows(mine(unit), half_b)]
            ship(view, view, 0, sum_recv.at[colour, 5, slot], to_y)

        def y_done(unit, slot):
            arrived(gp_s.at[gp_rows(theirs(unit), half_b)], sum_recv.at[colour, 5, slot])

        scatter, gather = line_actions(zz, colour, block, PART_B, l_buf, r_buf, l_out, r_out, 0, 5)
        return scatter + [(3, y_send), (4, y_add), (5, y_done)] + gather

    def unit_of(colour, tick):
        inside = (tick >= 0) & (tick < UNITS_A)
        if colour < 2:
            return inside, tick
        return inside & (tick % EXTRA == 0), tick // EXTRA

    def run_actions(tick, hops):
        for zz in range(LINE):
            @pl.when(rep_z == zz)
            def _(zz=zz):
                todo = (
                    actions_a(zz),
                    actions_b(zz, 1, 0, (yb_buf, lb_buf, rb_buf), (yb_out, lb_out, rb_out)),
                    actions_b(zz, 2, UNITS_A, (yx_buf, lx_buf, rx_buf), (yx_out, lx_out, rx_out)),
                )
                for want in hops:
                    for colour in range(3):
                        fns = [fn for hop, fn in todo[colour] if hop == want]
                        if not fns:
                            continue
                        fresh, unit = unit_of(colour, tick - want)

                        @pl.when(fresh)
                        def _(fns=fns, unit=unit):
                            for fn in fns:
                                fn(unit, unit % SLOTS)

    def compute_for(tick):
        @pl.when(tick < UNITS_A)
        def _():
            compute_tile(tick)

        for colour, base in ((1, 0), (2, UNITS_A)):
            fresh, unit = unit_of(colour, tick)

            @pl.when(fresh & (unit % per_tile == 0))
            def _(unit=unit, base=base):
                compute_tile(UNITS_A + (base + unit) // per_tile)

    compute_for(0)

    def tick_step(tick, _):
        with jax.named_scope('tsend'):
            run_actions(tick, [0])
        with jax.named_scope('tcomp'):
            compute_for(tick + 1)
        with jax.named_scope('trest'):
            run_actions(tick, range(1, 9))
        return 0

    lax.fori_loop(0, UNITS_A + 8, tick_step, 0)

    def sent_all(link, size):
        view = gp_s.at[pl.ds(0, size)]
        pltpu.make_async_copy(view, view, sum_send.at[link]).wait()

    for zz in range(LINE):
        @pl.when(rep_z == zz)
        def _(zz=zz):
            line_rows = UNITS_A * (half_a // LINE) + (UNITS_A + UNITS_X) * part_b
            sent_all(0, UNITS_A * half_a + (UNITS_A + UNITS_X) * half_b)
            if zz < LINE - 1:
                sent_all(1, line_rows * (zz + 1))
            if zz > 0:
                sent_all(2, line_rows * (LINE - zz))
            for slot in range(SLOTS):
                for colour, (out_y, out_l, out_r) in enumerate(
                        ((ya_out, la_out, ra_out), (yb_out, lb_out, rb_out), (yx_out, lx_out, rx_out))):
                    size = out_l.shape[1]
                    part_done(out_y.at[slot], colour, 0, slot)
                    if zz < LINE - 1:
                        part_done(out_r.at[slot, (zz + 1) * size // LINE:size], colour, 1, slot)
                    if zz > 0:
                        part_done(out_l.at[slot, 0:zz * size // LINE], colour, 2, slot)

    for step in range(1, DATA):
        peer = (rep + step) % DATA
        pltpu.make_async_copy(gain_all.at[peer], gain_all.at[peer], gain_recv.at[peer]).wait()
    total = gain_all[0]
    for peer in range(1, DATA):
        total = total + gain_all[peer]
    gain_ref[...] = total
    pltpu.make_async_copy(gain_all.at[pl.ds(0, DATA - 1)], gain_all.at[pl.ds(0, DATA - 1)], gain_send).wait()

    lax.fori_loop(0, n_mb, functools.partial(sent, SEQ_MB), 0)

    @pl.when(pos < last)
    def _():
        pltpu.make_async_copy(out_ref, out_ref, home_sem).wait()

    for step in range(1, PIPE):
        pltpu.make_async_copy(lens_buf.at[own_slab], lens_buf.at[own_slab], in_sem.at[step - 1]).wait()
    for src, _, send, _, target in spread:
        @pl.when(target != pos)
        def _(src=src, send=send):
            pltpu.make_async_copy(src, src, send).wait()


def run_pass(acts, cots, lens, w_qkv, w_out, w_up, w_down, gain_a, gain_m):
    n_tok = acts.shape[0] * PIPE
    n_seq = n_tok // SEQ
    n_mb = n_seq // SEQ_MB
    any_spec = pl.BlockSpec(memory_space=pl.ANY)
    vmem_spec = pl.BlockSpec(memory_space=pltpu.VMEM)
    dma = pltpu.SemaphoreType.DMA
    return pl.pallas_call(
        functools.partial(pass_kernel, n_seq),
        out_shape=(
            pltpu.VMEM(acts.shape, BF16),
            pltpu.VMEM((n_tok * FFN // D, D), F32),
            pltpu.VMEM((8, D), F32),
        ),
        in_specs=[any_spec] * 2 + [pl.BlockSpec(memory_space=pltpu.SMEM)] + [any_spec] * 4 + [vmem_spec] * 2,
        out_specs=[vmem_spec] * 3,
        scratch_shapes=[
            pltpu.VMEM((D, 3 * D), BF16),
            pltpu.VMEM((D, D), BF16),
            pltpu.VMEM((D, FFN), BF16),
            pltpu.VMEM((FFN, D), BF16),
            pltpu.VMEM((n_seq, 8, 128), jnp.int32),
            pltpu.VMEM((n_tok, D), BF16),
            pltpu.VMEM((n_tok, D), BF16),
            pltpu.VMEM((n_tok, D), BF16),
            pltpu.VMEM((n_tok, D), BF16),
            pltpu.VMEM((n_tok, 3 * D), BF16),
            pltpu.VMEM((n_tok, D), BF16),
            pltpu.VMEM((n_tok, D), BF16),
            pltpu.VMEM((n_tok, D), BF16),
            pltpu.VMEM((n_tok, FFN), BF16),
            pltpu.VMEM((n_tok, FFN), BF16),
            pltpu.VMEM((n_tok, D), BF16),
            pltpu.VMEM((n_tok * PAIRS, 128), F32),
            pltpu.VMEM((SEQ_MB * PAIRS * SEQ, 128), F32),
            pltpu.VMEM((2, 8, D), F32),
            pltpu.VMEM((DATA, 8, D), F32),
        ] + [
            pltpu.VMEM((SLOTS, size, D), F32)
            for size in ((TILE // 2,) * 3 + (PART_B // LINE // 2, PART_B, PART_B) * 2) * 2
        ] + [
            dma((4,)),
            dma((2 * (n_seq // PIPE) + PIPE - 1,)),
            dma((n_mb,)),
            dma((n_mb,)),
            dma((PIPE,)),
            dma((n_mb,)),
            dma,
            dma((3, 6, SLOTS)),
            dma((3,)),
            dma((3, 3, SLOTS)),
            dma((DATA,)),
            dma,
        ],
        compiler_params=pltpu.CompilerParams(collective_id=0, has_side_effects=True, vmem_limit_bytes=50 * 1024 * 1024),
    )(acts, cots, lens, w_qkv, w_out, w_up, w_down, gain_a, gain_m)


def write_kernel(acts_ref, tiles_ref, gain_ref, out_ref, gqkv_ref, gout_ref, gup_ref, gdown_ref, gga_ref, ggm_ref,
                 out_sem, put_sem):
    give = pltpu.make_async_copy(acts_ref, out_ref, out_sem)
    give.start()
    row = 0
    dsts = (gdown_ref, gup_ref, gqkv_ref, gout_ref)
    for dst in dsts:
        for at_row in range(0, dst.shape[0], TILE):
            for at_col in range(0, dst.shape[1], D):
                pltpu.make_async_copy(tiles_ref.at[row:row + TILE], dst.at[at_row:at_row + TILE, at_col:at_col + D],
                                      put_sem).start()
                row += TILE
    gga_ref[...] = gain_ref[0:1, :]
    ggm_ref[...] = gain_ref[1:2, :]
    give.wait()
    pltpu.make_async_copy(tiles_ref, tiles_ref, put_sem).wait()


def write_out(acts, tiles, gains):
    any_spec = pl.BlockSpec(memory_space=pl.ANY)
    vmem_spec = pl.BlockSpec(memory_space=pltpu.VMEM)
    dma = pltpu.SemaphoreType.DMA
    return pl.pallas_call(
        write_kernel,
        out_shape=(
            jax.ShapeDtypeStruct(acts.shape, BF16),
            jax.ShapeDtypeStruct((D, 3 * D), F32),
            jax.ShapeDtypeStruct((D, D), F32),
            jax.ShapeDtypeStruct((D, FFN), F32),
            jax.ShapeDtypeStruct((FFN, D), F32),
            jax.ShapeDtypeStruct((1, D), F32),
            jax.ShapeDtypeStruct((1, D), F32),
        ),
        in_specs=[any_spec, any_spec, vmem_spec],
        out_specs=[any_spec] * 5 + [vmem_spec] * 2,
        scratch_shapes=[dma, dma],
        compiler_params=pltpu.CompilerParams(vmem_limit_bytes=4 * 1024 * 1024),
    )(acts, tiles, gains)


def solution(mesh):
    row_spec = P(('data', 'pipe'))
    stage_spec = P('pipe')

    def device_pass(acts_in, cot_out, seq_lens, w_qkv, w_out, w_up, w_down, gain_attn, gain_mlp):
        outs = run_pass(acts_in.reshape(-1, D), cot_out.reshape(-1, D), seq_lens, w_qkv.reshape(D, 3 * D),
                        w_out.reshape(D, D), w_up.reshape(D, FFN), w_down.reshape(FFN, D),
                        gain_attn, gain_mlp)
        acts_out, g_qkv, g_out, g_up, g_down, g_ga, g_gm = write_out(*outs)
        grads = (g_qkv.reshape(w_qkv.shape), g_out.reshape(w_out.shape), g_up.reshape(w_up.shape), g_down.reshape(w_down.shape),
                 g_ga, g_gm)
        return (acts_out.reshape(acts_in.shape),) + grads

    return jax.shard_map(device_pass, mesh=mesh, in_specs=(row_spec, row_spec, row_spec) + (stage_spec,) * 6, out_specs=(row_spec,) + (stage_spec,) * 6, check_vma=False)
```

```python
import functools
import jax
import jax.numpy as jnp
from jax import lax
from jax.experimental import pallas as pl
from jax.experimental.pallas import tpu as pltpu
from jax.sharding import PartitionSpec as P

NORM_EPS = 1e-5
MESH = pl.DeviceIdType.MESH
F32 = jnp.float32
BF16 = jnp.bfloat16
SEQ = 64
HEAD = 64
D = 512
FFN = 2048
PIPE = 4
DATA = 8
LINE = 4
TILE = 128
PART_B = 64
UNITS_A = 30
EXTRA = 5
UNITS_X = UNITS_A // EXTRA
SLOTS = 4
SEQ_MB = 4
PAIRS = 4


def dot_nn(lhs, rhs):
    return lax.dot_general(lhs, rhs, (((1,), (0,)), ((), ())), preferred_element_type=F32)


def dot_nt(lhs, rhs):
    return lax.dot_general(lhs, rhs, (((1,), (1,)), ((), ())), preferred_element_type=F32)


def dot_tn(lhs, rhs):
    return lax.dot_general(lhs, rhs, (((0,), (0,)), ((), ())), preferred_element_type=F32)


def pass_kernel(n_seq, acts_ref, cot_ref, lens_ref, wqkv_hbm, wout_hbm, wup_hbm, wdown_hbm, ga_ref, gm_ref,
                out_ref, gp_s, gain_ref,
                wqkv, wout, wup, wdown, lens_buf, xin, cin, hout, na_s, qkv_s, ctx_s, mid_s, nm_s, gelu_s,
                dpre_s, dmid_s, p_s, s_scr, gain_acc, gain_all, ya_buf, la_buf, ra_buf, yb_buf, lb_buf, rb_buf, yx_buf, lx_buf, rx_buf,
                ya_out, la_out, ra_out, yb_out, lb_out, rb_out, yx_out, lx_out, rx_out,
                w_sem, in_sem, x_sem, c_sem, len_sem, send_sem, home_sem, sum_recv, sum_send, part_send, gain_recv, gain_send):
    pos = lax.axis_index('pipe')
    rep = lax.axis_index('data')
    rep_z, rep_y = rep // 2, rep % 2
    n_tok = n_seq * SEQ
    n_mb = n_seq // SEQ_MB
    n_own = n_seq // PIPE
    own_slab = pl.ds(pos * n_own, n_own)
    for seq in range(n_own):
        lens_buf[pos * n_own + seq] = jnp.full((8, 128), lens_ref[seq], jnp.int32)
    last = PIPE - 1

    w_copies = [pltpu.make_async_copy(src, dst, w_sem.at[idx]) for idx, (src, dst) in enumerate(
        ((wqkv_hbm, wqkv), (wout_hbm, wout), (wup_hbm, wup), (wdown_hbm, wdown)))]
    for w_copy in w_copies:
        w_copy.start()

    barrier = pltpu.get_barrier_semaphore()
    for step in range(1, PIPE):
        pl.semaphore_signal(barrier, inc=1, device_id={'pipe': (pos + step) % PIPE}, device_id_type=MESH)
    for step in range(1, DATA):
        pl.semaphore_signal(barrier, inc=1, device_id={'data': (rep + step) % DATA}, device_id_type=MESH)
    pl.semaphore_wait(barrier, PIPE - 1 + DATA - 1)

    def first_seq(mb, size):
        return mb * size

    def rows_of(mb, size):
        return pl.ds(pl.multiple_of(first_seq(mb, size) * SEQ, SEQ), size * SEQ)

    def seq_rows(mb, size, seq):
        return pl.ds(pl.multiple_of((first_seq(mb, size) + seq) * SEQ, SEQ), SEQ)

    def part_rows(mb, size, part):
        return pl.ds(pl.multiple_of(part * n_tok + first_seq(mb, size) * SEQ, SEQ), size * SEQ)

    def send_to(src, dst, send, recv, target):
        pltpu.make_async_remote_copy(src_ref=src, dst_ref=dst, send_sem=send, recv_sem=recv,
                                     device_id={'pipe': target}, device_id_type=MESH).start()

    def place(src, dst, send, recv, target):
        @pl.when(target == pos)
        def _():
            pltpu.make_async_copy(src, dst, recv).start()

        @pl.when(target != pos)
        def _():
            send_to(src, dst, send, recv, target)

    for step in range(1, PIPE):
        send_to(lens_buf.at[own_slab], lens_buf.at[own_slab], in_sem.at[step - 1], len_sem.at[pos], (pos + step) % PIPE)
    spread = []
    for src, dst, sem, target in ((acts_ref, xin, x_sem, 0), (cot_ref, cin, c_sem, last)):
        for seq in range(n_own):
            at = pos * n_own + seq
            mb = at // SEQ_MB
            spread.append((src.at[pl.ds(seq * SEQ, SEQ)], dst.at[pl.ds(pl.multiple_of(at * SEQ, SEQ), SEQ)],
                           in_sem.at[PIPE - 1 + len(spread)], sem.at[mb], target))
    for item in spread:
        place(*item)

    lane = lax.broadcasted_iota(jnp.int32, (SEQ, 128), 1)
    row = lax.broadcasted_iota(jnp.int32, (SEQ, 128), 0)
    first = lane < HEAD
    key_pos = jnp.where(first, lane, lane - HEAD)
    lane_row = lax.broadcasted_iota(jnp.int32, (1, 128), 1)
    take_a = jnp.where(lane_row < HEAD, 1.0, 0.0).astype(BF16)
    take_b = jnp.where(lane_row < HEAD, 0.0, 1.0).astype(BF16)

    def blocks(pair_cols):
        return jnp.concatenate([pair_cols * take_a, pair_cols * take_b], axis=0)

    def halves_sum(arr):
        sum_a = jnp.sum(jnp.where(first[None], arr, 0.0), axis=-1, keepdims=True)
        sum_b = jnp.sum(jnp.where(first[None], 0.0, arr), axis=-1, keepdims=True)
        return sum_a, sum_b

    def lens_of(mb, size, seq):
        return lens_buf[first_seq(mb, size) + seq][0:1, :]

    def valid_mask(lens_row):
        ok = jnp.where(row < lens_row, 1.0, 0.0)
        return jnp.concatenate([ok] * (D // 128), axis=1)

    def inv_rms(val):
        return lax.rsqrt(jnp.mean(val * val, axis=-1, keepdims=True) + NORM_EPS)

    def forward(size, mb, _):
        rows = rows_of(mb, size)
        start = first_seq(mb, size)

        for home in range(PIPE):
            @pl.when((mb == home * n_own // size) & (home != pos))
            def _(home=home):
                slab = lens_buf.at[pl.ds(home * n_own, n_own)]
                pltpu.make_async_copy(slab, slab, len_sem.at[home]).wait()

        x_view = xin.at[rows]
        pltpu.make_async_copy(x_view, x_view, x_sem.at[mb]).wait()
        gain_a = ga_ref[...].astype(F32)
        hid = xin[rows, :].astype(F32)
        normed = (hid * inv_rms(hid) * gain_a).astype(BF16)
        na_s[rows, :] = normed
        for part in range(3):
            cols = slice(part * D, (part + 1) * D)
            qkv_s[rows, cols] = dot_nn(normed, wqkv[:, cols]).astype(BF16)

        for seq in range(size):
            for pair in range(PAIRS):
                q_cols = qkv_s[seq_rows(mb, size, seq), pair * 128:(pair + 1) * 128]
                k_cols = qkv_s[seq_rows(mb, size, seq), D + pair * 128:D + (pair + 1) * 128]
                spot = (seq * PAIRS + pair) * SEQ
                s_scr[spot:spot + SEQ, :] = dot_nt(q_cols, blocks(k_cols))
        for seq in range(size):
            visible = (key_pos <= row) & (key_pos < lens_of(mb, size, seq))
            spot = seq * PAIRS * SEQ
            scores = s_scr[spot:spot + PAIRS * SEQ, :].reshape(PAIRS, SEQ, 128) * (HEAD ** -0.5)
            scores = jnp.where(visible[None], scores, -1e30)
            max_a = jnp.max(jnp.where(first[None], scores, -3e38), axis=-1, keepdims=True)
            max_b = jnp.max(jnp.where(first[None], -3e38, scores), axis=-1, keepdims=True)
            expd = jnp.exp(scores - jnp.where(first[None], max_a, max_b))
            sum_a, sum_b = halves_sum(expd)
            probs = expd * jnp.where(first[None], 1.0 / sum_a, 1.0 / sum_b)
            p_rows = pl.ds(pl.multiple_of(start * PAIRS * SEQ + spot, SEQ), PAIRS * SEQ)
            p_s[p_rows, :] = probs.reshape(PAIRS * SEQ, 128)
        for seq in range(size):
            for pair in range(PAIRS):
                v_cols = qkv_s[seq_rows(mb, size, seq), 2 * D + pair * 128:2 * D + (pair + 1) * 128]
                p_rows = pl.ds(pl.multiple_of((start * PAIRS + seq * PAIRS + pair) * SEQ, SEQ), SEQ)
                ctx_s[seq_rows(mb, size, seq), pair * 128:(pair + 1) * 128] = dot_nn(
                    p_s[p_rows, :].astype(BF16), blocks(v_cols)).astype(BF16)
        mid = (hid + dot_nn(ctx_s[rows, :], wout[...])).astype(BF16)
        mid_s[rows, :] = mid
        mid_f = mid.astype(F32)
        normed_m = (mid_f * inv_rms(mid_f) * gm_ref[...].astype(F32)).astype(BF16)
        nm_s[rows, :] = normed_m
        for part in range(FFN // D):
            cols = slice(part * D, (part + 1) * D)
            pre = dot_nn(normed_m, wup[:, cols])
            cdf = 0.5 + 0.5 * lax.erf(pre * (0.5 ** 0.5))
            gelu_s[rows, cols] = (pre * cdf).astype(BF16)
            gp_s[part_rows(mb, size, part), :] = cdf + pre * (jnp.exp(pre * pre * -0.5) * 0.3989422804014327)
        top = mid_f + dot_nn(gelu_s[rows, :], wdown[...])
        for seq in range(size):
            mask = valid_mask(jnp.where(pos == last, lens_of(mb, size, seq), SEQ))
            piece = top[seq * SEQ:(seq + 1) * SEQ, :].astype(BF16)
            hout[seq_rows(mb, size, seq), :] = jnp.where(mask > 0.0, piece.astype(F32), 0.0).astype(BF16)

        h_view = hout.at[rows]

        @pl.when(pos < last)
        def _():
            send_to(h_view, xin.at[rows], send_sem.at[mb], x_sem.at[mb], pos + 1)

        @pl.when(pos == last)
        def _():
            for seq in range(size):
                at = start + seq
                home = at // n_own
                s_view = hout.at[seq_rows(mb, size, seq)]
                o_view = out_ref.at[pl.ds(pl.multiple_of((at % n_own) * SEQ, SEQ), SEQ)]

                @pl.when(home == pos)
                def _(s_view=s_view, o_view=o_view):
                    pltpu.make_async_copy(s_view, o_view, send_sem.at[mb]).start()

                @pl.when(home != pos)
                def _(s_view=s_view, o_view=o_view, home=home):
                    send_to(s_view, o_view, send_sem.at[mb], home_sem, home)

        return 0

    for w_copy in w_copies:
        w_copy.wait()
    lax.fori_loop(0, n_mb, functools.partial(forward, SEQ_MB), 0)

    def sent(size, mb, _):
        h_view = hout.at[rows_of(mb, size)]
        pltpu.make_async_copy(h_view, h_view, send_sem.at[mb]).wait()
        return 0

    gain_acc[...] = jnp.zeros_like(gain_acc)

    def norm_back(hid, gain, d_normed):
        inv = inv_rms(hid)
        unit = hid * inv
        d_gain = jnp.sum((d_normed * unit).reshape(hid.shape[0] // 8, 8, D), axis=0)
        scaled = d_normed * gain
        return inv * (scaled - unit * jnp.mean(unit * scaled, axis=-1, keepdims=True)), d_gain

    def backward(size, mb, _):
        rows = rows_of(mb, size)
        start = first_seq(mb, size)
        c_view = cin.at[rows]
        pltpu.make_async_copy(c_view, c_view, c_sem.at[mb]).wait()

        for seq in range(size):
            mask = valid_mask(lens_of(mb, size, seq))
            cin[seq_rows(mb, size, seq), :] = jnp.where(mask > 0.0, cin[seq_rows(mb, size, seq), :].astype(F32), 0.0).astype(BF16)
        d_top = cin[rows, :]
        for part in range(FFN // D):
            cols = slice(part * D, (part + 1) * D)
            d_gelu = dot_nt(d_top, wdown[cols, :])
            dpre_s[rows, cols] = (d_gelu * gp_s[part_rows(mb, size, part), :]).astype(BF16)
        d_nm = dot_nt(dpre_s[rows, :], wup[...])
        d_add, d_gain = norm_back(mid_s[rows, :].astype(F32), gm_ref[...].astype(F32), d_nm)
        gain_acc[1] += d_gain
        d_mid = d_top.astype(F32) + d_add
        d_mid_bf = d_mid.astype(BF16)
        dmid_s[rows, :] = d_mid_bf
        d_ctx = dot_nt(d_mid_bf, wout[...]).astype(BF16)
        for seq in range(size):
            for pair in range(PAIRS):
                v_cols = qkv_s[seq_rows(mb, size, seq), 2 * D + pair * 128:2 * D + (pair + 1) * 128]
                dc = d_ctx[seq * SEQ:(seq + 1) * SEQ, pair * 128:(pair + 1) * 128]
                spot = (seq * PAIRS + pair) * SEQ
                p_rows = pl.ds(pl.multiple_of(start * PAIRS * SEQ + spot, SEQ), SEQ)
                s_scr[spot:spot + SEQ, :] = dot_nt(dc, blocks(v_cols))
                both = dot_tn(p_s[p_rows, :].astype(BF16), dc)
                qkv_s[seq_rows(mb, size, seq), 2 * D + pair * 128:2 * D + (pair + 1) * 128] = jnp.where(
                    first, both[:SEQ], both[SEQ:]).astype(BF16)
        for seq in range(size):
            spot = seq * PAIRS * SEQ
            p_rows = pl.ds(pl.multiple_of(start * PAIRS * SEQ + spot, SEQ), PAIRS * SEQ)
            probs = p_s[p_rows, :].reshape(PAIRS, SEQ, 128)
            d_probs = s_scr[spot:spot + PAIRS * SEQ, :].reshape(PAIRS, SEQ, 128)
            sum_a, sum_b = halves_sum(probs * d_probs)
            d_scores = probs * (d_probs - jnp.where(first[None], sum_a, sum_b)) * (HEAD ** -0.5)
            s_scr[spot:spot + PAIRS * SEQ, :] = d_scores.reshape(PAIRS * SEQ, 128)
        for seq in range(size):
            for pair in range(PAIRS):
                q_at = slice(pair * 128, (pair + 1) * 128)
                k_at = slice(D + pair * 128, D + (pair + 1) * 128)
                q_cols = qkv_s[seq_rows(mb, size, seq), q_at]
                k_cols = qkv_s[seq_rows(mb, size, seq), k_at]
                spot = (seq * PAIRS + pair) * SEQ
                d_sc = s_scr[spot:spot + SEQ, :].astype(BF16)
                both = dot_tn(d_sc, q_cols)
                qkv_s[seq_rows(mb, size, seq), q_at] = dot_nn(d_sc, blocks(k_cols)).astype(BF16)
                qkv_s[seq_rows(mb, size, seq), k_at] = jnp.where(first, both[:SEQ], both[SEQ:]).astype(BF16)
        d_na = dot_nt(qkv_s[rows, :], wqkv[...])
        d_add, d_gain = norm_back(xin[rows, :].astype(F32), ga_ref[...].astype(F32), d_na)
        gain_acc[0] += d_gain

        @pl.when(pos > 0)
        def _():
            sent(size, mb, 0)
            hout[rows, :] = (d_mid + d_add).astype(BF16)
            send_to(hout.at[rows], cin.at[rows], send_sem.at[mb], c_sem.at[mb], pos - 1)

        return 0

    lax.fori_loop(0, n_mb, functools.partial(backward, SEQ_MB), 0)

    gain_all[rep] = jnp.concatenate([jnp.sum(gain_acc[0], axis=0, keepdims=True), jnp.sum(gain_acc[1], axis=0, keepdims=True),
                                     jnp.zeros((6, D), F32)], axis=0)
    for step in range(1, DATA):
        pltpu.make_async_remote_copy(src_ref=gain_all.at[rep], dst_ref=gain_all.at[rep], send_sem=gain_send,
                                     recv_sem=gain_recv.at[rep], device_id={'data': (rep + step) % DATA},
                                     device_id_type=MESH).start()

    per_tile = TILE // PART_B
    n_down, n_up, n_qkv = FFN // TILE, (D // TILE) * (FFN // D), (D // TILE) * 3

    def tile_kinds(tile):
        up, qkv, out = tile - n_down, tile - n_down - n_up, tile - n_down - n_up - n_qkv
        return (
            (tile < n_down, gelu_s, cin, tile, 0),
            ((up >= 0) & (qkv < 0), nm_s, dpre_s, up // (FFN // D), up % (FFN // D)),
            ((qkv >= 0) & (out < 0), na_s, qkv_s, qkv // 3, qkv % 3),
            (out >= 0, ctx_s, dmid_s, out, 0),
        )

    def tile_at(tile):
        return pl.ds(pl.multiple_of(tile * TILE, TILE), TILE)

    def compute_tile(tile):
        for cond, lhs, rhs, at_row, at_col in tile_kinds(tile):
            @pl.when(cond)
            def _(lhs=lhs, rhs=rhs, at_row=at_row, at_col=at_col):
                cols = pl.ds(0, D) if rhs.shape[1] == D else pl.ds(pl.multiple_of(at_col * D, D), D)
                gp_s[tile_at(tile), :] = dot_tn(lhs[:, pl.ds(pl.multiple_of(at_row * TILE, TILE), TILE)], rhs[:, cols])

    to_y, to_right, to_left = rep + 1 - 2 * rep_y, rep + 2, rep - 2

    def part_done(src, colour, link, slot):
        pltpu.make_async_copy(src, src, part_send.at[colour, link, slot]).wait()

    def ship_part(unit, slot, src, dst, colour, link, target, value):
        @pl.when(unit >= SLOTS)
        def _():
            part_done(src, colour, link, slot)

        src[...] = value
        pltpu.make_async_remote_copy(src_ref=src, dst_ref=dst, send_sem=part_send.at[colour, link, slot],
                                     recv_sem=sum_recv.at[colour, link, slot], device_id={'data': target},
                                     device_id_type=MESH).start()

    def ship(src, dst, link, recv, target):
        pltpu.make_async_remote_copy(src_ref=src, dst_ref=dst, send_sem=sum_send.at[link], recv_sem=recv,
                                     device_id={'data': target}, device_id_type=MESH).start()

    def arrived(view, recv):
        pltpu.make_async_copy(view, view, recv).wait()

    def gp_rows(start, size):
        return pl.ds(pl.multiple_of(start, 8), size)

    def line_actions(zz, colour, block, size, buf_l, buf_r, out_l, out_r, hop_rs, hop_ag):
        chunk = size // LINE
        own, above = zz * chunk, (zz + 1) * chunk

        def rs_right(unit, slot):
            at = block(unit)
            if zz > 0:
                arrived(buf_l.at[slot, own:size], sum_recv.at[colour, 1, slot])
                gp_s[gp_rows(at + own, chunk), :] += buf_l[slot, own:above, :]
            if zz < LINE - 1:
                value = gp_s[gp_rows(at + above, size - above), :]
                if zz > 0:
                    value = value + buf_l[slot, above:size, :]
                ship_part(unit, slot, out_r.at[slot, above:size], buf_l.at[slot, above:size], colour, 1, to_right, value)

        def rs_left(unit, slot):
            at = block(unit)
            if zz < LINE - 1:
                arrived(buf_r.at[slot, 0:above], sum_recv.at[colour, 2, slot])
                gp_s[gp_rows(at + own, chunk), :] += buf_r[slot, own:above, :]
            if zz > 0:
                value = gp_s[gp_rows(at, own), :]
                if zz < LINE - 1:
                    value = value + buf_r[slot, 0:own, :]
                ship_part(unit, slot, out_l.at[slot, 0:own], buf_r.at[slot, 0:own], colour, 2, to_left, value)

        def ag_right(unit, slot):
            at = block(unit)
            if zz > 0:
                arrived(gp_s.at[gp_rows(at, own)], sum_recv.at[colour, 3, slot])
            if zz < LINE - 1:
                view = gp_s.at[gp_rows(at, above)]
                ship(view, view, 1, sum_recv.at[colour, 3, slot], to_right)

        def ag_left(unit, slot):
            at = block(unit)
            if zz < LINE - 1:
                arrived(gp_s.at[gp_rows(at + above, size - above)], sum_recv.at[colour, 4, slot])
            if zz > 0:
                view = gp_s.at[gp_rows(at + own, size - own)]
                ship(view, view, 2, sum_recv.at[colour, 4, slot], to_left)

        return ([(hop_rs + zz, rs_right), (hop_rs + LINE - 1 - zz, rs_left)],
                [(hop_ag + zz, ag_right), (hop_ag + LINE - 1 - zz, ag_left)])

    half_a, part_b = TILE // 2, PART_B // LINE
    half_b = part_b // 2

    def actions_a(zz):
        def mine(unit):
            return unit * TILE + rep_y * half_a

        def theirs(unit):
            return unit * TILE + (1 - rep_y) * half_a

        def y_send(unit, slot):
            ship_part(unit, slot, ya_out.at[slot], ya_buf.at[slot], 0, 0, to_y, gp_s[gp_rows(theirs(unit), half_a), :])

        def y_add(unit, slot):
            arrived(ya_buf.at[slot], sum_recv.at[0, 0, slot])
            gp_s[gp_rows(mine(unit), half_a), :] += ya_buf[slot]

        def y_give(unit, slot):
            view = gp_s.at[gp_rows(mine(unit), half_a)]
            ship(view, view, 0, sum_recv.at[0, 5, slot], to_y)

        def finish(unit, slot):
            arrived(gp_s.at[gp_rows(theirs(unit), half_a)], sum_recv.at[0, 5, slot])

        scatter, gather = line_actions(zz, 0, mine, half_a, la_buf, ra_buf, la_out, ra_out, 1, 4)
        return [(0, y_send), (1, y_add)] + scatter + gather + [(7, y_give), (8, finish)]

    def actions_b(zz, colour, base, bufs, outs):
        y_buf, l_buf, r_buf = bufs
        y_out, l_out, r_out = outs

        def block(unit):
            return UNITS_A * TILE + (base + unit) * PART_B

        def mine(unit):
            return block(unit) + zz * part_b + rep_y * half_b

        def theirs(unit):
            return block(unit) + zz * part_b + (1 - rep_y) * half_b

        def y_send(unit, slot):
            ship_part(unit, slot, y_out.at[slot], y_buf.at[slot], colour, 0, to_y, gp_s[gp_rows(theirs(unit), half_b), :])

        def y_add(unit, slot):
            arrived(y_buf.at[slot], sum_recv.at[colour, 0, slot])
            gp_s[gp_rows(mine(unit), half_b), :] += y_buf[slot]
            view = gp_s.at[gp_rows(mine(unit), half_b)]
            ship(view, view, 0, sum_recv.at[colour, 5, slot], to_y)

        def y_done(unit, slot):
            arrived(gp_s.at[gp_rows(theirs(unit), half_b)], sum_recv.at[colour, 5, slot])

        scatter, gather = line_actions(zz, colour, block, PART_B, l_buf, r_buf, l_out, r_out, 0, 5)
        return scatter + [(3, y_send), (4, y_add), (5, y_done)] + gather

    def unit_of(colour, tick):
        inside = (tick >= 0) & (tick < UNITS_A)
        if colour < 2:
            return inside, tick
        return inside & (tick % EXTRA == 0), tick // EXTRA

    def run_actions(tick, hops):
        for zz in range(LINE):
            @pl.when(rep_z == zz)
            def _(zz=zz):
                todo = (
                    actions_a(zz),
                    actions_b(zz, 1, 0, (yb_buf, lb_buf, rb_buf), (yb_out, lb_out, rb_out)),
                    actions_b(zz, 2, UNITS_A, (yx_buf, lx_buf, rx_buf), (yx_out, lx_out, rx_out)),
                )
                for want in hops:
                    for colour in range(3):
                        fns = [fn for hop, fn in todo[colour] if hop == want]
                        if not fns:
                            continue
                        fresh, unit = unit_of(colour, tick - want)

                        @pl.when(fresh)
                        def _(fns=fns, unit=unit):
                            for fn in fns:
                                fn(unit, unit % SLOTS)

    def compute_for(tick):
        @pl.when(tick < UNITS_A)
        def _():
            compute_tile(tick)

        for colour, base in ((1, 0), (2, UNITS_A)):
            fresh, unit = unit_of(colour, tick)

            @pl.when(fresh & (unit % per_tile == 0))
            def _(unit=unit, base=base):
                compute_tile(UNITS_A + (base + unit) // per_tile)

    compute_for(0)

    def tick_step(tick, _):
        run_actions(tick, [0])
        compute_for(tick + 1)
        run_actions(tick, range(1, 9))
        return 0

    lax.fori_loop(0, UNITS_A + 8, tick_step, 0)

    def sent_all(link, size):
        view = gp_s.at[pl.ds(0, size)]
        pltpu.make_async_copy(view, view, sum_send.at[link]).wait()

    for zz in range(LINE):
        @pl.when(rep_z == zz)
        def _(zz=zz):
            line_rows = UNITS_A * (half_a // LINE) + (UNITS_A + UNITS_X) * part_b
            sent_all(0, UNITS_A * half_a + (UNITS_A + UNITS_X) * half_b)
            if zz < LINE - 1:
                sent_all(1, line_rows * (zz + 1))
            if zz > 0:
                sent_all(2, line_rows * (LINE - zz))
            for slot in range(SLOTS):
                for colour, (out_y, out_l, out_r) in enumerate(
                        ((ya_out, la_out, ra_out), (yb_out, lb_out, rb_out), (yx_out, lx_out, rx_out))):
                    size = out_l.shape[1]
                    part_done(out_y.at[slot], colour, 0, slot)
                    if zz < LINE - 1:
                        part_done(out_r.at[slot, (zz + 1) * size // LINE:size], colour, 1, slot)
                    if zz > 0:
                        part_done(out_l.at[slot, 0:zz * size // LINE], colour, 2, slot)

    for step in range(1, DATA):
        peer = (rep + step) % DATA
        pltpu.make_async_copy(gain_all.at[peer], gain_all.at[peer], gain_recv.at[peer]).wait()
    total = gain_all[0]
    for peer in range(1, DATA):
        total = total + gain_all[peer]
    gain_ref[...] = total
    pltpu.make_async_copy(gain_all.at[pl.ds(0, DATA - 1)], gain_all.at[pl.ds(0, DATA - 1)], gain_send).wait()

    lax.fori_loop(0, n_mb, functools.partial(sent, SEQ_MB), 0)

    @pl.when(pos < last)
    def _():
        pltpu.make_async_copy(out_ref, out_ref, home_sem).wait()

    for step in range(1, PIPE):
        pltpu.make_async_copy(lens_buf.at[own_slab], lens_buf.at[own_slab], in_sem.at[step - 1]).wait()
    for src, _, send, _, target in spread:
        @pl.when(target != pos)
        def _(src=src, send=send):
            pltpu.make_async_copy(src, src, send).wait()


def run_pass(acts, cots, lens, w_qkv, w_out, w_up, w_down, gain_a, gain_m):
    n_tok = acts.shape[0] * PIPE
    n_seq = n_tok // SEQ
    n_mb = n_seq // SEQ_MB
    any_spec = pl.BlockSpec(memory_space=pl.ANY)
    vmem_spec = pl.BlockSpec(memory_space=pltpu.VMEM)
    dma = pltpu.SemaphoreType.DMA
    return pl.pallas_call(
        functools.partial(pass_kernel, n_seq),
        out_shape=(
            pltpu.VMEM(acts.shape, BF16),
            pltpu.VMEM((n_tok * FFN // D, D), F32),
            pltpu.VMEM((8, D), F32),
        ),
        in_specs=[any_spec] * 2 + [pl.BlockSpec(memory_space=pltpu.SMEM)] + [any_spec] * 4 + [vmem_spec] * 2,
        out_specs=[vmem_spec] * 3,
        scratch_shapes=[
            pltpu.VMEM((D, 3 * D), BF16),
            pltpu.VMEM((D, D), BF16),
            pltpu.VMEM((D, FFN), BF16),
            pltpu.VMEM((FFN, D), BF16),
            pltpu.VMEM((n_seq, 8, 128), jnp.int32),
            pltpu.VMEM((n_tok, D), BF16),
            pltpu.VMEM((n_tok, D), BF16),
            pltpu.VMEM((n_tok, D), BF16),
            pltpu.VMEM((n_tok, D), BF16),
            pltpu.VMEM((n_tok, 3 * D), BF16),
            pltpu.VMEM((n_tok, D), BF16),
            pltpu.VMEM((n_tok, D), BF16),
            pltpu.VMEM((n_tok, D), BF16),
            pltpu.VMEM((n_tok, FFN), BF16),
            pltpu.VMEM((n_tok, FFN), BF16),
            pltpu.VMEM((n_tok, D), BF16),
            pltpu.VMEM((n_tok * PAIRS, 128), F32),
            pltpu.VMEM((SEQ_MB * PAIRS * SEQ, 128), F32),
            pltpu.VMEM((2, 8, D), F32),
            pltpu.VMEM((DATA, 8, D), F32),
        ] + [
            pltpu.VMEM((SLOTS, size, D), F32)
            for size in ((TILE // 2,) * 3 + (PART_B // LINE // 2, PART_B, PART_B) * 2) * 2
        ] + [
            dma((4,)),
            dma((2 * (n_seq // PIPE) + PIPE - 1,)),
            dma((n_mb,)),
            dma((n_mb,)),
            dma((PIPE,)),
            dma((n_mb,)),
            dma,
            dma((3, 6, SLOTS)),
            dma((3,)),
            dma((3, 3, SLOTS)),
            dma((DATA,)),
            dma,
        ],
        compiler_params=pltpu.CompilerParams(collective_id=0, has_side_effects=True, vmem_limit_bytes=50 * 1024 * 1024),
    )(acts, cots, lens, w_qkv, w_out, w_up, w_down, gain_a, gain_m)


def write_kernel(acts_ref, tiles_ref, gain_ref, out_ref, gqkv_ref, gout_ref, gup_ref, gdown_ref, gga_ref, ggm_ref,
                 out_sem, put_sem):
    give = pltpu.make_async_copy(acts_ref, out_ref, out_sem)
    give.start()
    row = 0
    dsts = (gdown_ref, gup_ref, gqkv_ref, gout_ref)
    for dst in dsts:
        for at_row in range(0, dst.shape[0], TILE):
            for at_col in range(0, dst.shape[1], D):
                pltpu.make_async_copy(tiles_ref.at[row:row + TILE], dst.at[at_row:at_row + TILE, at_col:at_col + D],
                                      put_sem).start()
                row += TILE
    gga_ref[...] = gain_ref[0:1, :]
    ggm_ref[...] = gain_ref[1:2, :]
    give.wait()
    pltpu.make_async_copy(tiles_ref, tiles_ref, put_sem).wait()


def write_out(acts, tiles, gains):
    any_spec = pl.BlockSpec(memory_space=pl.ANY)
    vmem_spec = pl.BlockSpec(memory_space=pltpu.VMEM)
    dma = pltpu.SemaphoreType.DMA
    return pl.pallas_call(
        write_kernel,
        out_shape=(
            jax.ShapeDtypeStruct(acts.shape, BF16),
            jax.ShapeDtypeStruct((D, 3 * D), F32),
            jax.ShapeDtypeStruct((D, D), F32),
            jax.ShapeDtypeStruct((D, FFN), F32),
            jax.ShapeDtypeStruct((FFN, D), F32),
            jax.ShapeDtypeStruct((1, D), F32),
            jax.ShapeDtypeStruct((1, D), F32),
        ),
        in_specs=[any_spec, any_spec, vmem_spec],
        out_specs=[any_spec] * 5 + [vmem_spec] * 2,
        scratch_shapes=[dma, dma],
        compiler_params=pltpu.CompilerParams(vmem_limit_bytes=4 * 1024 * 1024),
    )(acts, tiles, gains)


def solution(mesh):
    row_spec = P(('data', 'pipe'))
    stage_spec = P('pipe')

    def device_pass(acts_in, cot_out, seq_lens, w_qkv, w_out, w_up, w_down, gain_attn, gain_mlp):
        outs = run_pass(acts_in.reshape(-1, D), cot_out.reshape(-1, D), seq_lens, w_qkv.reshape(D, 3 * D),
                        w_out.reshape(D, D), w_up.reshape(D, FFN), w_down.reshape(FFN, D),
                        gain_attn, gain_mlp)
        acts_out, g_qkv, g_out, g_up, g_down, g_ga, g_gm = write_out(*outs)
        grads = (g_qkv.reshape(w_qkv.shape), g_out.reshape(w_out.shape), g_up.reshape(w_up.shape), g_down.reshape(w_down.shape),
                 g_ga, g_gm)
        return (acts_out.reshape(acts_in.shape),) + grads

    return jax.shard_map(device_pass, mesh=mesh, in_specs=(row_spec, row_spec, row_spec) + (stage_spec,) * 6, out_specs=(row_spec,) + (stage_spec,) * 6, check_vma=False)
```

```python
import functools
import jax
import jax.numpy as jnp
from jax import lax
from jax.experimental import pallas as pl
from jax.experimental.pallas import tpu as pltpu
from jax.sharding import PartitionSpec as P

NORM_EPS = 1e-5
MESH = pl.DeviceIdType.MESH
F32 = jnp.float32
BF16 = jnp.bfloat16
SEQ = 64
HEAD = 64
D = 512
FFN = 2048
PIPE = 4
DATA = 8
LINE = 4
TILE = 128
PART_B = 64
UNITS_A = 30
EXTRA = 5
UNITS_X = UNITS_A // EXTRA
SLOTS = 4
SEQ_MB = 6
PAIRS = 4


def dot_nn(lhs, rhs):
    return lax.dot_general(lhs, rhs, (((1,), (0,)), ((), ())), preferred_element_type=F32)


def dot_nt(lhs, rhs):
    return lax.dot_general(lhs, rhs, (((1,), (1,)), ((), ())), preferred_element_type=F32)


def dot_tn(lhs, rhs):
    return lax.dot_general(lhs, rhs, (((0,), (0,)), ((), ())), preferred_element_type=F32)


def pass_kernel(n_seq, acts_ref, cot_ref, lens_ref, wqkv_hbm, wout_hbm, wup_hbm, wdown_hbm, ga_ref, gm_ref,
                out_ref, gp_s, gain_ref,
                wqkv, wout, wup, wdown, lens_buf, xin, cin, hout, na_s, qkv_s, ctx_s, mid_s, nm_s, gelu_s,
                dpre_s, dmid_s, p_s, s_scr, gain_acc, gain_all, ya_buf, la_buf, ra_buf, yb_buf, lb_buf, rb_buf, yx_buf, lx_buf, rx_buf,
                ya_out, la_out, ra_out, yb_out, lb_out, rb_out, yx_out, lx_out, rx_out,
                w_sem, in_sem, x_sem, c_sem, len_sem, send_sem, home_sem, sum_recv, sum_send, part_send, gain_recv, gain_send):
    pos = lax.axis_index('pipe')
    rep = lax.axis_index('data')
    rep_z, rep_y = rep // 2, rep % 2
    n_tok = n_seq * SEQ
    n_mb = n_seq // SEQ_MB
    n_own = n_seq // PIPE
    own_slab = pl.ds(pos * n_own, n_own)
    for seq in range(n_own):
        lens_buf[pos * n_own + seq] = jnp.full((8, 128), lens_ref[seq], jnp.int32)
    last = PIPE - 1

    w_copies = [pltpu.make_async_copy(src, dst, w_sem.at[idx]) for idx, (src, dst) in enumerate(
        ((wqkv_hbm, wqkv), (wout_hbm, wout), (wup_hbm, wup), (wdown_hbm, wdown)))]
    for w_copy in w_copies:
        w_copy.start()

    barrier = pltpu.get_barrier_semaphore()
    for step in range(1, PIPE):
        pl.semaphore_signal(barrier, inc=1, device_id={'pipe': (pos + step) % PIPE}, device_id_type=MESH)
    for step in range(1, DATA):
        pl.semaphore_signal(barrier, inc=1, device_id={'data': (rep + step) % DATA}, device_id_type=MESH)
    pl.semaphore_wait(barrier, PIPE - 1 + DATA - 1)

    def first_seq(mb, size):
        return mb * size

    def rows_of(mb, size):
        return pl.ds(pl.multiple_of(first_seq(mb, size) * SEQ, SEQ), size * SEQ)

    def seq_rows(mb, size, seq):
        return pl.ds(pl.multiple_of((first_seq(mb, size) + seq) * SEQ, SEQ), SEQ)

    def part_rows(mb, size, part):
        return pl.ds(pl.multiple_of(part * n_tok + first_seq(mb, size) * SEQ, SEQ), size * SEQ)

    def send_to(src, dst, send, recv, target):
        pltpu.make_async_remote_copy(src_ref=src, dst_ref=dst, send_sem=send, recv_sem=recv,
                                     device_id={'pipe': target}, device_id_type=MESH).start()

    def place(src, dst, send, recv, target):
        @pl.when(target == pos)
        def _():
            pltpu.make_async_copy(src, dst, recv).start()

        @pl.when(target != pos)
        def _():
            send_to(src, dst, send, recv, target)

    for step in range(1, PIPE):
        send_to(lens_buf.at[own_slab], lens_buf.at[own_slab], in_sem.at[step - 1], len_sem.at[pos], (pos + step) % PIPE)
    spread = []
    for src, dst, sem, target in ((acts_ref, xin, x_sem, 0), (cot_ref, cin, c_sem, last)):
        for seq in range(n_own):
            at = pos * n_own + seq
            mb = at // SEQ_MB
            spread.append((src.at[pl.ds(seq * SEQ, SEQ)], dst.at[pl.ds(pl.multiple_of(at * SEQ, SEQ), SEQ)],
                           in_sem.at[PIPE - 1 + len(spread)], sem.at[mb], target))
    for item in spread:
        place(*item)

    lane = lax.broadcasted_iota(jnp.int32, (SEQ, 128), 1)
    row = lax.broadcasted_iota(jnp.int32, (SEQ, 128), 0)
    first = lane < HEAD
    key_pos = jnp.where(first, lane, lane - HEAD)
    lane_row = lax.broadcasted_iota(jnp.int32, (1, 128), 1)
    take_a = jnp.where(lane_row < HEAD, 1.0, 0.0).astype(BF16)
    take_b = jnp.where(lane_row < HEAD, 0.0, 1.0).astype(BF16)

    def blocks(pair_cols):
        return jnp.concatenate([pair_cols * take_a, pair_cols * take_b], axis=0)

    def halves_sum(arr):
        sum_a = jnp.sum(jnp.where(first[None], arr, 0.0), axis=-1, keepdims=True)
        sum_b = jnp.sum(jnp.where(first[None], 0.0, arr), axis=-1, keepdims=True)
        return sum_a, sum_b

    def lens_of(mb, size, seq):
        return lens_buf[first_seq(mb, size) + seq][0:1, :]

    def valid_mask(lens_row):
        ok = jnp.where(row < lens_row, 1.0, 0.0)
        return jnp.concatenate([ok] * (D // 128), axis=1)

    def inv_rms(val):
        return lax.rsqrt(jnp.mean(val * val, axis=-1, keepdims=True) + NORM_EPS)

    def forward(size, mb, _):
        rows = rows_of(mb, size)
        start = first_seq(mb, size)

        for home in range(PIPE):
            @pl.when((mb == home * n_own // size) & (home != pos))
            def _(home=home):
                slab = lens_buf.at[pl.ds(home * n_own, n_own)]
                pltpu.make_async_copy(slab, slab, len_sem.at[home]).wait()

        x_view = xin.at[rows]
        pltpu.make_async_copy(x_view, x_view, x_sem.at[mb]).wait()
        gain_a = ga_ref[...].astype(F32)
        hid = xin[rows, :].astype(F32)
        normed = (hid * inv_rms(hid) * gain_a).astype(BF16)
        na_s[rows, :] = normed
        for part in range(3):
            cols = slice(part * D, (part + 1) * D)
            qkv_s[rows, cols] = dot_nn(normed, wqkv[:, cols]).astype(BF16)

        for seq in range(size):
            for pair in range(PAIRS):
                q_cols = qkv_s[seq_rows(mb, size, seq), pair * 128:(pair + 1) * 128]
                k_cols = qkv_s[seq_rows(mb, size, seq), D + pair * 128:D + (pair + 1) * 128]
                spot = (seq * PAIRS + pair) * SEQ
                s_scr[spot:spot + SEQ, :] = dot_nt(q_cols, blocks(k_cols))
        for seq in range(size):
            visible = (key_pos <= row) & (key_pos < lens_of(mb, size, seq))
            spot = seq * PAIRS * SEQ
            scores = s_scr[spot:spot + PAIRS * SEQ, :].reshape(PAIRS, SEQ, 128) * (HEAD ** -0.5)
            scores = jnp.where(visible[None], scores, -1e30)
            max_a = jnp.max(jnp.where(first[None], scores, -3e38), axis=-1, keepdims=True)
            max_b = jnp.max(jnp.where(first[None], -3e38, scores), axis=-1, keepdims=True)
            expd = jnp.exp(scores - jnp.where(first[None], max_a, max_b))
            sum_a, sum_b = halves_sum(expd)
            probs = expd * jnp.where(first[None], 1.0 / sum_a, 1.0 / sum_b)
            p_rows = pl.ds(pl.multiple_of(start * PAIRS * SEQ + spot, SEQ), PAIRS * SEQ)
            p_s[p_rows, :] = probs.reshape(PAIRS * SEQ, 128)
        for seq in range(size):
            for pair in range(PAIRS):
                v_cols = qkv_s[seq_rows(mb, size, seq), 2 * D + pair * 128:2 * D + (pair + 1) * 128]
                p_rows = pl.ds(pl.multiple_of((start * PAIRS + seq * PAIRS + pair) * SEQ, SEQ), SEQ)
                ctx_s[seq_rows(mb, size, seq), pair * 128:(pair + 1) * 128] = dot_nn(
                    p_s[p_rows, :].astype(BF16), blocks(v_cols)).astype(BF16)
        mid = (hid + dot_nn(ctx_s[rows, :], wout[...])).astype(BF16)
        mid_s[rows, :] = mid
        mid_f = mid.astype(F32)
        normed_m = (mid_f * inv_rms(mid_f) * gm_ref[...].astype(F32)).astype(BF16)
        nm_s[rows, :] = normed_m
        for part in range(FFN // D):
            cols = slice(part * D, (part + 1) * D)
            pre = dot_nn(normed_m, wup[:, cols])
            cdf = 0.5 + 0.5 * lax.erf(pre * (0.5 ** 0.5))
            gelu_s[rows, cols] = (pre * cdf).astype(BF16)
            gp_s[part_rows(mb, size, part), :] = cdf + pre * (jnp.exp(pre * pre * -0.5) * 0.3989422804014327)
        top = mid_f + dot_nn(gelu_s[rows, :], wdown[...])
        for seq in range(size):
            mask = valid_mask(jnp.where(pos == last, lens_of(mb, size, seq), SEQ))
            piece = top[seq * SEQ:(seq + 1) * SEQ, :].astype(BF16)
            hout[seq_rows(mb, size, seq), :] = jnp.where(mask > 0.0, piece.astype(F32), 0.0).astype(BF16)

        h_view = hout.at[rows]

        @pl.when(pos < last)
        def _():
            send_to(h_view, xin.at[rows], send_sem.at[mb], x_sem.at[mb], pos + 1)

        @pl.when(pos == last)
        def _():
            for seq in range(size):
                at = start + seq
                home = at // n_own
                s_view = hout.at[seq_rows(mb, size, seq)]
                o_view = out_ref.at[pl.ds(pl.multiple_of((at % n_own) * SEQ, SEQ), SEQ)]

                @pl.when(home == pos)
                def _(s_view=s_view, o_view=o_view):
                    pltpu.make_async_copy(s_view, o_view, send_sem.at[mb]).start()

                @pl.when(home != pos)
                def _(s_view=s_view, o_view=o_view, home=home):
                    send_to(s_view, o_view, send_sem.at[mb], home_sem, home)

        return 0

    for w_copy in w_copies:
        w_copy.wait()
    lax.fori_loop(0, n_mb, functools.partial(forward, SEQ_MB), 0)

    def sent(size, mb, _):
        h_view = hout.at[rows_of(mb, size)]
        pltpu.make_async_copy(h_view, h_view, send_sem.at[mb]).wait()
        return 0

    gain_acc[...] = jnp.zeros_like(gain_acc)

    def norm_back(hid, gain, d_normed):
        inv = inv_rms(hid)
        unit = hid * inv
        d_gain = jnp.sum((d_normed * unit).reshape(hid.shape[0] // 8, 8, D), axis=0)
        scaled = d_normed * gain
        return inv * (scaled - unit * jnp.mean(unit * scaled, axis=-1, keepdims=True)), d_gain

    def backward(size, mb, _):
        rows = rows_of(mb, size)
        start = first_seq(mb, size)
        c_view = cin.at[rows]
        pltpu.make_async_copy(c_view, c_view, c_sem.at[mb]).wait()

        for seq in range(size):
            mask = valid_mask(lens_of(mb, size, seq))
            cin[seq_rows(mb, size, seq), :] = jnp.where(mask > 0.0, cin[seq_rows(mb, size, seq), :].astype(F32), 0.0).astype(BF16)
        d_top = cin[rows, :]
        for part in range(FFN // D):
            cols = slice(part * D, (part + 1) * D)
            d_gelu = dot_nt(d_top, wdown[cols, :])
            dpre_s[rows, cols] = (d_gelu * gp_s[part_rows(mb, size, part), :]).astype(BF16)
        d_nm = dot_nt(dpre_s[rows, :], wup[...])
        d_add, d_gain = norm_back(mid_s[rows, :].astype(F32), gm_ref[...].astype(F32), d_nm)
        gain_acc[1] += d_gain
        d_mid = d_top.astype(F32) + d_add
        d_mid_bf = d_mid.astype(BF16)
        dmid_s[rows, :] = d_mid_bf
        d_ctx = dot_nt(d_mid_bf, wout[...]).astype(BF16)
        for seq in range(size):
            for pair in range(PAIRS):
                v_cols = qkv_s[seq_rows(mb, size, seq), 2 * D + pair * 128:2 * D + (pair + 1) * 128]
                dc = d_ctx[seq * SEQ:(seq + 1) * SEQ, pair * 128:(pair + 1) * 128]
                spot = (seq * PAIRS + pair) * SEQ
                p_rows = pl.ds(pl.multiple_of(start * PAIRS * SEQ + spot, SEQ), SEQ)
                s_scr[spot:spot + SEQ, :] = dot_nt(dc, blocks(v_cols))
                both = dot_tn(p_s[p_rows, :].astype(BF16), dc)
                qkv_s[seq_rows(mb, size, seq), 2 * D + pair * 128:2 * D + (pair + 1) * 128] = jnp.where(
                    first, both[:SEQ], both[SEQ:]).astype(BF16)
        for seq in range(size):
            spot = seq * PAIRS * SEQ
            p_rows = pl.ds(pl.multiple_of(start * PAIRS * SEQ + spot, SEQ), PAIRS * SEQ)
            probs = p_s[p_rows, :].reshape(PAIRS, SEQ, 128)
            d_probs = s_scr[spot:spot + PAIRS * SEQ, :].reshape(PAIRS, SEQ, 128)
            sum_a, sum_b = halves_sum(probs * d_probs)
            d_scores = probs * (d_probs - jnp.where(first[None], sum_a, sum_b)) * (HEAD ** -0.5)
            s_scr[spot:spot + PAIRS * SEQ, :] = d_scores.reshape(PAIRS * SEQ, 128)
        for seq in range(size):
            for pair in range(PAIRS):
                q_at = slice(pair * 128, (pair + 1) * 128)
                k_at = slice(D + pair * 128, D + (pair + 1) * 128)
                q_cols = qkv_s[seq_rows(mb, size, seq), q_at]
                k_cols = qkv_s[seq_rows(mb, size, seq), k_at]
                spot = (seq * PAIRS + pair) * SEQ
                d_sc = s_scr[spot:spot + SEQ, :].astype(BF16)
                both = dot_tn(d_sc, q_cols)
                qkv_s[seq_rows(mb, size, seq), q_at] = dot_nn(d_sc, blocks(k_cols)).astype(BF16)
                qkv_s[seq_rows(mb, size, seq), k_at] = jnp.where(first, both[:SEQ], both[SEQ:]).astype(BF16)
        d_na = dot_nt(qkv_s[rows, :], wqkv[...])
        d_add, d_gain = norm_back(xin[rows, :].astype(F32), ga_ref[...].astype(F32), d_na)
        gain_acc[0] += d_gain

        @pl.when(pos > 0)
        def _():
            sent(size, mb, 0)
            hout[rows, :] = (d_mid + d_add).astype(BF16)
            send_to(hout.at[rows], cin.at[rows], send_sem.at[mb], c_sem.at[mb], pos - 1)

        return 0

    lax.fori_loop(0, n_mb, functools.partial(backward, SEQ_MB), 0)

    gain_all[rep] = jnp.concatenate([jnp.sum(gain_acc[0], axis=0, keepdims=True), jnp.sum(gain_acc[1], axis=0, keepdims=True),
                                     jnp.zeros((6, D), F32)], axis=0)
    for step in range(1, DATA):
        pltpu.make_async_remote_copy(src_ref=gain_all.at[rep], dst_ref=gain_all.at[rep], send_sem=gain_send,
                                     recv_sem=gain_recv.at[rep], device_id={'data': (rep + step) % DATA},
                                     device_id_type=MESH).start()

    per_tile = TILE // PART_B
    n_down, n_up, n_qkv = FFN // TILE, (D // TILE) * (FFN // D), (D // TILE) * 3

    def tile_kinds(tile):
        up, qkv, out = tile - n_down, tile - n_down - n_up, tile - n_down - n_up - n_qkv
        return (
            (tile < n_down, gelu_s, cin, tile, 0),
            ((up >= 0) & (qkv < 0), nm_s, dpre_s, up // (FFN // D), up % (FFN // D)),
            ((qkv >= 0) & (out < 0), na_s, qkv_s, qkv // 3, qkv % 3),
            (out >= 0, ctx_s, dmid_s, out, 0),
        )

    def tile_at(tile):
        return pl.ds(pl.multiple_of(tile * TILE, TILE), TILE)

    def compute_tile(tile):
        for cond, lhs, rhs, at_row, at_col in tile_kinds(tile):
            @pl.when(cond)
            def _(lhs=lhs, rhs=rhs, at_row=at_row, at_col=at_col):
                cols = pl.ds(0, D) if rhs.shape[1] == D else pl.ds(pl.multiple_of(at_col * D, D), D)
                gp_s[tile_at(tile), :] = dot_tn(lhs[:, pl.ds(pl.multiple_of(at_row * TILE, TILE), TILE)], rhs[:, cols])

    to_y, to_right, to_left = rep + 1 - 2 * rep_y, rep + 2, rep - 2

    def part_done(src, colour, link, slot):
        pltpu.make_async_copy(src, src, part_send.at[colour, link, slot]).wait()

    def ship_part(unit, slot, src, dst, colour, link, target, value):
        @pl.when(unit >= SLOTS)
        def _():
            part_done(src, colour, link, slot)

        src[...] = value
        pltpu.make_async_remote_copy(src_ref=src, dst_ref=dst, send_sem=part_send.at[colour, link, slot],
                                     recv_sem=sum_recv.at[colour, link, slot], device_id={'data': target},
                                     device_id_type=MESH).start()

    def ship(src, dst, link, recv, target):
        pltpu.make_async_remote_copy(src_ref=src, dst_ref=dst, send_sem=sum_send.at[link], recv_sem=recv,
                                     device_id={'data': target}, device_id_type=MESH).start()

    def arrived(view, recv):
        pltpu.make_async_copy(view, view, recv).wait()

    def gp_rows(start, size):
        return pl.ds(pl.multiple_of(start, 8), size)

    def line_actions(zz, colour, block, size, buf_l, buf_r, out_l, out_r, hop_rs, hop_ag):
        chunk = size // LINE
        own, above = zz * chunk, (zz + 1) * chunk

        def rs_right(unit, slot):
            at = block(unit)
            if zz > 0:
                arrived(buf_l.at[slot, own:size], sum_recv.at[colour, 1, slot])
                gp_s[gp_rows(at + own, chunk), :] += buf_l[slot, own:above, :]
            if zz < LINE - 1:
                value = gp_s[gp_rows(at + above, size - above), :]
                if zz > 0:
                    value = value + buf_l[slot, above:size, :]
                ship_part(unit, slot, out_r.at[slot, above:size], buf_l.at[slot, above:size], colour, 1, to_right, value)

        def rs_left(unit, slot):
            at = block(unit)
            if zz < LINE - 1:
                arrived(buf_r.at[slot, 0:above], sum_recv.at[colour, 2, slot])
                gp_s[gp_rows(at + own, chunk), :] += buf_r[slot, own:above, :]
            if zz > 0:
                value = gp_s[gp_rows(at, own), :]
                if zz < LINE - 1:
                    value = value + buf_r[slot, 0:own, :]
                ship_part(unit, slot, out_l.at[slot, 0:own], buf_r.at[slot, 0:own], colour, 2, to_left, value)

        def ag_right(unit, slot):
            at = block(unit)
            if zz > 0:
                arrived(gp_s.at[gp_rows(at, own)], sum_recv.at[colour, 3, slot])
            if zz < LINE - 1:
                view = gp_s.at[gp_rows(at, above)]
                ship(view, view, 1, sum_recv.at[colour, 3, slot], to_right)

        def ag_left(unit, slot):
            at = block(unit)
            if zz < LINE - 1:
                arrived(gp_s.at[gp_rows(at + above, size - above)], sum_recv.at[colour, 4, slot])
            if zz > 0:
                view = gp_s.at[gp_rows(at + own, size - own)]
                ship(view, view, 2, sum_recv.at[colour, 4, slot], to_left)

        return ([(hop_rs + zz, rs_right), (hop_rs + LINE - 1 - zz, rs_left)],
                [(hop_ag + zz, ag_right), (hop_ag + LINE - 1 - zz, ag_left)])

    half_a, part_b = TILE // 2, PART_B // LINE
    half_b = part_b // 2

    def actions_a(zz):
        def mine(unit):
            return unit * TILE + rep_y * half_a

        def theirs(unit):
            return unit * TILE + (1 - rep_y) * half_a

        def y_send(unit, slot):
            ship_part(unit, slot, ya_out.at[slot], ya_buf.at[slot], 0, 0, to_y, gp_s[gp_rows(theirs(unit), half_a), :])

        def y_add(unit, slot):
            arrived(ya_buf.at[slot], sum_recv.at[0, 0, slot])
            gp_s[gp_rows(mine(unit), half_a), :] += ya_buf[slot]

        def y_give(unit, slot):
            view = gp_s.at[gp_rows(mine(unit), half_a)]
            ship(view, view, 0, sum_recv.at[0, 5, slot], to_y)

        def finish(unit, slot):
            arrived(gp_s.at[gp_rows(theirs(unit), half_a)], sum_recv.at[0, 5, slot])

        scatter, gather = line_actions(zz, 0, mine, half_a, la_buf, ra_buf, la_out, ra_out, 1, 4)
        return [(0, y_send), (1, y_add)] + scatter + gather + [(7, y_give), (8, finish)]

    def actions_b(zz, colour, base, bufs, outs):
        y_buf, l_buf, r_buf = bufs
        y_out, l_out, r_out = outs

        def block(unit):
            return UNITS_A * TILE + (base + unit) * PART_B

        def mine(unit):
            return block(unit) + zz * part_b + rep_y * half_b

        def theirs(unit):
            return block(unit) + zz * part_b + (1 - rep_y) * half_b

        def y_send(unit, slot):
            ship_part(unit, slot, y_out.at[slot], y_buf.at[slot], colour, 0, to_y, gp_s[gp_rows(theirs(unit), half_b), :])

        def y_add(unit, slot):
            arrived(y_buf.at[slot], sum_recv.at[colour, 0, slot])
            gp_s[gp_rows(mine(unit), half_b), :] += y_buf[slot]
            view = gp_s.at[gp_rows(mine(unit), half_b)]
            ship(view, view, 0, sum_recv.at[colour, 5, slot], to_y)

        def y_done(unit, slot):
            arrived(gp_s.at[gp_rows(theirs(unit), half_b)], sum_recv.at[colour, 5, slot])

        scatter, gather = line_actions(zz, colour, block, PART_B, l_buf, r_buf, l_out, r_out, 0, 5)
        return scatter + [(3, y_send), (4, y_add), (5, y_done)] + gather

    def unit_of(colour, tick):
        inside = (tick >= 0) & (tick < UNITS_A)
        if colour < 2:
            return inside, tick
        return inside & (tick % EXTRA == 0), tick // EXTRA

    def run_actions(tick, hops):
        for zz in range(LINE):
            @pl.when(rep_z == zz)
            def _(zz=zz):
                todo = (
                    actions_a(zz),
                    actions_b(zz, 1, 0, (yb_buf, lb_buf, rb_buf), (yb_out, lb_out, rb_out)),
                    actions_b(zz, 2, UNITS_A, (yx_buf, lx_buf, rx_buf), (yx_out, lx_out, rx_out)),
                )
                for want in hops:
                    for colour in range(3):
                        fns = [fn for hop, fn in todo[colour] if hop == want]
                        if not fns:
                            continue
                        fresh, unit = unit_of(colour, tick - want)

                        @pl.when(fresh)
                        def _(fns=fns, unit=unit):
                            for fn in fns:
                                fn(unit, unit % SLOTS)

    def compute_for(tick):
        @pl.when(tick < UNITS_A)
        def _():
            compute_tile(tick)

        for colour, base in ((1, 0), (2, UNITS_A)):
            fresh, unit = unit_of(colour, tick)

            @pl.when(fresh & (unit % per_tile == 0))
            def _(unit=unit, base=base):
                compute_tile(UNITS_A + (base + unit) // per_tile)

    compute_for(0)

    def tick_step(tick, _):
        run_actions(tick, [0])
        compute_for(tick + 1)
        run_actions(tick, range(1, 9))
        return 0

    lax.fori_loop(0, UNITS_A + 8, tick_step, 0)

    def sent_all(link, size):
        view = gp_s.at[pl.ds(0, size)]
        pltpu.make_async_copy(view, view, sum_send.at[link]).wait()

    for zz in range(LINE):
        @pl.when(rep_z == zz)
        def _(zz=zz):
            line_rows = UNITS_A * (half_a // LINE) + (UNITS_A + UNITS_X) * part_b
            sent_all(0, UNITS_A * half_a + (UNITS_A + UNITS_X) * half_b)
            if zz < LINE - 1:
                sent_all(1, line_rows * (zz + 1))
            if zz > 0:
                sent_all(2, line_rows * (LINE - zz))
            for slot in range(SLOTS):
                for colour, (out_y, out_l, out_r) in enumerate(
                        ((ya_out, la_out, ra_out), (yb_out, lb_out, rb_out), (yx_out, lx_out, rx_out))):
                    size = out_l.shape[1]
                    part_done(out_y.at[slot], colour, 0, slot)
                    if zz < LINE - 1:
                        part_done(out_r.at[slot, (zz + 1) * size // LINE:size], colour, 1, slot)
                    if zz > 0:
                        part_done(out_l.at[slot, 0:zz * size // LINE], colour, 2, slot)

    for step in range(1, DATA):
        peer = (rep + step) % DATA
        pltpu.make_async_copy(gain_all.at[peer], gain_all.at[peer], gain_recv.at[peer]).wait()
    total = gain_all[0]
    for peer in range(1, DATA):
        total = total + gain_all[peer]
    gain_ref[...] = total
    pltpu.make_async_copy(gain_all.at[pl.ds(0, DATA - 1)], gain_all.at[pl.ds(0, DATA - 1)], gain_send).wait()

    lax.fori_loop(0, n_mb, functools.partial(sent, SEQ_MB), 0)

    @pl.when(pos < last)
    def _():
        pltpu.make_async_copy(out_ref, out_ref, home_sem).wait()

    for step in range(1, PIPE):
        pltpu.make_async_copy(lens_buf.at[own_slab], lens_buf.at[own_slab], in_sem.at[step - 1]).wait()
    for src, _, send, _, target in spread:
        @pl.when(target != pos)
        def _(src=src, send=send):
            pltpu.make_async_copy(src, src, send).wait()


def run_pass(acts, cots, lens, w_qkv, w_out, w_up, w_down, gain_a, gain_m):
    n_tok = acts.shape[0] * PIPE
    n_seq = n_tok // SEQ
    n_mb = n_seq // SEQ_MB
    any_spec = pl.BlockSpec(memory_space=pl.ANY)
    vmem_spec = pl.BlockSpec(memory_space=pltpu.VMEM)
    dma = pltpu.SemaphoreType.DMA
    return pl.pallas_call(
        functools.partial(pass_kernel, n_seq),
        out_shape=(
            pltpu.VMEM(acts.shape, BF16),
            pltpu.VMEM((n_tok * FFN // D, D), F32),
            pltpu.VMEM((8, D), F32),
        ),
        in_specs=[any_spec] * 2 + [pl.BlockSpec(memory_space=pltpu.SMEM)] + [any_spec] * 4 + [vmem_spec] * 2,
        out_specs=[vmem_spec] * 3,
        scratch_shapes=[
            pltpu.VMEM((D, 3 * D), BF16),
            pltpu.VMEM((D, D), BF16),
            pltpu.VMEM((D, FFN), BF16),
            pltpu.VMEM((FFN, D), BF16),
            pltpu.VMEM((n_seq, 8, 128), jnp.int32),
            pltpu.VMEM((n_tok, D), BF16),
            pltpu.VMEM((n_tok, D), BF16),
            pltpu.VMEM((n_tok, D), BF16),
            pltpu.VMEM((n_tok, D), BF16),
            pltpu.VMEM((n_tok, 3 * D), BF16),
            pltpu.VMEM((n_tok, D), BF16),
            pltpu.VMEM((n_tok, D), BF16),
            pltpu.VMEM((n_tok, D), BF16),
            pltpu.VMEM((n_tok, FFN), BF16),
            pltpu.VMEM((n_tok, FFN), BF16),
            pltpu.VMEM((n_tok, D), BF16),
            pltpu.VMEM((n_tok * PAIRS, 128), F32),
            pltpu.VMEM((SEQ_MB * PAIRS * SEQ, 128), F32),
            pltpu.VMEM((2, 8, D), F32),
            pltpu.VMEM((DATA, 8, D), F32),
        ] + [
            pltpu.VMEM((SLOTS, size, D), F32)
            for size in ((TILE // 2,) * 3 + (PART_B // LINE // 2, PART_B, PART_B) * 2) * 2
        ] + [
            dma((4,)),
            dma((2 * (n_seq // PIPE) + PIPE - 1,)),
            dma((n_mb,)),
            dma((n_mb,)),
            dma((PIPE,)),
            dma((n_mb,)),
            dma,
            dma((3, 6, SLOTS)),
            dma((3,)),
            dma((3, 3, SLOTS)),
            dma((DATA,)),
            dma,
        ],
        compiler_params=pltpu.CompilerParams(collective_id=0, has_side_effects=True, vmem_limit_bytes=50 * 1024 * 1024),
    )(acts, cots, lens, w_qkv, w_out, w_up, w_down, gain_a, gain_m)


def write_kernel(acts_ref, tiles_ref, gain_ref, out_ref, gqkv_ref, gout_ref, gup_ref, gdown_ref, gga_ref, ggm_ref,
                 out_sem, put_sem):
    give = pltpu.make_async_copy(acts_ref, out_ref, out_sem)
    give.start()
    row = 0
    dsts = (gdown_ref, gup_ref, gqkv_ref, gout_ref)
    for dst in dsts:
        for at_row in range(0, dst.shape[0], TILE):
            for at_col in range(0, dst.shape[1], D):
                pltpu.make_async_copy(tiles_ref.at[row:row + TILE], dst.at[at_row:at_row + TILE, at_col:at_col + D],
                                      put_sem).start()
                row += TILE
    gga_ref[...] = gain_ref[0:1, :]
    ggm_ref[...] = gain_ref[1:2, :]
    give.wait()
    pltpu.make_async_copy(tiles_ref, tiles_ref, put_sem).wait()


def write_out(acts, tiles, gains):
    any_spec = pl.BlockSpec(memory_space=pl.ANY)
    vmem_spec = pl.BlockSpec(memory_space=pltpu.VMEM)
    dma = pltpu.SemaphoreType.DMA
    return pl.pallas_call(
        write_kernel,
        out_shape=(
            jax.ShapeDtypeStruct(acts.shape, BF16),
            jax.ShapeDtypeStruct((D, 3 * D), F32),
            jax.ShapeDtypeStruct((D, D), F32),
            jax.ShapeDtypeStruct((D, FFN), F32),
            jax.ShapeDtypeStruct((FFN, D), F32),
            jax.ShapeDtypeStruct((1, D), F32),
            jax.ShapeDtypeStruct((1, D), F32),
        ),
        in_specs=[any_spec, any_spec, vmem_spec],
        out_specs=[any_spec] * 5 + [vmem_spec] * 2,
        scratch_shapes=[dma, dma],
        compiler_params=pltpu.CompilerParams(vmem_limit_bytes=4 * 1024 * 1024),
    )(acts, tiles, gains)


def solution(mesh):
    row_spec = P(('data', 'pipe'))
    stage_spec = P('pipe')

    def device_pass(acts_in, cot_out, seq_lens, w_qkv, w_out, w_up, w_down, gain_attn, gain_mlp):
        outs = run_pass(acts_in.reshape(-1, D), cot_out.reshape(-1, D), seq_lens, w_qkv.reshape(D, 3 * D),
                        w_out.reshape(D, D), w_up.reshape(D, FFN), w_down.reshape(FFN, D),
                        gain_attn, gain_mlp)
        acts_out, g_qkv, g_out, g_up, g_down, g_ga, g_gm = write_out(*outs)
        grads = (g_qkv.reshape(w_qkv.shape), g_out.reshape(w_out.shape), g_up.reshape(w_up.shape), g_down.reshape(w_down.shape),
                 g_ga, g_gm)
        return (acts_out.reshape(acts_in.shape),) + grads

    return jax.shard_map(device_pass, mesh=mesh, in_specs=(row_spec, row_spec, row_spec) + (stage_spec,) * 6, out_specs=(row_spec,) + (stage_spec,) * 6, check_vma=False)
```
